32 devices in a mesh: seq: 8 (over y, x, core), tp: 4 (over z).
Axes of the slice: x: 2, y: 2, z: 4, core: 2. Of those that a mesh axis runs over, the one named last changes fastest.
Arguments:
- states: bfloat16 [8, 128, 2048], P('seq', None, 'tp'), may hold values from -60 to 60, as said below
- cotangent: bfloat16 [8, 128, 2048], P('seq', None, 'tp'), may hold values from -12 to 12, as said below
- wq: bfloat16 [2048, 2048], P(None, 'tp'), may hold values from -0.125 to 0.125
- wk: bfloat16 [2048, 512], P(None, 'tp'), may hold values from -0.125 to 0.125
- wv: bfloat16 [2048, 512], P(None, 'tp'), may hold values from -0.125 to 0.125
- wo: bfloat16 [2048, 2048], P('tp'), may hold values from -0.125 to 0.125
Outputs:
- gram: float32 [8, 8], P('seq')
The draws below stay inside these ranges and needn't reach their ends.
Inputs may be any that keep to these rules, and one draw needn't show every extreme that they name: `states`: finite values. `cotangent`: finite values.
All inputs are finite; a program needn't handle non-finite values.
Results may differ from the reference program's by a relative error of at most 0.0025.
Values may be sent and summed in bfloat16 or wider, within the bound.
A program may use at most 64 MiB of HBM per device.

```python
import jax
import jax.numpy as jnp
from jax import lax

D = 2048
HEADS = 32
KV_HEADS = 8
HEAD_DIM = 64
TOKENS_PER_SEQ = 128
SEQUENCE_COUNT = 8


def candidate_rows(key):
    pick_key = jax.random.fold_in(key, 17)
    picked = jax.random.randint(pick_key, (SEQUENCE_COUNT, TOKENS_PER_SEQ), 0, 2).astype(jnp.int32)
    return picked + 2 * jnp.arange(TOKENS_PER_SEQ, dtype=jnp.int32)[None, :]


def draw_states(key, part):
    row_index = candidate_rows(key)
    table_key = jax.random.fold_in(key, 301)
    noise_key = jax.random.fold_in(key, 302)
    candidates = jax.random.normal(table_key, (2 * TOKENS_PER_SEQ, D), jnp.float32)
    noise = 0.4 * jax.random.normal(noise_key, (SEQUENCE_COUNT, TOKENS_PER_SEQ, D), jnp.float32)
    tokens_base = jnp.take(candidates, row_index, axis=0)
    return jnp.clip(tokens_base + noise, -12.0, 12.0).astype(jnp.bfloat16)


def draw_cotangent(key, part):
    row_index = candidate_rows(key)
    table_key = jax.random.fold_in(key, 401)
    noise_key = jax.random.fold_in(key, 402)
    candidates = jax.random.normal(table_key, (2 * TOKENS_PER_SEQ, D), jnp.float32)
    noise = 0.4 * jax.random.normal(noise_key, (SEQUENCE_COUNT, TOKENS_PER_SEQ, D), jnp.float32)
    tokens_base = jnp.take(candidates, row_index, axis=0)
    return jnp.clip(tokens_base + noise, -12.0, 12.0).astype(jnp.bfloat16)


def shard_levels(own_key, shape, cuts, low, high):
    def one(axis_at, parts):
        draws = jax.random.uniform(jax.random.fold_in(jax.random.fold_in(own_key, 6), axis_at), (parts,), jnp.float32, low / len(cuts), high / len(cuts))
        return jnp.repeat(jnp.exp(draws), shape[axis_at] // parts).reshape((-1,) + (1,) * (len(shape) - axis_at - 1))

    gain = one(*cuts[0])
    for cut in cuts[1:]:
        gain = gain * one(*cut)
    return gain


def centred(rng, extent, deviation, limit, shards=(), kind=jnp.bfloat16):
    drawn = deviation * jax.random.normal(rng, extent, jnp.float32)
    if shards:
        drawn = drawn * shard_levels(rng, extent, shards, -0.22, 0.18)
    return jnp.clip(drawn, -limit, limit).astype(kind)


def setup_inputs(seed: int = 0) -> dict:
    seeds = jax.random.split(jax.random.key(seed), 7)
    return {
        "states": draw_states(jax.random.fold_in(seeds[6], 71), 0),
        "cotangent": draw_cotangent(jax.random.fold_in(seeds[6], 71), 0),
        "wq": centred(seeds[2], (D, D), D ** -0.5, 0.125, ((1, 4),)),
        "wk": centred(seeds[3], (D, KV_HEADS * HEAD_DIM), D ** -0.5, 0.125, ((1, 4),)),
        "wv": centred(seeds[4], (D, KV_HEADS * HEAD_DIM), D ** -0.5, 0.125, ((1, 4),)),
        "wo": centred(seeds[5], (D, D), D ** -0.5, 0.125, ((0, 4),)),
    }


theta_base = 500000.0

def rope_tables(length, head_dim):
    half_dim = head_dim // 2
    freqs_k = theta_base ** (-(jnp.arange(half_dim, dtype=jnp.float32) * 2.0 / head_dim))
    angles = jnp.arange(length, dtype=jnp.float32)[:, None] * freqs_k[None, :]
    angles = jnp.concatenate([angles, angles], axis=1)
    return (jnp.cos(angles)[:, None, :], jnp.sin(angles)[:, None, :])

def rotate(values_in, cos_table, sine_table):
    half_dim = values_in.shape[-1] // 2
    turned = jnp.concatenate([-values_in[..., half_dim:], values_in[..., :half_dim]], axis=-1)
    return values_in * cos_table + turned * sine_table

def reference(states, cotangent, wq, wk, wv, wo):
    seqs, length, model_width = states.shape
    group_size = HEADS // KV_HEADS
    tok_rows = seqs * length
    cos_table, sine_table = rope_tables(length, HEAD_DIM)
    flat_states = states.reshape(tok_rows, model_width)
    query_heads = jnp.dot(flat_states, wq, preferred_element_type=jnp.float32).reshape(seqs, length, HEADS, HEAD_DIM)
    query_heads = rotate(query_heads, cos_table, sine_table).astype(jnp.bfloat16).reshape(seqs, length, KV_HEADS, group_size, HEAD_DIM)
    key_heads = jnp.dot(flat_states, wk, preferred_element_type=jnp.float32).reshape(seqs, length, KV_HEADS, HEAD_DIM)
    key_heads = rotate(key_heads, cos_table, sine_table).astype(jnp.bfloat16)
    value_heads = jnp.dot(flat_states, wv, preferred_element_type=jnp.float32).astype(jnp.bfloat16).reshape(seqs, length, KV_HEADS, HEAD_DIM)
    scores = jnp.einsum('sqkgd,stkd->skgqt', query_heads.astype(jnp.float32), key_heads.astype(jnp.float32)) * HEAD_DIM ** (-0.5)
    causal = jnp.arange(length)[:, None] >= jnp.arange(length)[None, :]
    scores = jnp.where(causal, scores, -jnp.inf)
    weights_bf = jax.nn.softmax(scores, axis=-1).astype(jnp.bfloat16)
    attended = jnp.einsum('skgqt,stkd->sqkgd', weights_bf.astype(jnp.float32), value_heads.astype(jnp.float32)).astype(jnp.bfloat16).reshape(seqs, length, model_width)
    grad_attended = lax.dot_general(cotangent.reshape(tok_rows, model_width), wo, (((1,), (1,)), ((), ())), preferred_element_type=jnp.float32).astype(jnp.bfloat16).reshape(seqs, length, KV_HEADS, group_size, HEAD_DIM)
    value_gradient = jnp.einsum('skgqt,sqkgd->stkd', weights_bf.astype(jnp.float32), grad_attended.astype(jnp.float32)).astype(jnp.bfloat16).reshape(seqs, length, KV_HEADS * HEAD_DIM)
    states_wide = states.astype(jnp.float32)
    grad_wv = jnp.einsum('std,stv->sdv', states_wide, value_gradient.astype(jnp.float32), precision=lax.Precision.HIGHEST)
    kernel = jnp.einsum('sdv,rdv->sr', grad_wv, grad_wv, precision=lax.Precision.HIGHEST)
    attended_wide = attended.astype(jnp.float32)
    cot_wide = cotangent.astype(jnp.float32)
    block_cols = model_width // 8

    def block_term(begin_col):
        cot_block = lax.dynamic_slice_in_dim(cot_wide, begin_col, block_cols, 2)
        grad_wo = jnp.einsum('std,ste->sde', attended_wide, cot_block, precision=lax.Precision.HIGHEST)
        return jnp.einsum('sde,rde->sr', grad_wo, grad_wo, precision=lax.Precision.HIGHEST)
    starts = (jnp.arange(8) * block_cols).astype(jnp.int32)
    kernel = kernel + lax.optimization_barrier(jnp.sum(lax.map(block_term, starts), axis=0))
    kernel_diag = jnp.diagonal(kernel)
    return kernel / jnp.sqrt(kernel_diag[:, None] * kernel_diag[None, :])
```

```python
import functools

import jax
import jax.numpy as jnp
import numpy as np
from jax import lax
from jax.experimental import pallas as pl
from jax.experimental.pallas import tpu as pltpu
from jax.sharding import PartitionSpec as P

HEADS = 32
KV_HEADS = 8
HEAD_DIM = 64
THETA = 500000.0
LANES = 128
HALVES = 2
GROUP = HEADS // KV_HEADS
F32, BF16 = jnp.float32, jnp.bfloat16

NT = (((1,), (1,)), ((), ()))
TN = (((0,), (0,)), ((), ()))


def rope_tables(length):
    half = HEAD_DIM // 2
    freqs = np.float32(THETA) ** (-(np.arange(half, dtype=np.float32) * np.float32(2.0 / HEAD_DIM)))
    angles = np.arange(length, dtype=np.float32)[:, None] * freqs[None, :].astype(np.float32)
    cos, sin = np.cos(angles), np.sin(angles)
    return (
        np.concatenate([cos, cos] * 2, axis=1).astype(np.float32),
        np.concatenate([-sin, sin] * 2, axis=1).astype(np.float32),
    )


def dot(a, b, dims=None):
    if dims is None:
        return jnp.dot(a, b, preferred_element_type=F32)
    return lax.dot_general(a, b, dims, preferred_element_type=F32)


def place_of(index, n):
    if n % 8:
        return index
    block, rest = index // 8, index % 8
    row, col, core = rest // 4, (rest // 2) % 2, rest % 2
    return block * 8 + 2 * (2 * row + (row + col) % 2) + core


def index_at(place, n):
    if n % 8:
        return place
    block, rest = place // 8, place % 8
    spot, core = rest // 2, rest % 2
    row = spot // 2
    return block * 8 + 2 * (2 * row + (row + spot) % 2) + core


def kernel(
    n, tp,
    states_ref, cot_ref, cos_ref, sin_ref, wq_hbm, wk_hbm, wv_hbm, wo_hbm,
    out_ref,
    xs, cs, wqb, wkb, wvb, wob, q_acc, k_acc, v_acc, g_acc,
    x_in, c_in, d_in, b_in, att_own, a_in, ad_in, ab_in, gv_own, g_in, gd_in, gb_in,
    probs, ad, rin, xin, full, t2,
    w_sem, z_snd, z_rcv, p_snd, p_rcv, f_snd, f_rcv, b_snd, b_rcv,
    a_snd, a_rcv, af_snd, af_rcv, g_snd, g_rcv,
    i_snd, r_rcv, s_rcv, o_snd, o_rcv, r2_snd, r2_rcv,
):
    length, width = states_ref.shape
    kv_cols = k_acc.shape[1]
    ring = n // 2
    far = ring // 2
    mid = tp // 2
    hrows = length // HALVES
    lanes = t2.shape[3]
    me = lax.axis_index("seq")
    col = lax.axis_index("tp")
    place = place_of(me, n)
    chip, core = place // 2, place % 2
    low_chip = chip < far
    last = tp - 1

    def device(hop, c):
        return index_at(2 * ((chip + hop + ring) % ring) + c, n)

    partner = device(0, 1 - core)

    def each(lo, hi, body):
        if hi - lo <= 8:
            for i in range(lo, hi):
                body(i)
        else:
            lax.fori_loop(lo, hi, lambda i, c: (body(i), c)[1], 0)

    def remote(src, dst, snd, rcv, to):
        return pltpu.make_async_remote_copy(
            src_ref=src, dst_ref=dst, send_sem=snd, recv_sem=rcv, device_id=to
        )

    weight_copies = []
    for k in range(tp):
        at = pl.ds(pl.multiple_of(((col - k + tp) % tp) * width, width), width)
        weight_copies.append([
            pltpu.make_async_copy(wq_hbm.at[at, :], wqb.at[k], w_sem.at[4 * k]),
            pltpu.make_async_copy(wk_hbm.at[at, :], wkb.at[k], w_sem.at[4 * k + 1]),
            pltpu.make_async_copy(wv_hbm.at[at, :], wvb.at[k], w_sem.at[4 * k + 2]),
            pltpu.make_async_copy(wo_hbm.at[:, at], wob.at[k], w_sem.at[4 * k + 3]),
        ])

    barrier = pltpu.get_barrier_semaphore()
    pl.when(col > 0)(
        lambda: pl.semaphore_signal(barrier, inc=1, device_id={"tp": col - 1})
    )
    pl.when(col < last)(
        lambda: pl.semaphore_signal(barrier, inc=1, device_id={"tp": col + 1})
    )
    each(1, n, lambda o: pl.semaphore_signal(barrier, inc=1, device_id={"seq": (me + o) % n}))
    order = [0] + [s for k in range(1, tp) for s in dict.fromkeys((k, tp - k)) if k <= tp - k]
    for part in (slice(0, 3), slice(3, 4)):
        for k in order:
            for c in weight_copies[k][part]:
                c.start()
    ends = (col == 0).astype(jnp.int32) + (col == last).astype(jnp.int32)
    pl.semaphore_wait(barrier, n + 1 - ends)

    inputs = (states_ref, cot_ref)
    held = (xs, cs)

    def rows_of(h):
        return pl.ds(h * hrows, hrows)

    def up(which, k, h):
        src = inputs[which] if k == 1 else held[which].at[k - 2]
        return remote(
            src.at[rows_of(h), :], held[which].at[k - 1, rows_of(h), :],
            z_snd.at[which, 0, k - 1, h], z_rcv.at[which, k - 1, h], {"tp": (col + 1) % tp},
        )

    def down(which, k, h):
        src = inputs[which] if k == 1 else held[which].at[tp - k]
        return remote(
            src.at[rows_of(h), :], held[which].at[tp - k - 1, rows_of(h), :],
            z_snd.at[which, 1, k - 1, h], z_rcv.at[which, tp - k - 1, h],
            {"tp": (col + tp - 1) % tp},
        )

    def sends_up(k):
        return (col >= k - 1) & (col < last)

    def sends_down(k):
        return (col + k - 1 < tp) & (col > 0)

    def landed(which, slot, h):
        remote(
            inputs[which].at[rows_of(h), :], held[which].at[slot - 1, rows_of(h), :],
            z_snd.at[which, 0, 0, h], z_rcv.at[which, slot - 1, h], {"tp": (col + 1) % tp},
        ).wait_recv()

    def begin_up(which):
        for h in range(HALVES):
            up(which, 1, h).start()

    def begin_down(which):
        for h in range(HALVES):
            down(which, 1, h).start()

    def relay(which, k):
        for h in range(HALVES):
            @pl.when((col >= k) & (col < last))
            def _():
                landed(which, k, h)
                up(which, k + 1, h).start()

            @pl.when((col + k < tp) & (col > 0))
            def _():
                landed(which, tp - k, h)
                down(which, k + 1, h).start()

    def settle(which, k):
        for h in range(HALVES):
            pl.when((col >= k) & (col == last))(lambda: landed(which, k, h))
            pl.when((col + k < tp) & (col == 0))(lambda: landed(which, tp - k, h))

    def arrivals(k, body):
        pl.when(col >= k)(lambda: body(k))
        pl.when(col + k < tp)(lambda: body(tp - k))

    def follow(k):
        pl.when((col == k) & (col < last))(lambda: begin_up(1))
        pl.when((last - col == k) & (col > 0))(lambda: begin_down(1))

    pl.when(col < last)(lambda: begin_up(0))
    pl.when(col > 0)(lambda: begin_down(0))
    follow(0)

    def x_copy(d):
        return remote(
            states_ref, x_in.at[2 * (d - 1)], p_snd.at[0, d - 1], p_rcv.at[0, d - 1],
            {"seq": device(-d, core)},
        )

    def c_copy(d):
        return remote(
            cot_ref, c_in.at[2 * (d - 1)], p_snd.at[1, d - 1], p_rcv.at[1, d - 1],
            {"seq": device(d, core)},
        )

    def far_copy(src):
        return remote(
            src, d_in.at[0], p_snd.at[2, 0], p_rcv.at[2, 0], {"seq": device(far, core)}
        )

    def beside_copy(src):
        return remote(src, b_in, b_snd.at[0], b_rcv.at[0], {"seq": partner})

    def x_pass(d):
        return remote(
            x_in.at[2 * (d - 1)], x_in.at[2 * (d - 1) + 1], f_snd.at[0, d - 1],
            f_rcv.at[0, d - 1], {"seq": partner},
        )

    def c_pass(d):
        return remote(
            c_in.at[2 * (d - 1)], c_in.at[2 * (d - 1) + 1], f_snd.at[1, d - 1],
            f_rcv.at[1, d - 1], {"seq": partner},
        )

    def far_pass():
        return remote(
            d_in.at[0], d_in.at[1], f_snd.at[2, 0], f_rcv.at[2, 0], {"seq": partner}
        )

    def start_near(d):
        x_copy(d).start()
        c_copy(d).start()

    pl.when(core == 1)(lambda: beside_copy(states_ref).start())
    pl.when(core == 0)(lambda: beside_copy(cot_ref).start())
    each(1, far, start_near)
    pl.when(low_chip)(lambda: far_copy(states_ref).start())
    pl.when(chip >= far)(lambda: far_copy(cot_ref).start())

    def pass_near(d):
        x_copy(d).wait_recv()
        x_pass(d).start()
        c_copy(d).wait_recv()
        c_pass(d).start()

    def pass_far():
        far_copy(states_ref).wait_recv()
        far_pass().start()

    def project_states(slot):
        for c in weight_copies[slot][:3]:
            c.wait()
        x = states_ref[...] if slot == 0 else xs[slot - 1]
        for acc, w in ((q_acc, wqb), (k_acc, wkb), (v_acc, wvb)):
            piece = dot(x, w[slot])
            acc[...] = piece if slot == 0 else acc[...] + piece

    def project_cot(slot):
        weight_copies[slot][3].wait()
        y = cot_ref[...] if slot == 0 else cs[slot - 1]
        piece = dot(y, wob[slot], NT)
        g_acc[...] = piece if slot == 0 else g_acc[...] + piece

    def group_at(g):
        return (0, 3) if isinstance(g, int) and g == 0 else (2 * g + 1, 2)

    def inner(g, act):
        lo, count = group_at(g)
        part = pl.ds(lo, count)

        def copy(dst, rcv, to):
            return remote(ad.at[part], dst.at[part], i_snd.at[g], rcv.at[g], {"tp": to})

        pl.when(col < mid - 1)(lambda: act(copy(rin, r_rcv, (col + 1) % tp)))
        pl.when(col > mid)(lambda: act(copy(rin, r_rcv, (col + tp - 1) % tp)))
        pl.when(col == mid - 1)(lambda: act(copy(xin, s_rcv, (col + 1) % tp)))
        pl.when(col == mid)(lambda: act(copy(xin, s_rcv, (col + tp - 1) % tp)))

    def outer(g, act):
        lo, count = group_at(g)
        part = pl.ds(lo, count)

        def copy(to):
            return remote(full.at[part], full.at[part], o_snd.at[g], o_rcv.at[g], {"tp": to})

        pl.when((col < mid) & (col > 0))(lambda: act(copy((col + tp - 1) % tp)))
        pl.when((col >= mid) & (col < last))(lambda: act(copy((col + 1) % tp)))

    def waits_on(buf, rcv, g):
        lo, count = group_at(g)
        part = pl.ds(lo, count)
        remote(
            buf.at[part], buf.at[part], o_snd.at[g], rcv.at[g], {"tp": (col + 1) % tp}
        ).wait_recv()

    edge = (col == 0) | (col == last)
    central = (col == mid - 1) | (col == mid)

    def publish(g):
        pl.when(edge)(lambda: inner(g, lambda c: c.start()))

    def chain(g):
        lo, count = group_at(g)
        part = pl.ds(lo, count)

        @pl.when(jnp.logical_not(edge))
        def _():
            waits_on(rin, r_rcv, g)
            ad[part] = (ad[part].astype(F32) + rin[part].astype(F32)).astype(BF16)
            inner(g, lambda c: c.start())

    def total(g):
        lo, count = group_at(g)
        part = pl.ds(lo, count)

        @pl.when(central)
        def _():
            waits_on(xin, s_rcv, g)
            full[part] = (ad[part].astype(F32) + xin[part].astype(F32)).astype(BF16)
            outer(g, lambda c: c.start())

    def totals_here(g):
        @pl.when(jnp.logical_not(central))
        def _():
            waits_on(full, o_rcv, g)
            pl.when(jnp.logical_not(edge))(lambda: outer(g, lambda c: c.start()))

    def two(own, buf, at):
        both = buf[pl.ds(at, 2)].reshape(2 * length, buf.shape[2])
        return dot(own[...], both, NT)

    def put(g, tiles):
        lo = 2 * g + 1
        ad[lo] = tiles[:, :length].astype(BF16)
        ad[lo + 1] = tiles[:, length:].astype(BF16)
        publish(g)

    def multiply_near(d):
        x_pass(d).wait_recv()
        put(2 * d - 1, two(states_ref, x_in, 2 * (d - 1)))
        c_pass(d).wait_recv()
        put(2 * d, two(cot_ref, c_in, 2 * (d - 1)))

    def multiply_far():
        far_pass().wait_recv()

        @pl.when(low_chip)
        def _():
            put(ring - 1, two(cot_ref, d_in, 0))

        @pl.when(chip >= far)
        def _():
            put(ring - 1, two(states_ref, d_in, 0))

    def multiply_own():
        ad[0] = dot(states_ref[...], states_ref[...], NT).astype(BF16)
        ad[1] = dot(cot_ref[...], cot_ref[...], NT).astype(BF16)

    def multiply_beside():
        beside_copy(states_ref).wait_recv()

        @pl.when(core == 0)
        def _():
            ad[2] = dot(states_ref[...], b_in[...], NT).astype(BF16)

        @pl.when(core == 1)
        def _():
            ad[2] = dot(cot_ref[...], b_in[...], NT).astype(BF16)

        publish(0)

    lane = lax.broadcasted_iota(jnp.int32, (length, LANES), 1)
    low = lane < HEAD_DIM
    first = lane % HEAD_DIM < HEAD_DIM // 2
    cos, sin = cos_ref[...], sin_ref[...]
    causal = lax.broadcasted_iota(jnp.int32, (length, length), 0) >= lax.broadcasted_iota(
        jnp.int32, (length, length), 1
    )

    def swap(v):
        return pltpu.roll(v, HEAD_DIM, 1)

    def rope(v):
        turned = jnp.where(
            first, pltpu.roll(v, LANES - HEAD_DIM // 2, 1), pltpu.roll(v, HEAD_DIM // 2, 1)
        )
        return v * cos + turned * sin

    def halves(v):
        other = swap(v)
        zero = jnp.zeros_like(v)
        return (
            (jnp.where(low, v, zero).astype(BF16), jnp.where(low, zero, other).astype(BF16)),
            (jnp.where(low, other, zero).astype(BF16), jnp.where(low, zero, v).astype(BF16)),
        )

    blocks = [
        (b, g, (b * 2 + g) * (GROUP // 2) + pair)
        for b in range(kv_cols // LANES)
        for g in range(2)
        for pair in range(GROUP // 2)
    ]

    def attend():
        for b, g, at in blocks:
            kcut, cut = slice(b * LANES, (b + 1) * LANES), slice(at * LANES, (at + 1) * LANES)
            keys = halves(rope(k_acc[:, kcut]))
            values = halves(v_acc[:, kcut])
            q = rope(q_acc[:, cut]).astype(BF16)
            att = None
            for side in range(2):
                s = dot(q, keys[g][side], NT) * HEAD_DIM ** (-0.5)
                s = jnp.where(causal, s, -jnp.inf)
                e = jnp.exp(s - jnp.max(s, axis=1, keepdims=True))
                p = (e / jnp.sum(e, axis=1, keepdims=True)).astype(BF16)
                probs[2 * at + side] = p
                a = dot(p, values[g][side])
                att = a if att is None else att + a
            att_own[:, cut] = att.astype(BF16)

    def grad_values():
        sums = {}
        for b, g, at in blocks:
            ga = g_acc[:, at * LANES : (at + 1) * LANES].astype(BF16)
            for side in range(2):
                u = dot(probs[2 * at + side], ga, TN)
                key = (b, g, side)
                sums[key] = sums[key] + u if key in sums else u
        for b in range(kv_cols // LANES):
            grad = jnp.where(
                low,
                sums[b, 0, 0] + swap(sums[b, 0, 1]),
                swap(sums[b, 1, 0]) + sums[b, 1, 1],
            )
            gv_own[:, b * LANES : (b + 1) * LANES] = grad.astype(BF16)

    def a_copy(d):
        return remote(
            att_own, a_in.at[2 * (d - 1)], a_snd.at[d - 1], a_rcv.at[d - 1],
            {"seq": device(d, core)},
        )

    def a_far():
        return remote(
            att_own, ad_in.at[0], a_snd.at[far - 1], a_rcv.at[far - 1],
            {"seq": device(far, core)},
        )

    def a_beside():
        return remote(att_own, ab_in, b_snd.at[1], b_rcv.at[1], {"seq": partner})

    def a_pass(d):
        return remote(
            a_in.at[2 * (d - 1)], a_in.at[2 * (d - 1) + 1], af_snd.at[d - 1],
            af_rcv.at[d - 1], {"seq": partner},
        )

    def a_far_pass():
        return remote(
            ad_in.at[0], ad_in.at[1], af_snd.at[far - 1], af_rcv.at[far - 1], {"seq": partner}
        )

    def send_attended():
        each(1, far, lambda d: a_copy(d).start())
        pl.when(chip >= far)(lambda: a_far().start())
        pl.when(core == 0)(lambda: a_beside().start())

    def pass_attended():
        def one(d):
            a_copy(d).wait_recv()
            a_pass(d).start()

        each(1, far, one)

        @pl.when(low_chip)
        def _():
            a_far().wait_recv()
            a_far_pass().start()

    def g_copy(d, other):
        return remote(
            gv_own, g_in.at[2 * (d - 1) + other], g_snd.at[other, d - 1],
            g_rcv.at[other, d - 1], {"seq": device(-d, (core + other) % 2)},
        )

    def g_far(other):
        return remote(
            gv_own, gd_in.at[other], g_snd.at[other, far - 1], g_rcv.at[other, far - 1],
            {"seq": device(far, (core + other) % 2)},
        )

    def g_beside():
        return remote(gv_own, gb_in, b_snd.at[2], b_rcv.at[2], {"seq": partner})

    def send_grads():
        @pl.when(low_chip)
        def _():
            for other in range(2):
                g_far(other).start()

        def one(d):
            for other in range(2):
                g_copy(d, other).start()

        each(1, far, one)
        pl.when(core == 1)(lambda: g_beside().start())

    lane_at = lax.broadcasted_iota(jnp.int32, (1, lanes), 1)

    def weigh(tile, b):
        product = full[tile].astype(F32) * b
        return jnp.sum(jnp.sum(product, axis=0, keepdims=True), axis=1, keepdims=True)

    def note(source, value):
        t2[col, me] += jnp.where(lane_at == source, value, 0.0)

    def score_two(g, hop, own, buf, at):
        b = two(own, buf, at)
        for other in range(2):
            note(
                device(hop, (core + other) % 2),
                weigh(2 * g + 1 + other, b[:, other * length : (other + 1) * length]),
            )

    def score_attended(d):
        a_pass(d).wait_recv()
        score_two(2 * d, -d, att_own, a_in, 2 * (d - 1))

    def score_grads(d):
        for other in range(2):
            g_copy(d, other).wait_recv()
        score_two(2 * d - 1, d, gv_own, g_in, 2 * (d - 1))

    multiply_own()
    project_states(0)
    relay(0, 1)
    follow(1)
    multiply_beside()
    settle(0, 1)
    arrivals(1, project_states)
    each(1, far, pass_near)
    if tp > 2:
        relay(0, 2)
        follow(2)
    relay(1, 1)
    each(1, far, multiply_near)
    for k in range(2, tp):
        settle(0, k)
        arrivals(k, project_states)
        if k + 1 < tp:
            relay(0, k + 1)
            follow(k + 1)
    project_cot(0)
    pass_far()
    attend()
    send_attended()
    multiply_far()
    settle(1, 1)
    arrivals(1, project_cot)
    each(0, min(ring, 2), chain)
    for k in range(2, tp):
        relay(1, k)
    each(min(ring, 2), ring, chain)
    for k in range(2, tp):
        settle(1, k)
        arrivals(k, project_cot)
        if k == 2:
            each(0, min(ring, 2), total)
    if tp <= 2:
        each(0, min(ring, 2), total)
    grad_values()
    send_grads()
    pass_attended()
    each(min(ring, 2), ring, total)
    totals_here(0)
    each(1, ring, totals_here)

    t2[col, me] = jnp.zeros((1, lanes), F32)
    note(me, weigh(1, dot(att_own[...], att_own[...], NT)))
    note(me, weigh(0, dot(gv_own[...], gv_own[...], NT)))

    @pl.when(core == 1)
    def _():
        a_beside().wait_recv()
        note(partner, weigh(2, dot(att_own[...], ab_in[...], NT)))

    @pl.when(core == 0)
    def _():
        g_beside().wait_recv()
        note(partner, weigh(2, dot(gv_own[...], gb_in[...], NT)))

    each(1, far, score_attended)

    @pl.when(low_chip)
    def _():
        a_far_pass().wait_recv()
        score_two(ring - 1, far, att_own, ad_in, 0)

    each(1, far, score_grads)

    @pl.when(chip >= far)
    def _():
        for other in range(2):
            g_far(other).wait_recv()
        score_two(ring - 1, far, gv_own, gd_in, 0)

    def r2_copy(o):
        mine = t2.at[col, me]
        to = {"seq": (me + o) % n, "tp": (col + o // n) % tp}
        return remote(mine, mine, r2_snd.at[o - 1], r2_rcv.at[o - 1], to)

    def every(act):
        if n * tp <= 32:
            for o in range(1, n * tp):
                act(r2_copy(o))
        else:
            each(1, n * tp, lambda o: act(r2_copy(o)))

    every(lambda c: c.start())
    every(lambda c: c.wait_recv())

    table = t2[0].reshape(n, lanes)
    for q in range(1, tp):
        table = table + t2[q].reshape(n, lanes)
    rank = lax.broadcasted_iota(jnp.int32, (n, lanes), 0)
    spot = lax.broadcasted_iota(jnp.int32, (n, lanes), 1)
    eye = rank == spot
    column = jnp.sum(jnp.where(spot == me, table, 0.0), axis=1, keepdims=True)
    theirs = eye & (rank != me)
    mirrored = jnp.sum(jnp.where(theirs, column, 0.0), axis=0, keepdims=True)
    own = jnp.sum(jnp.where(rank == me, table, 0.0), axis=0, keepdims=True)
    diag = jnp.sum(jnp.where(eye, table, 0.0), axis=0, keepdims=True)
    own_diag = jnp.sum(jnp.where(lane_at == me, diag, 0.0), axis=1, keepdims=True)
    gram = (own + mirrored) / jnp.sqrt(own_diag * diag)
    out_ref[...] = gram[:, :n]

    for k in range(1, tp):
        for which in range(2):
            for h in range(HALVES):
                pl.when(sends_up(k))(lambda: up(which, k, h).wait_send())
                pl.when(sends_down(k))(lambda: down(which, k, h).wait_send())

    def drain_near(d):
        for c in (x_copy(d), c_copy(d), x_pass(d), c_pass(d), a_copy(d), a_pass(d)):
            c.wait_send()
        for other in range(2):
            g_copy(d, other).wait_send()

    each(1, far, drain_near)
    far_copy(states_ref).wait_send()
    far_pass().wait_send()
    beside_copy(states_ref).wait_send()
    pl.when(chip >= far)(lambda: a_far().wait_send())
    pl.when(core == 0)(lambda: a_beside().wait_send())
    pl.when(core == 1)(lambda: g_beside().wait_send())

    @pl.when(low_chip)
    def _():
        a_far_pass().wait_send()
        for other in range(2):
            g_far(other).wait_send()

    def drain_sums(g):
        inner(g, lambda c: c.wait_send())
        outer(g, lambda c: c.wait_send())

    drain_sums(0)
    each(1, ring, drain_sums)
    every(lambda c: c.wait_send())


def on_device(n, tp, states, cotangent, wq, wk, wv, wo):
    seq_dev, length, width = states.shape
    assert seq_dev == 1 and n % 4 == 0 and length == LANES and tp > 1
    kv = wk.shape[1]
    ring = n // 2
    far = ring // 2
    near = max(far - 1, 1)
    tiles = 2 * ring + 1
    lanes = -(-n // LANES) * LANES
    cos, sin = rope_tables(length)
    vmem = pl.BlockSpec(memory_space=pltpu.VMEM)
    hbm = pl.BlockSpec(memory_space=pl.ANY)
    sem = pltpu.SemaphoreType.DMA

    def half(*shape):
        return pltpu.VMEM(shape, BF16)

    def wide(*shape):
        return pltpu.VMEM(shape, F32)

    return pl.pallas_call(
        functools.partial(kernel, n, tp),
        out_shape=jax.ShapeDtypeStruct((1, n), F32),
        in_specs=[vmem] * 4 + [hbm] * 4,
        out_specs=vmem,
        scratch_shapes=[
            half(tp - 1, length, width),
            half(tp - 1, length, width),
            half(tp, width, wq.shape[1]),
            half(tp, width, kv),
            half(tp, width, kv),
            half(tp, wo.shape[0], width),
            wide(length, wq.shape[1]),
            wide(length, kv),
            wide(length, kv),
            wide(length, wo.shape[0]),
            half(2 * near, length, width),
            half(2 * near, length, width),
            half(2, length, width),
            half(length, width),
            half(length, width),
            half(2 * near, length, width),
            half(2, length, width),
            half(length, width),
            half(length, kv),
            half(2 * near, length, kv),
            half(2, length, kv),
            half(length, kv),
            half(width // HEAD_DIM, length, length),
            half(tiles, length, length),
            half(tiles, length, length),
            half(tiles, length, length),
            half(tiles, length, length),
            wide(tp, n, 1, lanes),
            sem((4 * tp,)),
            sem((2, 2, tp - 1, HALVES)),
            sem((2, tp - 1, HALVES)),
            sem((3, far)),
            sem((3, far)),
            sem((3, far)),
            sem((3, far)),
            sem((3,)),
            sem((3,)),
            sem((far,)),
            sem((far,)),
            sem((far,)),
            sem((far,)),
            sem((2, far)),
            sem((2, far)),
            sem((ring,)),
            sem((ring,)),
            sem((ring,)),
            sem((ring,)),
            sem((ring,)),
            sem((n * tp - 1,)),
            sem((n * tp - 1,)),
        ],
        compiler_params=pltpu.CompilerParams(
            collective_id=0, has_side_effects=True, vmem_limit_bytes=60 * 1024 * 1024
        ),
        name="ntk_gram",
    )(
        states.reshape(length, width), cotangent.reshape(length, width),
        jnp.asarray(cos), jnp.asarray(sin), wq, wk, wv, wo,
    )


def solution(mesh):
    in_specs = (
        P("seq", None, "tp"),
        P("seq", None, "tp"),
        P(None, "tp"),
        P(None, "tp"),
        P(None, "tp"),
        P("tp", None),
    )
    return jax.shard_map(
        functools.partial(on_device, mesh.shape["seq"], mesh.shape["tp"]),
        mesh=mesh, in_specs=in_specs, out_specs=P("seq", None), check_vma=False,
    )
```

```python
import functools

import jax
import jax.numpy as jnp
import numpy as np
from jax import lax
from jax.experimental import pallas as pl
from jax.experimental.pallas import tpu as pltpu
from jax.sharding import PartitionSpec as P

HEADS = 32
KV_HEADS = 8
HEAD_DIM = 64
THETA = 500000.0
LANES = 128
HALVES = 2
GROUP = HEADS // KV_HEADS
F32, BF16 = jnp.float32, jnp.bfloat16

NT = (((1,), (1,)), ((), ()))
TN = (((0,), (0,)), ((), ()))


def rope_tables(length):
    half = HEAD_DIM // 2
    freqs = np.float32(THETA) ** (-(np.arange(half, dtype=np.float32) * np.float32(2.0 / HEAD_DIM)))
    angles = np.arange(length, dtype=np.float32)[:, None] * freqs[None, :].astype(np.float32)
    cos, sin = np.cos(angles), np.sin(angles)
    return (
        np.concatenate([cos, cos] * 2, axis=1).astype(np.float32),
        np.concatenate([-sin, sin] * 2, axis=1).astype(np.float32),
    )


def dot(a, b, dims=None):
    if dims is None:
        return jnp.dot(a, b, preferred_element_type=F32)
    return lax.dot_general(a, b, dims, preferred_element_type=F32)


def place_of(index, n):
    if n % 8:
        return index
    block, rest = index // 8, index % 8
    row, col, core = rest // 4, (rest // 2) % 2, rest % 2
    return block * 8 + 2 * (2 * row + (row + col) % 2) + core


def index_at(place, n):
    if n % 8:
        return place
    block, rest = place // 8, place % 8
    spot, core = rest // 2, rest % 2
    row = spot // 2
    return block * 8 + 2 * (2 * row + (row + spot) % 2) + core


def kernel(
    n, tp,
    states_hbm, cot_hbm, cos_hbm, sin_hbm, wq_hbm, wk_hbm, wv_hbm, wo_hbm,
    out_ref,
    states_ref, cot_ref, cos_ref, sin_ref, xs, cs, wqb, wkb, wvb, wob, q_acc, k_acc, v_acc, g_acc,
    x_in, c_in, d_in, b_in, att_own, a_in, ad_in, ab_in, gv_own, g_in, gd_in, gb_in,
    probs, ad, rin, xin, full, near, sums, t2,
    in_sem, w_sem, z_snd, z_rcv, p_snd, p_rcv, f_snd, f_rcv, b_snd, b_rcv,
    a_snd, a_rcv, af_snd, af_rcv, g_snd, g_rcv,
    i_snd, r_rcv, s_rcv, o_snd, o_rcv, r2_snd, r2_rcv,
):
    length, width = states_ref.shape
    kv_cols = k_acc.shape[1]
    ring = n // 2
    far = ring // 2
    mid = tp // 2
    hrows = length // HALVES
    lanes = t2.shape[2]
    me = lax.axis_index("seq")
    col = lax.axis_index("tp")
    place = place_of(me, n)
    chip, core = place // 2, place % 2
    low_chip = chip < far
    last = tp - 1

    def device(hop, c):
        return index_at(2 * ((chip + hop + ring) % ring) + c, n)

    partner = device(0, 1 - core)

    def each(lo, hi, body):
        if hi - lo <= 8:
            for i in range(lo, hi):
                body(i)
        else:
            lax.fori_loop(lo, hi, lambda i, c: (body(i), c)[1], 0)

    def remote(src, dst, snd, rcv, to):
        return pltpu.make_async_remote_copy(
            src_ref=src, dst_ref=dst, send_sem=snd, recv_sem=rcv, device_id=to
        )

    input_copies = [
        pltpu.make_async_copy(src, dst, in_sem.at[i])
        for i, (src, dst) in enumerate((
            (states_hbm, states_ref), (cot_hbm, cot_ref),
            (cos_hbm, cos_ref), (sin_hbm, sin_ref),
        ))
    ]
    weight_copies = []
    for k in range(tp):
        at = pl.ds(pl.multiple_of(((col - k + tp) % tp) * width, width), width)
        weight_copies.append([
            pltpu.make_async_copy(wq_hbm.at[at, :], wqb.at[k], w_sem.at[4 * k]),
            pltpu.make_async_copy(wk_hbm.at[at, :], wkb.at[k], w_sem.at[4 * k + 1]),
            pltpu.make_async_copy(wv_hbm.at[at, :], wvb.at[k], w_sem.at[4 * k + 2]),
            pltpu.make_async_copy(wo_hbm.at[:, at], wob.at[k], w_sem.at[4 * k + 3]),
        ])

    barrier = pltpu.get_barrier_semaphore()
    pl.when(col > 0)(
        lambda: pl.semaphore_signal(barrier, inc=1, device_id={"tp": col - 1})
    )
    pl.when(col < last)(
        lambda: pl.semaphore_signal(barrier, inc=1, device_id={"tp": col + 1})
    )
    each(1, n, lambda o: pl.semaphore_signal(barrier, inc=1, device_id={"seq": (me + o) % n}))
    for c in input_copies:
        c.start()
    order = [0] + [s for k in range(1, tp) for s in dict.fromkeys((k, tp - k)) if k <= tp - k]
    for part in (slice(0, 3), slice(3, 4)):
        for k in order:
            for c in weight_copies[k][part]:
                c.start()
    for c in input_copies[:2]:
        c.wait()
    ends = (col == 0).astype(jnp.int32) + (col == last).astype(jnp.int32)
    pl.semaphore_wait(barrier, n + 1 - ends)

    inputs = (states_ref, cot_ref)
    held = (xs, cs)

    def rows_of(h):
        return pl.ds(h * hrows, hrows)

    def up(which, k, h):
        src = inputs[which] if k == 1 else held[which].at[k - 2]
        return remote(
            src.at[rows_of(h), :], held[which].at[k - 1, rows_of(h), :],
            z_snd.at[which, 0, k - 1, h], z_rcv.at[which, k - 1, h], {"tp": (col + 1) % tp},
        )

    def down(which, k, h):
        src = inputs[which] if k == 1 else held[which].at[tp - k]
        return remote(
            src.at[rows_of(h), :], held[which].at[tp - k - 1, rows_of(h), :],
            z_snd.at[which, 1, k - 1, h], z_rcv.at[which, tp - k - 1, h],
            {"tp": (col + tp - 1) % tp},
        )

    def sends_up(k):
        return (col >= k - 1) & (col < last)

    def sends_down(k):
        return (col + k - 1 < tp) & (col > 0)

    def landed(which, slot, h):
        remote(
            inputs[which].at[rows_of(h), :], held[which].at[slot - 1, rows_of(h), :],
            z_snd.at[which, 0, 0, h], z_rcv.at[which, slot - 1, h], {"tp": (col + 1) % tp},
        ).wait_recv()

    def begin_up(which):
        for h in range(HALVES):
            up(which, 1, h).start()

    def begin_down(which):
        for h in range(HALVES):
            down(which, 1, h).start()

    def relay(which, k):
        for h in range(HALVES):
            @pl.when((col >= k) & (col < last))
            def _():
                landed(which, k, h)
                up(which, k + 1, h).start()

            @pl.when((col + k < tp) & (col > 0))
            def _():
                landed(which, tp - k, h)
                down(which, k + 1, h).start()

    def settle(which, k):
        for h in range(HALVES):
            pl.when((col >= k) & (col == last))(lambda: landed(which, k, h))
            pl.when((col + k < tp) & (col == 0))(lambda: landed(which, tp - k, h))

    def arrivals(k, body):
        pl.when(col >= k)(lambda: body(k))
        pl.when(col + k < tp)(lambda: body(tp - k))

    def follow(k):
        pl.when((col == k) & (col < last))(lambda: begin_up(1))
        pl.when((last - col == k) & (col > 0))(lambda: begin_down(1))

    pl.when(col < last)(lambda: begin_up(0))
    pl.when(col > 0)(lambda: begin_down(0))
    follow(0)

    def x_copy(d):
        return remote(
            states_ref, x_in.at[2 * (d - 1)], p_snd.at[0, d - 1], p_rcv.at[0, d - 1],
            {"seq": device(-d, core)},
        )

    def c_copy(d):
        return remote(
            cot_ref, c_in.at[2 * (d - 1)], p_snd.at[1, d - 1], p_rcv.at[1, d - 1],
            {"seq": device(d, core)},
        )

    def far_copy(src):
        return remote(
            src, d_in.at[0], p_snd.at[2, 0], p_rcv.at[2, 0], {"seq": device(far, core)}
        )

    def x_pass(d):
        return remote(
            x_in.at[2 * (d - 1)], x_in.at[2 * (d - 1) + 1], f_snd.at[0, d - 1],
            f_rcv.at[0, d - 1], {"seq": partner},
        )

    def c_pass(d):
        return remote(
            c_in.at[2 * (d - 1)], c_in.at[2 * (d - 1) + 1], f_snd.at[1, d - 1],
            f_rcv.at[1, d - 1], {"seq": partner},
        )

    def far_pass():
        return remote(
            d_in.at[0], d_in.at[1], f_snd.at[2, 0], f_rcv.at[2, 0], {"seq": partner}
        )

    def start_near(d):
        x_copy(d).start()
        c_copy(d).start()

    each(1, far, start_near)
    pl.when(low_chip)(lambda: far_copy(states_ref).start())
    pl.when(chip >= far)(lambda: far_copy(cot_ref).start())

    def pass_near(d):
        x_copy(d).wait_recv()
        x_pass(d).start()
        c_copy(d).wait_recv()
        c_pass(d).start()

    def pass_far():
        far_copy(states_ref).wait_recv()
        far_pass().start()

    def own_block(which, slot):
        return inputs[which] if slot == 0 else held[which].at[slot - 1]

    def beside(which, slot):
        return remote(
            own_block(which, slot), b_in.at[slot], b_snd.at[slot], b_rcv.at[slot],
            {"seq": partner},
        )

    def square(which, slot):
        x = own_block(which, slot)[...]
        piece = dot(x, x, NT)
        near[which] = piece if slot == 0 else near[which] + piece
        pl.when(core == 1 - which)(lambda: beside(which, slot).start())

    def multiply_beside(which):
        @pl.when(core == which)
        def _():
            acc = None
            for slot in range(tp):
                beside(which, slot).wait_recv()
                piece = dot(own_block(which, slot)[...], b_in[slot], NT)
                acc = piece if acc is None else acc + piece
            near[2] = acc

    def project_states(slot):
        for c in weight_copies[slot][:3]:
            c.wait()
        square(0, slot)
        x = states_ref[...] if slot == 0 else xs[slot - 1]
        for acc, w in ((q_acc, wqb), (k_acc, wkb), (v_acc, wvb)):
            piece = dot(x, w[slot])
            acc[...] = piece if slot == 0 else acc[...] + piece

    def project_cot(slot):
        weight_copies[slot][3].wait()
        square(1, slot)
        y = cot_ref[...] if slot == 0 else cs[slot - 1]
        piece = dot(y, wob[slot], NT)
        g_acc[...] = piece if slot == 0 else g_acc[...] + piece

    def inner(g, act):
        part = pl.ds(2 * g, 2)

        def copy(dst, rcv, to):
            return remote(ad.at[part], dst.at[part], i_snd.at[g], rcv.at[g], {"tp": to})

        pl.when(col < mid - 1)(lambda: act(copy(rin, r_rcv, (col + 1) % tp)))
        pl.when(col > mid)(lambda: act(copy(rin, r_rcv, (col + tp - 1) % tp)))
        pl.when(col == mid - 1)(lambda: act(copy(xin, s_rcv, (col + 1) % tp)))
        pl.when(col == mid)(lambda: act(copy(xin, s_rcv, (col + tp - 1) % tp)))

    def outer(g, act):
        part = pl.ds(2 * g, 2)

        def copy(to):
            return remote(full.at[part], full.at[part], o_snd.at[g], o_rcv.at[g], {"tp": to})

        pl.when((col < mid) & (col > 0))(lambda: act(copy((col + tp - 1) % tp)))
        pl.when((col >= mid) & (col < last))(lambda: act(copy((col + 1) % tp)))

    def waits_on(buf, rcv, g):
        part = pl.ds(2 * g, 2)
        remote(
            buf.at[part], buf.at[part], o_snd.at[g], rcv.at[g], {"tp": (col + 1) % tp}
        ).wait_recv()

    edge = (col == 0) | (col == last)
    central = (col == mid - 1) | (col == mid)

    def publish(g):
        pl.when(edge)(lambda: inner(g, lambda c: c.start()))

    def chain(g):
        part = pl.ds(2 * g, 2)

        @pl.when(jnp.logical_not(edge))
        def _():
            waits_on(rin, r_rcv, g)
            ad[part] = (ad[part].astype(F32) + rin[part].astype(F32)).astype(BF16)
            inner(g, lambda c: c.start())

    def total(g):
        part = pl.ds(2 * g, 2)

        @pl.when(central)
        def _():
            waits_on(xin, s_rcv, g)
            full[part] = (ad[part].astype(F32) + xin[part].astype(F32)).astype(BF16)
            outer(g, lambda c: c.start())

    def totals_here(g):
        @pl.when(jnp.logical_not(central))
        def _():
            waits_on(full, o_rcv, g)
            pl.when(jnp.logical_not(edge))(lambda: outer(g, lambda c: c.start()))

    def two(own, buf, at):
        both = buf[pl.ds(at, 2)].reshape(2 * length, buf.shape[2])
        return dot(own[...], both, NT)

    def put(g, tiles):
        ad[2 * g] = tiles[:, :length].astype(BF16)
        ad[2 * g + 1] = tiles[:, length:].astype(BF16)
        publish(g)

    def multiply_near(d):
        x_pass(d).wait_recv()
        put(2 * d - 2, two(states_ref, x_in, 2 * (d - 1)))
        c_pass(d).wait_recv()
        put(2 * d - 1, two(cot_ref, c_in, 2 * (d - 1)))

    def multiply_far():
        far_pass().wait_recv()

        @pl.when(low_chip)
        def _():
            put(ring - 2, two(cot_ref, d_in, 0))

        @pl.when(chip >= far)
        def _():
            put(ring - 2, two(states_ref, d_in, 0))

    lane = lax.broadcasted_iota(jnp.int32, (length, LANES), 1)
    low = lane < HEAD_DIM
    first = lane % HEAD_DIM < HEAD_DIM // 2
    for c in input_copies[2:]:
        c.wait()
    cos, sin = cos_ref[...], sin_ref[...]
    causal = lax.broadcasted_iota(jnp.int32, (length, length), 0) >= lax.broadcasted_iota(
        jnp.int32, (length, length), 1
    )

    def swap(v):
        return pltpu.roll(v, HEAD_DIM, 1)

    def rope(v):
        turned = jnp.where(
            first, pltpu.roll(v, LANES - HEAD_DIM // 2, 1), pltpu.roll(v, HEAD_DIM // 2, 1)
        )
        return v * cos + turned * sin

    def halves(v):
        other = swap(v)
        zero = jnp.zeros_like(v)
        return (
            (jnp.where(low, v, zero).astype(BF16), jnp.where(low, zero, other).astype(BF16)),
            (jnp.where(low, other, zero).astype(BF16), jnp.where(low, zero, v).astype(BF16)),
        )

    blocks = [
        (b, g, (b * 2 + g) * (GROUP // 2) + pair)
        for b in range(kv_cols // LANES)
        for g in range(2)
        for pair in range(GROUP // 2)
    ]

    def attend():
        for b, g, at in blocks:
            kcut, cut = slice(b * LANES, (b + 1) * LANES), slice(at * LANES, (at + 1) * LANES)
            keys = halves(rope(k_acc[:, kcut]))
            values = halves(v_acc[:, kcut])
            q = rope(q_acc[:, cut]).astype(BF16)
            att = None
            for side in range(2):
                s = dot(q, keys[g][side], NT) * HEAD_DIM ** (-0.5)
                s = jnp.where(causal, s, -jnp.inf)
                e = jnp.exp(s - jnp.max(s, axis=1, keepdims=True))
                p = (e / jnp.sum(e, axis=1, keepdims=True)).astype(BF16)
                probs[2 * at + side] = p
                a = dot(p, values[g][side])
                att = a if att is None else att + a
            att_own[:, cut] = att.astype(BF16)

    def grad_values():
        sums = {}
        for b, g, at in blocks:
            ga = g_acc[:, at * LANES : (at + 1) * LANES].astype(BF16)
            for side in range(2):
                u = dot(probs[2 * at + side], ga, TN)
                key = (b, g, side)
                sums[key] = sums[key] + u if key in sums else u
        for b in range(kv_cols // LANES):
            grad = jnp.where(
                low,
                sums[b, 0, 0] + swap(sums[b, 0, 1]),
                swap(sums[b, 1, 0]) + sums[b, 1, 1],
            )
            gv_own[:, b * LANES : (b + 1) * LANES] = grad.astype(BF16)

    def a_copy(d):
        return remote(
            att_own, a_in.at[2 * (d - 1)], a_snd.at[d - 1], a_rcv.at[d - 1],
            {"seq": device(d, core)},
        )

    def a_far():
        return remote(
            att_own, ad_in.at[0], a_snd.at[far - 1], a_rcv.at[far - 1],
            {"seq": device(far, core)},
        )

    def a_beside():
        return remote(att_own, ab_in, b_snd.at[tp], b_rcv.at[tp], {"seq": partner})

    def a_pass(d):
        return remote(
            a_in.at[2 * (d - 1)], a_in.at[2 * (d - 1) + 1], af_snd.at[d - 1],
            af_rcv.at[d - 1], {"seq": partner},
        )

    def a_far_pass():
        return remote(
            ad_in.at[0], ad_in.at[1], af_snd.at[far - 1], af_rcv.at[far - 1], {"seq": partner}
        )

    def send_attended():
        each(1, far, lambda d: a_copy(d).start())
        pl.when(chip >= far)(lambda: a_far().start())
        pl.when(core == 0)(lambda: a_beside().start())

    def pass_attended():
        def one(d):
            a_copy(d).wait_recv()
            a_pass(d).start()

        each(1, far, one)

        @pl.when(low_chip)
        def _():
            a_far().wait_recv()
            a_far_pass().start()

    def g_copy(d, other):
        return remote(
            gv_own, g_in.at[2 * (d - 1) + other], g_snd.at[other, d - 1],
            g_rcv.at[other, d - 1], {"seq": device(-d, (core + other) % 2)},
        )

    def g_far(other):
        return remote(
            gv_own, gd_in.at[other], g_snd.at[other, far - 1], g_rcv.at[other, far - 1],
            {"seq": device(far, (core + other) % 2)},
        )

    def g_beside():
        return remote(gv_own, gb_in, b_snd.at[tp + 1], b_rcv.at[tp + 1], {"seq": partner})

    def send_grads():
        @pl.when(low_chip)
        def _():
            for other in range(2):
                g_far(other).start()

        def one(d):
            for other in range(2):
                g_copy(d, other).start()

        each(1, far, one)
        pl.when(core == 1)(lambda: g_beside().start())

    lane_at = lax.broadcasted_iota(jnp.int32, (1, lanes), 1)

    def weigh(source, d, b):
        at = pl.ds(source, 1)
        sums[at, :] = sums[at, :] + jnp.sum(d * b, axis=0, keepdims=True)

    def score_two(g, hop, own, buf, at):
        b = two(own, buf, at)
        for other in range(2):
            weigh(
                device(hop, (core + other) % 2), full[2 * g + other].astype(F32),
                b[:, other * length : (other + 1) * length],
            )

    def score_attended(d):
        a_pass(d).wait_recv()
        score_two(2 * d - 1, -d, att_own, a_in, 2 * (d - 1))

    def score_grads(d):
        for other in range(2):
            g_copy(d, other).wait_recv()
        score_two(2 * d - 2, d, gv_own, g_in, 2 * (d - 1))

    def near_totals(g):
        chain(g)
        total(g)

    project_states(0)
    relay(0, 1)
    follow(1)
    each(1, far, pass_near)
    settle(0, 1)
    arrivals(1, project_states)
    if tp > 2:
        relay(0, 2)
        follow(2)
    each(1, far, multiply_near)
    for k in range(3, tp):
        relay(0, k)
        follow(k)
    pass_far()
    project_cot(0)
    relay(1, 1)
    multiply_far()
    for k in range(2, tp):
        settle(0, k)
        arrivals(k, project_states)
    each(0, ring - 1, chain)
    attend()
    send_attended()
    settle(1, 1)
    arrivals(1, project_cot)
    for k in range(2, tp):
        relay(1, k)
    each(0, ring - 1, total)
    for k in range(2, tp):
        settle(1, k)
        arrivals(k, project_cot)
    grad_values()
    send_grads()
    multiply_beside(0)
    multiply_beside(1)
    pass_attended()
    sums[...] = jnp.zeros_like(sums)
    weigh(me, near[1], dot(att_own[...], att_own[...], NT))
    weigh(me, near[0], dot(gv_own[...], gv_own[...], NT))

    @pl.when(core == 1)
    def _():
        a_beside().wait_recv()
        weigh(partner, near[2], dot(att_own[...], ab_in[...], NT))

    @pl.when(core == 0)
    def _():
        g_beside().wait_recv()
        weigh(partner, near[2], dot(gv_own[...], gb_in[...], NT))

    each(0, ring - 1, totals_here)
    each(1, far, score_attended)

    @pl.when(low_chip)
    def _():
        a_far_pass().wait_recv()
        score_two(ring - 2, far, att_own, ad_in, 0)

    each(1, far, score_grads)

    @pl.when(chip >= far)
    def _():
        for other in range(2):
            g_far(other).wait_recv()
        score_two(ring - 2, far, gv_own, gd_in, 0)

    row_at = lax.broadcasted_iota(jnp.int32, (n, lanes), 0)
    spot_at = lax.broadcasted_iota(jnp.int32, (n, lanes), 1)
    pairs = jnp.sum(sums[...], axis=1, keepdims=True)[:n]
    t2[col * n + me] = jnp.sum(
        jnp.where(row_at == spot_at, pairs, 0.0), axis=0, keepdims=True
    )

    def r2_copy(o):
        mine = t2.at[col * n + me]
        to = {"seq": (me + o) % n, "tp": (col + o // n) % tp}
        return remote(mine, mine, r2_snd.at[0], r2_rcv.at[0], to)

    if n * tp <= 32:
        for o in range(n * tp - 1, 0, -1):
            r2_copy(o).start()
    else:
        each(1, n * tp, lambda o: r2_copy(o).start())

    for k in range(1, tp):
        for which in range(2):
            for h in range(HALVES):
                pl.when(sends_up(k))(lambda: up(which, k, h).wait_send())
                pl.when(sends_down(k))(lambda: down(which, k, h).wait_send())

    def drain_near(d):
        for c in (x_copy(d), c_copy(d), x_pass(d), c_pass(d), a_copy(d), a_pass(d)):
            c.wait_send()
        for other in range(2):
            g_copy(d, other).wait_send()

    each(1, far, drain_near)
    far_copy(states_ref).wait_send()
    far_pass().wait_send()
    for slot in range(tp):
        beside(0, slot).wait_send()
    pl.when(chip >= far)(lambda: a_far().wait_send())
    pl.when(core == 0)(lambda: a_beside().wait_send())
    pl.when(core == 1)(lambda: g_beside().wait_send())

    @pl.when(low_chip)
    def _():
        a_far_pass().wait_send()
        for other in range(2):
            g_far(other).wait_send()

    def drain_sums(g):
        inner(g, lambda c: c.wait_send())
        outer(g, lambda c: c.wait_send())

    each(0, ring - 1, drain_sums)
    others = t2.at[pl.ds(0, n * tp - 1)]
    everyone = remote(others, others, r2_snd.at[0], r2_rcv.at[0], {"seq": partner})
    everyone.wait_recv()
    table = t2[pl.ds(0, n)].reshape(n, lanes)
    for q in range(1, tp):
        table = table + t2[pl.ds(q * n, n)].reshape(n, lanes)
    rank, spot = row_at, spot_at
    eye = rank == spot
    column = jnp.sum(jnp.where(spot == me, table, 0.0), axis=1, keepdims=True)
    theirs = eye & (rank != me)
    mirrored = jnp.sum(jnp.where(theirs, column, 0.0), axis=0, keepdims=True)
    own = jnp.sum(jnp.where(rank == me, table, 0.0), axis=0, keepdims=True)
    diag = jnp.sum(jnp.where(eye, table, 0.0), axis=0, keepdims=True)
    own_diag = jnp.sum(jnp.where(lane_at == me, diag, 0.0), axis=1, keepdims=True)
    gram = (own + mirrored) / jnp.sqrt(own_diag * diag)
    out_ref[...] = gram[:, :n]
    everyone.wait_send()


def on_device(n, tp, states, cotangent, wq, wk, wv, wo):
    seq_dev, length, width = states.shape
    assert seq_dev == 1 and n % 4 == 0 and length == LANES and tp > 1
    kv = wk.shape[1]
    ring = n // 2
    far = ring // 2
    near = max(far - 1, 1)
    tiles = 2 * (ring - 1)
    lanes = -(-n // LANES) * LANES
    cos, sin = rope_tables(length)
    vmem = pl.BlockSpec(memory_space=pltpu.VMEM)
    hbm = pl.BlockSpec(memory_space=pl.ANY)
    sem = pltpu.SemaphoreType.DMA

    def half(*shape):
        return pltpu.VMEM(shape, BF16)

    def wide(*shape):
        return pltpu.VMEM(shape, F32)

    return pl.pallas_call(
        functools.partial(kernel, n, tp),
        out_shape=jax.ShapeDtypeStruct((1, n), F32),
        in_specs=[hbm] * 8,
        out_specs=vmem,
        scratch_shapes=[
            half(length, width),
            half(length, width),
            wide(length, LANES),
            wide(length, LANES),
            half(tp - 1, length, width),
            half(tp - 1, length, width),
            half(tp, width, wq.shape[1]),
            half(tp, width, kv),
            half(tp, width, kv),
            half(tp, wo.shape[0], width),
            wide(length, wq.shape[1]),
            wide(length, kv),
            wide(length, kv),
            wide(length, wo.shape[0]),
            half(2 * near, length, width),
            half(2 * near, length, width),
            half(2, length, width),
            half(tp, length, width),
            half(length, width),
            half(2 * near, length, width),
            half(2, length, width),
            half(length, width),
            half(length, kv),
            half(2 * near, length, kv),
            half(2, length, kv),
            half(length, kv),
            half(width // HEAD_DIM, length, length),
            half(tiles, length, length),
            half(tiles, length, length),
            half(tiles, length, length),
            half(tiles, length, length),
            wide(3, length, length),
            wide(-(-n // 8) * 8, LANES),
            wide(tp * n, 1, lanes),
            sem((4,)),
            sem((4 * tp,)),
            sem((2, 2, tp - 1, HALVES)),
            sem((2, tp - 1, HALVES)),
            sem((3, far)),
            sem((3, far)),
            sem((3, far)),
            sem((3, far)),
            sem((tp + 2,)),
            sem((tp + 2,)),
            sem((far,)),
            sem((far,)),
            sem((far,)),
            sem((far,)),
            sem((2, far)),
            sem((2, far)),
            sem((ring - 1,)),
            sem((ring - 1,)),
            sem((ring - 1,)),
            sem((ring - 1,)),
            sem((ring - 1,)),
            sem((1,)),
            sem((1,)),
        ],
        compiler_params=pltpu.CompilerParams(
            collective_id=0, has_side_effects=True, vmem_limit_bytes=60 * 1024 * 1024
        ),
        name="ntk_gram",
    )(
        states.reshape(length, width), cotangent.reshape(length, width),
        jnp.asarray(cos), jnp.asarray(sin), wq, wk, wv, wo,
    )


def solution(mesh):
    in_specs = (
        P("seq", None, "tp"),
        P("seq", None, "tp"),
        P(None, "tp"),
        P(None, "tp"),
        P(None, "tp"),
        P("tp", None),
    )
    return jax.shard_map(
        functools.partial(on_device, mesh.shape["seq"], mesh.shape["tp"]),
        mesh=mesh, in_specs=in_specs, out_specs=P("seq", None), check_vma=False,
    )
```

```python
import functools

import jax
import jax.numpy as jnp
import numpy as np
from jax import lax
from jax.experimental import pallas as pl
from jax.experimental.pallas import tpu as pltpu
from jax.sharding import PartitionSpec as P

HEADS = 32
KV_HEADS = 8
HEAD_DIM = 64
THETA = 500000.0
LANES = 128
HALVES = 2
GROUP = HEADS // KV_HEADS
F32, BF16 = jnp.float32, jnp.bfloat16

NT = (((1,), (1,)), ((), ()))
TN = (((0,), (0,)), ((), ()))


def rope_tables(length):
    half = HEAD_DIM // 2
    freqs = np.float32(THETA) ** (-(np.arange(half, dtype=np.float32) * np.float32(2.0 / HEAD_DIM)))
    angles = np.arange(length, dtype=np.float32)[:, None] * freqs[None, :].astype(np.float32)
    cos, sin = np.cos(angles), np.sin(angles)
    return (
        np.concatenate([cos, cos] * 2, axis=1).astype(np.float32),
        np.concatenate([-sin, sin] * 2, axis=1).astype(np.float32),
    )


def dot(a, b, dims=None):
    if dims is None:
        return jnp.dot(a, b, preferred_element_type=F32)
    return lax.dot_general(a, b, dims, preferred_element_type=F32)


def place_of(index, n):
    if n % 8:
        return index
    block, rest = index // 8, index % 8
    row, col, core = rest // 4, (rest // 2) % 2, rest % 2
    return block * 8 + 2 * (2 * row + (row + col) % 2) + core


def index_at(place, n):
    if n % 8:
        return place
    block, rest = place // 8, place % 8
    spot, core = rest // 2, rest % 2
    row = spot // 2
    return block * 8 + 2 * (2 * row + (row + spot) % 2) + core


def kernel(
    n, tp,
    states_hbm, cot_hbm, cos_hbm, sin_hbm, wq_hbm, wk_hbm, wv_hbm, wo_hbm,
    out_ref,
    states_ref, cot_ref, cos_ref, sin_ref, xs, cs, wqb, wkb, wvb, wob, q_acc, k_acc, v_acc, g_acc,
    x_in, c_in, d_in, b_in, att_own, a_in, ad_in, ab_in, gv_own, g_in, gd_in, gb_in,
    probs, ad, rin, xin, full, near, over, sums, t2,
    in_sem, clear_sem, w_sem, z_snd, z_rcv, p_snd, p_rcv, f_snd, f_rcv, b_snd, b_rcv,
    a_snd, a_rcv, af_snd, af_rcv, g_snd, g_rcv,
    i_snd, r_rcv, s_rcv, o_snd, o_rcv, r2_snd, r2_rcv,
):
    length, width = states_ref.shape
    kv_cols = k_acc.shape[1]
    ring = n // 2
    far = ring // 2
    mid = tp // 2
    hrows = length // HALVES
    lanes = t2.shape[2]
    me = lax.axis_index("seq")
    col = lax.axis_index("tp")
    place = place_of(me, n)
    chip, core = place // 2, place % 2
    low_chip = chip < far
    last = tp - 1

    def device(hop, c):
        return index_at(2 * ((chip + hop + ring) % ring) + c, n)

    partner = device(0, 1 - core)

    def each(lo, hi, body):
        if hi - lo <= 8:
            for i in range(lo, hi):
                body(i)
        else:
            lax.fori_loop(lo, hi, lambda i, c: (body(i), c)[1], 0)

    def remote(src, dst, snd, rcv, to):
        return pltpu.make_async_remote_copy(
            src_ref=src, dst_ref=dst, send_sem=snd, recv_sem=rcv, device_id=to
        )

    input_copies = [
        pltpu.make_async_copy(src, dst, in_sem.at[i])
        for i, (src, dst) in enumerate((
            (states_hbm, states_ref), (cot_hbm, cot_ref),
            (cos_hbm, cos_ref), (sin_hbm, sin_ref),
        ))
    ]
    weight_copies = []
    for k in range(tp):
        at = pl.ds(pl.multiple_of(((col - k + tp) % tp) * width, width), width)
        weight_copies.append([
            pltpu.make_async_copy(wq_hbm.at[at, :], wqb.at[k], w_sem.at[4 * k]),
            pltpu.make_async_copy(wk_hbm.at[at, :], wkb.at[k], w_sem.at[4 * k + 1]),
            pltpu.make_async_copy(wv_hbm.at[at, :], wvb.at[k], w_sem.at[4 * k + 2]),
            pltpu.make_async_copy(wo_hbm.at[:, at], wob.at[k], w_sem.at[4 * k + 3]),
        ])

    barrier = pltpu.get_barrier_semaphore()
    pl.when(col > 0)(
        lambda: pl.semaphore_signal(barrier, inc=1, device_id={"tp": col - 1})
    )
    pl.when(col < last)(
        lambda: pl.semaphore_signal(barrier, inc=1, device_id={"tp": col + 1})
    )
    each(1, n, lambda o: pl.semaphore_signal(barrier, inc=1, device_id={"seq": (me + o) % n}))
    for c in input_copies:
        c.start()
    for c in input_copies[:2]:
        c.wait()
    ends = (col == 0).astype(jnp.int32) + (col == last).astype(jnp.int32)
    pl.semaphore_wait(barrier, n + 1 - ends)

    inputs = (states_ref, cot_ref)
    held = (xs, cs)

    def rows_of(h):
        return pl.ds(h * hrows, hrows)

    def up(which, k, h):
        src = inputs[which] if k == 1 else held[which].at[k - 2]
        return remote(
            src.at[rows_of(h), :], held[which].at[k - 1, rows_of(h), :],
            z_snd.at[which, 0, k - 1, h], z_rcv.at[which, k - 1, h], {"tp": (col + 1) % tp},
        )

    def down(which, k, h):
        src = inputs[which] if k == 1 else held[which].at[tp - k]
        return remote(
            src.at[rows_of(h), :], held[which].at[tp - k - 1, rows_of(h), :],
            z_snd.at[which, 1, k - 1, h], z_rcv.at[which, tp - k - 1, h],
            {"tp": (col + tp - 1) % tp},
        )

    def sends_up(k):
        return (col >= k - 1) & (col < last)

    def sends_down(k):
        return (col + k - 1 < tp) & (col > 0)

    def landed(which, slot, h):
        remote(
            inputs[which].at[rows_of(h), :], held[which].at[slot - 1, rows_of(h), :],
            z_snd.at[which, 0, 0, h], z_rcv.at[which, slot - 1, h], {"tp": (col + 1) % tp},
        ).wait_recv()

    def begin_up(which):
        for h in range(HALVES):
            up(which, 1, h).start()

    def begin_down(which):
        for h in range(HALVES):
            down(which, 1, h).start()

    def relay_up(which, k, side):
        @pl.when((col >= k) & (col < last) & side)
        def _():
            for h in range(HALVES):
                landed(which, k, h)
                up(which, k + 1, h).start()

    def relay_down(which, k, side):
        @pl.when((col + k < tp) & (col > 0) & side)
        def _():
            for h in range(HALVES):
                landed(which, tp - k, h)
                down(which, k + 1, h).start()

    def relay(which, k):
        relay_up(which, k, col < mid)
        relay_down(which, k, col >= mid)
        relay_up(which, k, col >= mid)
        relay_down(which, k, col < mid)

    def settle(which, k):
        for h in range(HALVES):
            pl.when((col >= k) & (col == last))(lambda: landed(which, k, h))
            pl.when((col + k < tp) & (col == 0))(lambda: landed(which, tp - k, h))

    def arrivals(k, body):
        pl.when(col >= k)(lambda: body(k))
        pl.when(col + k < tp)(lambda: body(tp - k))

    def follow(k):
        pl.when((col == k) & (col < last))(lambda: begin_up(1))
        pl.when((jnp.minimum(last - col, 1) == k) & (col > 0))(lambda: begin_down(1))

    pl.when(col < last)(lambda: begin_up(0))
    pl.when(col > 0)(lambda: begin_down(0))
    follow(0)

    def x_copy(d):
        return remote(
            states_ref, x_in.at[2 * (d - 1)], p_snd.at[0, d - 1], p_rcv.at[0, d - 1],
            {"seq": device(-d, core)},
        )

    def c_copy(d):
        return remote(
            cot_ref, c_in.at[2 * (d - 1)], p_snd.at[1, d - 1], p_rcv.at[1, d - 1],
            {"seq": device(d, core)},
        )

    def far_copy(src):
        return remote(
            src, d_in.at[0], p_snd.at[2, 0], p_rcv.at[2, 0], {"seq": device(far, core)}
        )

    def x_pass(d):
        return remote(
            x_in.at[2 * (d - 1)], x_in.at[2 * (d - 1) + 1], f_snd.at[0, d - 1],
            f_rcv.at[0, d - 1], {"seq": partner},
        )

    def c_pass(d):
        return remote(
            c_in.at[2 * (d - 1)], c_in.at[2 * (d - 1) + 1], f_snd.at[1, d - 1],
            f_rcv.at[1, d - 1], {"seq": partner},
        )

    def far_pass():
        return remote(
            d_in.at[0], d_in.at[1], f_snd.at[2, 0], f_rcv.at[2, 0], {"seq": partner}
        )

    def start_near(d):
        x_copy(d).start()
        c_copy(d).start()

    each(1, far, start_near)
    pl.when(low_chip)(lambda: far_copy(states_ref).start())
    pl.when(chip >= far)(lambda: far_copy(cot_ref).start())
    order = [0] + [s for k in range(1, tp) for s in dict.fromkeys((k, tp - k)) if k <= tp - k]
    for part in (slice(0, 3), slice(3, 4)):
        for k in order:
            for c in weight_copies[k][part]:
                c.start()

    def pass_near(d):
        x_copy(d).wait_recv()
        x_pass(d).start()
        c_copy(d).wait_recv()
        c_pass(d).start()

    def pass_far():
        far_copy(states_ref).wait_recv()
        far_pass().start()

    def own_block(which, slot):
        return inputs[which] if slot == 0 else held[which].at[slot - 1]

    def beside(which, slot):
        return remote(
            own_block(which, slot), b_in.at[slot], b_snd.at[slot], b_rcv.at[slot],
            {"seq": partner},
        )

    def square(which, slots):
        acc = None
        for slot in slots:
            x = own_block(which, slot)[...]
            piece = dot(x, x, NT)
            acc = piece if acc is None else acc + piece
        near[which] = acc

    def hand_over(which, slot):
        pl.when(core == 1 - which)(lambda: beside(which, slot).start())

    def multiply_beside(which):
        @pl.when(core == which)
        def _():
            acc = None
            for slot in range(tp):
                beside(which, slot).wait_recv()
                piece = dot(own_block(which, slot)[...], b_in[slot], NT)
                acc = piece if acc is None else acc + piece
            near[2] = acc

    def project_states(slot):
        for c in weight_copies[slot][:3]:
            c.wait()
        hand_over(0, slot)
        x = states_ref[...] if slot == 0 else xs[slot - 1]
        for acc, w in ((q_acc, wqb), (k_acc, wkb), (v_acc, wvb)):
            piece = dot(x, w[slot])
            acc[...] = piece if slot == 0 else acc[...] + piece

    def project_cot(slot):
        weight_copies[slot][3].wait()
        hand_over(1, slot)
        y = cot_ref[...] if slot == 0 else cs[slot - 1]
        piece = dot(y, wob[slot], NT)
        g_acc[...] = piece if slot == 0 else g_acc[...] + piece

    def inner(g, act):
        part = pl.ds(2 * g, 2)

        def copy(dst, rcv, to):
            return remote(ad.at[part], dst.at[part], i_snd.at[g], rcv.at[g], {"tp": to})

        pl.when(col < mid - 1)(lambda: act(copy(rin, r_rcv, (col + 1) % tp)))
        pl.when(col > mid)(lambda: act(copy(rin, r_rcv, (col + tp - 1) % tp)))
        pl.when(col == mid - 1)(lambda: act(copy(xin, s_rcv, (col + 1) % tp)))
        pl.when(col == mid)(lambda: act(copy(xin, s_rcv, (col + tp - 1) % tp)))

    def outer(g, act):
        part = pl.ds(2 * g, 2)

        def copy(to):
            return remote(full.at[part], full.at[part], o_snd.at[g], o_rcv.at[g], {"tp": to})

        pl.when((col < mid) & (col > 0))(lambda: act(copy((col + tp - 1) % tp)))
        pl.when((col >= mid) & (col < last))(lambda: act(copy((col + 1) % tp)))

    def waits_on(buf, rcv, g):
        part = pl.ds(2 * g, 2)
        remote(
            buf.at[part], buf.at[part], o_snd.at[g], rcv.at[g], {"tp": (col + 1) % tp}
        ).wait_recv()

    edge = (col == 0) | (col == last)
    central = (col == mid - 1) | (col == mid)

    def publish(g):
        pl.when(edge)(lambda: inner(g, lambda c: c.start()))

    def chain(g):
        part = pl.ds(2 * g, 2)

        @pl.when(jnp.logical_not(edge))
        def _():
            waits_on(rin, r_rcv, g)
            ad[part] = (ad[part].astype(F32) + rin[part].astype(F32)).astype(BF16)
            inner(g, lambda c: c.start())

    def total(g):
        part = pl.ds(2 * g, 2)

        @pl.when(central)
        def _():
            waits_on(xin, s_rcv, g)
            full[part] = (ad[part].astype(F32) + xin[part].astype(F32)).astype(BF16)

    def last_relays():
        for h in range(HALVES):
            @pl.when((col >= mid) & (col < last))
            def _():
                remote(
                    held[1].at[col - 1, rows_of(h), :], held[1].at[col, rows_of(h), :],
                    z_snd.at[1, 0, col, h], z_rcv.at[1, col, h], {"tp": (col + 1) % tp},
                ).wait_send()

            @pl.when((col < mid) & (col > 0))
            def _():
                remote(
                    held[1].at[col, rows_of(h), :], held[1].at[col - 1, rows_of(h), :],
                    z_snd.at[1, 1, last - col, h], z_rcv.at[1, col - 1, h],
                    {"tp": (col + tp - 1) % tp},
                ).wait_send()

    def send_totals():
        inside = jnp.logical_not(edge)
        pl.when(inside & (core == 1))(lambda: pl.semaphore_wait(clear_sem, 1))
        pl.when(central)(lambda: each(0, ring - 1, lambda g: outer(g, lambda c: c.start())))

        @pl.when(inside & (core == 0))
        def _():
            last_relays()
            pl.semaphore_signal(clear_sem, inc=1, device_id={"seq": partner})

    def totals_here(g):
        @pl.when(jnp.logical_not(central))
        def _():
            waits_on(full, o_rcv, g)
            pl.when(jnp.logical_not(edge))(lambda: outer(g, lambda c: c.start()))

    def two(own, buf, at):
        both = buf[pl.ds(at, 2)].reshape(2 * length, buf.shape[2])
        return dot(own[...], both, NT)

    def put(g, tiles):
        ad[2 * g] = tiles[:, :length].astype(BF16)
        ad[2 * g + 1] = tiles[:, length:].astype(BF16)
        publish(g)

    def multiply_near(d):
        x_pass(d).wait_recv()
        put(2 * d - 2, two(states_ref, x_in, 2 * (d - 1)))
        c_pass(d).wait_recv()
        put(2 * d - 1, two(cot_ref, c_in, 2 * (d - 1)))

    def multiply_far():
        far_pass().wait_recv()

        @pl.when(low_chip)
        def _():
            put(ring - 2, two(cot_ref, d_in, 0))

        @pl.when(chip >= far)
        def _():
            put(ring - 2, two(states_ref, d_in, 0))

    lane = lax.broadcasted_iota(jnp.int32, (length, LANES), 1)
    low = lane < HEAD_DIM
    first = lane % HEAD_DIM < HEAD_DIM // 2
    for c in input_copies[2:]:
        c.wait()
    cos, sin = cos_ref[...], sin_ref[...]
    causal = lax.broadcasted_iota(jnp.int32, (length, length), 0) >= lax.broadcasted_iota(
        jnp.int32, (length, length), 1
    )

    def swap(v):
        return pltpu.roll(v, HEAD_DIM, 1)

    def rope(v):
        turned = jnp.where(
            first, pltpu.roll(v, LANES - HEAD_DIM // 2, 1), pltpu.roll(v, HEAD_DIM // 2, 1)
        )
        return v * cos + turned * sin

    def halves(v):
        other = swap(v)
        zero = jnp.zeros_like(v)
        return (
            (jnp.where(low, v, zero).astype(BF16), jnp.where(low, zero, other).astype(BF16)),
            (jnp.where(low, other, zero).astype(BF16), jnp.where(low, zero, v).astype(BF16)),
        )

    blocks = [
        (b, g, (b * 2 + g) * (GROUP // 2) + pair)
        for b in range(kv_cols // LANES)
        for g in range(2)
        for pair in range(GROUP // 2)
    ]

    def attend():
        for b, g, at in blocks:
            kcut, cut = slice(b * LANES, (b + 1) * LANES), slice(at * LANES, (at + 1) * LANES)
            keys = halves(rope(k_acc[:, kcut]))
            values = halves(v_acc[:, kcut])
            q = rope(q_acc[:, cut]).astype(BF16)
            att = None
            for side in range(2):
                s = dot(q, keys[g][side], NT) * HEAD_DIM ** (-0.5)
                s = jnp.where(causal, s, -jnp.inf)
                e = jnp.exp(s - jnp.max(s, axis=1, keepdims=True))
                p = (e / jnp.sum(e, axis=1, keepdims=True)).astype(BF16)
                probs[2 * at + side] = p
                a = dot(p, values[g][side])
                att = a if att is None else att + a
            att_own[:, cut] = att.astype(BF16)

    def grad_values():
        sums = {}
        for b, g, at in blocks:
            ga = g_acc[:, at * LANES : (at + 1) * LANES].astype(BF16)
            for side in range(2):
                u = dot(probs[2 * at + side], ga, TN)
                key = (b, g, side)
                sums[key] = sums[key] + u if key in sums else u
        for b in range(kv_cols // LANES):
            grad = jnp.where(
                low,
                sums[b, 0, 0] + swap(sums[b, 0, 1]),
                swap(sums[b, 1, 0]) + sums[b, 1, 1],
            )
            gv_own[:, b * LANES : (b + 1) * LANES] = grad.astype(BF16)

    def a_copy(d):
        return remote(
            att_own, a_in.at[2 * (d - 1)], a_snd.at[d - 1], a_rcv.at[d - 1],
            {"seq": device(d, core)},
        )

    def a_far():
        return remote(
            att_own, ad_in.at[0], a_snd.at[far - 1], a_rcv.at[far - 1],
            {"seq": device(far, core)},
        )

    def a_beside():
        return remote(att_own, ab_in, b_snd.at[tp], b_rcv.at[tp], {"seq": partner})

    def a_pass(d):
        return remote(
            a_in.at[2 * (d - 1)], a_in.at[2 * (d - 1) + 1], af_snd.at[d - 1],
            af_rcv.at[d - 1], {"seq": partner},
        )

    def a_far_pass():
        return remote(
            ad_in.at[0], ad_in.at[1], af_snd.at[far - 1], af_rcv.at[far - 1], {"seq": partner}
        )

    def send_attended():
        each(1, far, lambda d: a_copy(d).start())
        pl.when(chip >= far)(lambda: a_far().start())
        pl.when(core == 0)(lambda: a_beside().start())

    def pass_attended():
        def one(d):
            a_copy(d).wait_recv()
            a_pass(d).start()

        each(1, far, one)

        @pl.when(low_chip)
        def _():
            a_far().wait_recv()
            a_far_pass().start()

    def g_copy(d, other):
        return remote(
            gv_own, g_in.at[2 * (d - 1) + other], g_snd.at[other, d - 1],
            g_rcv.at[other, d - 1], {"seq": device(-d, (core + other) % 2)},
        )

    def g_far(other):
        return remote(
            gv_own, gd_in.at[other], g_snd.at[other, far - 1], g_rcv.at[other, far - 1],
            {"seq": device(far, (core + other) % 2)},
        )

    def g_beside():
        return remote(gv_own, gb_in, b_snd.at[tp + 1], b_rcv.at[tp + 1], {"seq": partner})

    def send_grads():
        @pl.when(low_chip)
        def _():
            for other in range(2):
                g_far(other).start()

        def one(d):
            for other in range(2):
                g_copy(d, other).start()

        each(1, far, one)
        pl.when(core == 1)(lambda: g_beside().start())

    lane_at = lax.broadcasted_iota(jnp.int32, (1, lanes), 1)

    def weigh(source, d, b):
        at = pl.ds(source, 1)
        sums[at, :] = sums[at, :] + jnp.sum(d * b, axis=0, keepdims=True)

    def overlap_attended(d):
        a_pass(d).wait_recv()
        over[2 * d - 1] = two(att_own, a_in, 2 * (d - 1))

    def overlap_grads(d):
        for other in range(2):
            g_copy(d, other).wait_recv()
        over[2 * d - 2] = two(gv_own, g_in, 2 * (d - 1))

    def overlap_far_attended():
        @pl.when(low_chip)
        def _():
            a_far_pass().wait_recv()
            over[ring - 2] = two(att_own, ad_in, 0)

    def overlap_far_grads():
        @pl.when(chip >= far)
        def _():
            for other in range(2):
                g_far(other).wait_recv()
            over[ring - 2] = two(gv_own, gd_in, 0)

    def score(g, hop):
        for other in range(2):
            weigh(
                device(hop, (core + other) % 2), full[2 * g + other].astype(F32),
                over[g, :, other * length : (other + 1) * length],
            )

    def score_near(d):
        totals_here(2 * d - 2)
        score(2 * d - 2, d)
        totals_here(2 * d - 1)
        score(2 * d - 1, -d)

    lower, upper, anywhere = col < mid, col >= mid, col >= 0
    project_states(0)
    relay(0, 1)
    follow(1)
    each(1, far, pass_near)
    settle(0, 1)
    arrivals(1, project_states)
    if tp > 2:
        relay_up(0, 2, anywhere)
        follow(2)
    each(1, far, multiply_near)
    relay_up(1, 1, lower)
    relay_down(1, 1, upper)
    if tp > 2:
        relay_down(0, 2, anywhere)
    for k in range(3, tp):
        relay(0, k)
        follow(k)
    project_cot(0)
    relay_up(1, 1, upper)
    pass_far()
    for k in range(2, tp - 1):
        settle(0, k)
        arrivals(k, project_states)
    multiply_far()
    each(0, ring - 2, chain)
    relay_down(1, 1, lower)
    for k in range(2, tp):
        relay(1, k)
    chain(ring - 2)
    for k in range(max(2, tp - 1), tp):
        settle(0, k)
        arrivals(k, project_states)
    attend()
    send_attended()
    square(0, range(tp))
    for k in range(1, tp):
        settle(1, k)
        arrivals(k, project_cot)
    grad_values()
    send_grads()
    each(0, ring - 1, total)
    send_totals()
    square(1, range(tp))
    multiply_beside(0)
    pass_attended()
    sums[...] = jnp.zeros_like(sums)
    weigh(me, near[1], dot(att_own[...], att_own[...], NT))
    weigh(me, near[0], dot(gv_own[...], gv_own[...], NT))

    @pl.when(core == 0)
    def _():
        g_beside().wait_recv()
        weigh(partner, near[2], dot(gv_own[...], gb_in[...], NT))

    each(1, far, overlap_attended)
    overlap_far_attended()
    multiply_beside(1)

    @pl.when(core == 1)
    def _():
        a_beside().wait_recv()
        weigh(partner, near[2], dot(att_own[...], ab_in[...], NT))

    each(1, far, overlap_grads)
    overlap_far_grads()
    each(1, far, score_near)
    totals_here(ring - 2)
    score(ring - 2, far)

    row_at = lax.broadcasted_iota(jnp.int32, (n, lanes), 0)
    spot_at = lax.broadcasted_iota(jnp.int32, (n, lanes), 1)
    pairs = jnp.sum(sums[...], axis=1, keepdims=True)[:n]
    t2[col * n + me] = jnp.sum(
        jnp.where(row_at == spot_at, pairs, 0.0), axis=0, keepdims=True
    )

    def send_scalars(plane, o):
        mine = t2.at[col * n + me]
        to = {"seq": (me + o) % n, "tp": plane}
        remote(mine, mine, r2_snd.at[0], r2_rcv.at[0], to).start()

    for t in range(tp):
        plane = jnp.where(col >= mid, t, last - t)
        each(1, n, lambda o: send_scalars(plane, o))
        pl.when(plane != col)(lambda: send_scalars(plane, 0))

    for k in range(1, tp):
        for which in range(2):
            for h in range(HALVES):
                done_up = which * (k == col + 1) * (col >= mid) * (core == 0)
                done_down = which * (k == tp - col) * (col < mid) * (core == 0)
                pl.when(sends_up(k) & (done_up == 0))(lambda: up(which, k, h).wait_send())
                pl.when(sends_down(k) & (done_down == 0))(lambda: down(which, k, h).wait_send())

    def drain_near(d):
        for c in (x_copy(d), c_copy(d), x_pass(d), c_pass(d), a_copy(d), a_pass(d)):
            c.wait_send()
        for other in range(2):
            g_copy(d, other).wait_send()

    each(1, far, drain_near)
    far_copy(states_ref).wait_send()
    far_pass().wait_send()
    for slot in range(tp):
        beside(0, slot).wait_send()
    pl.when(chip >= far)(lambda: a_far().wait_send())
    pl.when(core == 0)(lambda: a_beside().wait_send())
    pl.when(core == 1)(lambda: g_beside().wait_send())

    @pl.when(low_chip)
    def _():
        a_far_pass().wait_send()
        for other in range(2):
            g_far(other).wait_send()

    def drain_sums(g):
        inner(g, lambda c: c.wait_send())
        outer(g, lambda c: c.wait_send())

    each(0, ring - 1, drain_sums)
    others = t2.at[pl.ds(0, n * tp - 1)]
    everyone = remote(others, others, r2_snd.at[0], r2_rcv.at[0], {"seq": partner})
    everyone.wait_recv()
    table = t2[pl.ds(0, n)].reshape(n, lanes)
    for q in range(1, tp):
        table = table + t2[pl.ds(q * n, n)].reshape(n, lanes)
    rank, spot = row_at, spot_at
    eye = rank == spot
    column = jnp.sum(jnp.where(spot == me, table, 0.0), axis=1, keepdims=True)
    theirs = eye & (rank != me)
    mirrored = jnp.sum(jnp.where(theirs, column, 0.0), axis=0, keepdims=True)
    own = jnp.sum(jnp.where(rank == me, table, 0.0), axis=0, keepdims=True)
    diag = jnp.sum(jnp.where(eye, table, 0.0), axis=0, keepdims=True)
    own_diag = jnp.sum(jnp.where(lane_at == me, diag, 0.0), axis=1, keepdims=True)
    gram = (own + mirrored) / jnp.sqrt(own_diag * diag)
    out_ref[...] = gram[:, :n]
    everyone.wait_send()


def on_device(n, tp, states, cotangent, wq, wk, wv, wo):
    seq_dev, length, width = states.shape
    assert seq_dev == 1 and n % 4 == 0 and length == LANES and tp > 1
    kv = wk.shape[1]
    ring = n // 2
    far = ring // 2
    near = max(far - 1, 1)
    tiles = 2 * (ring - 1)
    lanes = -(-n // LANES) * LANES
    cos, sin = rope_tables(length)
    vmem = pl.BlockSpec(memory_space=pltpu.VMEM)
    hbm = pl.BlockSpec(memory_space=pl.ANY)
    sem = pltpu.SemaphoreType.DMA

    def half(*shape):
        return pltpu.VMEM(shape, BF16)

    def wide(*shape):
        return pltpu.VMEM(shape, F32)

    return pl.pallas_call(
        functools.partial(kernel, n, tp),
        out_shape=jax.ShapeDtypeStruct((1, n), F32),
        in_specs=[hbm] * 8,
        out_specs=vmem,
        scratch_shapes=[
            half(length, width),
            half(length, width),
            wide(length, LANES),
            wide(length, LANES),
            half(tp - 1, length, width),
            half(tp - 1, length, width),
            half(tp, width, wq.shape[1]),
            half(tp, width, kv),
            half(tp, width, kv),
            half(tp, wo.shape[0], width),
            wide(length, wq.shape[1]),
            wide(length, kv),
            wide(length, kv),
            wide(length, wo.shape[0]),
            half(2 * near, length, width),
            half(2 * near, length, width),
            half(2, length, width),
            half(tp, length, width),
            half(length, width),
            half(2 * near, length, width),
            half(2, length, width),
            half(length, width),
            half(length, kv),
            half(2 * near, length, kv),
            half(2, length, kv),
            half(length, kv),
            half(width // HEAD_DIM, length, length),
            half(tiles, length, length),
            half(tiles, length, length),
            half(tiles, length, length),
            half(tiles, length, length),
            wide(3, length, length),
            wide(ring - 1, length, 2 * length),
            wide(-(-n // 8) * 8, LANES),
            wide(tp * n, 1, lanes),
            sem((4,)),
            pltpu.SemaphoreType.REGULAR,
            sem((4 * tp,)),
            sem((2, 2, tp - 1, HALVES)),
            sem((2, tp - 1, HALVES)),
            sem((3, far)),
            sem((3, far)),
            sem((3, far)),
            sem((3, far)),
            sem((tp + 2,)),
            sem((tp + 2,)),
            sem((far,)),
            sem((far,)),
            sem((far,)),
            sem((far,)),
            sem((2, far)),
            sem((2, far)),
            sem((ring - 1,)),
            sem((ring - 1,)),
            sem((ring - 1,)),
            sem((ring - 1,)),
            sem((ring - 1,)),
            sem((1,)),
            sem((1,)),
        ],
        compiler_params=pltpu.CompilerParams(
            collective_id=0, has_side_effects=True, vmem_limit_bytes=60 * 1024 * 1024
        ),
        name="ntk_gram",
    )(
        states.reshape(length, width), cotangent.reshape(length, width),
        jnp.asarray(cos), jnp.asarray(sin), wq, wk, wv, wo,
    )


def solution(mesh):
    in_specs = (
        P("seq", None, "tp"),
        P("seq", None, "tp"),
        P(None, "tp"),
        P(None, "tp"),
        P(None, "tp"),
        P("tp", None),
    )
    return jax.shard_map(
        functools.partial(on_device, mesh.shape["seq"], mesh.shape["tp"]),
        mesh=mesh, in_specs=in_specs, out_specs=P("seq", None), check_vma=False,
    )
```

```python
import functools

import jax
import jax.numpy as jnp
import numpy as np
from jax import lax
from jax.experimental import pallas as pl
from jax.experimental.pallas import tpu as pltpu
from jax.sharding import PartitionSpec as P

HEADS = 32
KV_HEADS = 8
HEAD_DIM = 64
THETA = 500000.0
LANES = 128
HALVES = 2
GROUP = HEADS // KV_HEADS
F32, BF16 = jnp.float32, jnp.bfloat16

NT = (((1,), (1,)), ((), ()))
TN = (((0,), (0,)), ((), ()))


def rope_tables(length):
    half = HEAD_DIM // 2
    freqs = np.float32(THETA) ** (-(np.arange(half, dtype=np.float32) * np.float32(2.0 / HEAD_DIM)))
    angles = np.arange(length, dtype=np.float32)[:, None] * freqs[None, :].astype(np.float32)
    cos, sin = np.cos(angles), np.sin(angles)
    return (
        np.concatenate([cos, cos] * 2, axis=1).astype(np.float32),
        np.concatenate([-sin, sin] * 2, axis=1).astype(np.float32),
    )


def dot(a, b, dims=None):
    if dims is None:
        return jnp.dot(a, b, preferred_element_type=F32)
    return lax.dot_general(a, b, dims, preferred_element_type=F32)


def place_of(index, n):
    if n % 8:
        return index
    block, rest = index // 8, index % 8
    row, col, core = rest // 4, (rest // 2) % 2, rest % 2
    return block * 8 + 2 * (2 * row + (row + col) % 2) + core


def index_at(place, n):
    if n % 8:
        return place
    block, rest = place // 8, place % 8
    spot, core = rest // 2, rest % 2
    row = spot // 2
    return block * 8 + 2 * (2 * row + (row + spot) % 2) + core


def kernel(
    n, tp,
    states_hbm, cot_hbm, cos_hbm, sin_hbm, wq_hbm, wk_hbm, wv_hbm, wo_hbm,
    out_ref,
    states_ref, cot_ref, cos_ref, sin_ref, xs, cs, wqb, wkb, wvb, wob, q_acc, k_acc, v_acc, g_acc,
    x_in, c_in, d_in, b_in, att_own, a_in, ad_in, ab_in, gv_own, g_in, gd_in, gb_in,
    probs, ad, rin, xin, full, near, over, sums, t2,
    in_sem, clear_sem, w_sem, z_snd, z_rcv, p_snd, p_rcv, f_snd, f_rcv, b_snd, b_rcv,
    a_snd, a_rcv, af_snd, af_rcv, g_snd, g_rcv,
    i_snd, r_rcv, s_rcv, o_snd, o_rcv, r2_snd, r2_rcv,
):
    length, width = states_ref.shape
    kv_cols = k_acc.shape[1]
    ring = n // 2
    far = ring // 2
    mid = tp // 2
    hrows = length // HALVES
    lanes = t2.shape[2]
    me = lax.axis_index("seq")
    col = lax.axis_index("tp")
    place = place_of(me, n)
    chip, core = place // 2, place % 2
    low_chip = chip < far
    last = tp - 1

    def device(hop, c):
        return index_at(2 * ((chip + hop + ring) % ring) + c, n)

    partner = device(0, 1 - core)

    def each(lo, hi, body):
        if hi - lo <= 8:
            for i in range(lo, hi):
                body(i)
        else:
            lax.fori_loop(lo, hi, lambda i, c: (body(i), c)[1], 0)

    def remote(src, dst, snd, rcv, to):
        return pltpu.make_async_remote_copy(
            src_ref=src, dst_ref=dst, send_sem=snd, recv_sem=rcv, device_id=to
        )

    input_copies = [
        pltpu.make_async_copy(src, dst, in_sem.at[i])
        for i, (src, dst) in enumerate((
            (states_hbm, states_ref), (cot_hbm, cot_ref),
            (cos_hbm, cos_ref), (sin_hbm, sin_ref),
        ))
    ]
    weight_copies = []
    for k in range(tp):
        at = pl.ds(pl.multiple_of(((col - k + tp) % tp) * width, width), width)
        weight_copies.append([
            pltpu.make_async_copy(wq_hbm.at[at, :], wqb.at[k], w_sem.at[4 * k]),
            pltpu.make_async_copy(wk_hbm.at[at, :], wkb.at[k], w_sem.at[4 * k + 1]),
            pltpu.make_async_copy(wv_hbm.at[at, :], wvb.at[k], w_sem.at[4 * k + 2]),
            pltpu.make_async_copy(wo_hbm.at[:, at], wob.at[k], w_sem.at[4 * k + 3]),
        ])

    barrier = pltpu.get_barrier_semaphore()
    pl.when(col > 0)(
        lambda: pl.semaphore_signal(barrier, inc=1, device_id={"tp": col - 1})
    )
    pl.when(col < last)(
        lambda: pl.semaphore_signal(barrier, inc=1, device_id={"tp": col + 1})
    )
    each(1, n, lambda o: pl.semaphore_signal(barrier, inc=1, device_id={"seq": (me + o) % n}))
    for c in input_copies:
        c.start()
    for c in input_copies[:2]:
        c.wait()
    ends = (col == 0).astype(jnp.int32) + (col == last).astype(jnp.int32)
    pl.semaphore_wait(barrier, n + 1 - ends)

    inputs = (states_ref, cot_ref)
    held = (xs, cs)

    def rows_of(h):
        return pl.ds(h * hrows, hrows)

    def up(which, k, h):
        src = inputs[which] if k == 1 else held[which].at[k - 2]
        return remote(
            src.at[rows_of(h), :], held[which].at[k - 1, rows_of(h), :],
            z_snd.at[which, 0, k - 1, h], z_rcv.at[which, k - 1, h], {"tp": (col + 1) % tp},
        )

    def down(which, k, h):
        src = inputs[which] if k == 1 else held[which].at[tp - k]
        return remote(
            src.at[rows_of(h), :], held[which].at[tp - k - 1, rows_of(h), :],
            z_snd.at[which, 1, k - 1, h], z_rcv.at[which, tp - k - 1, h],
            {"tp": (col + tp - 1) % tp},
        )

    def sends_up(k):
        return (col >= k - 1) & (col < last)

    def sends_down(k):
        return (col + k - 1 < tp) & (col > 0)

    def landed(which, slot, h):
        remote(
            inputs[which].at[rows_of(h), :], held[which].at[slot - 1, rows_of(h), :],
            z_snd.at[which, 0, 0, h], z_rcv.at[which, slot - 1, h], {"tp": (col + 1) % tp},
        ).wait_recv()

    def begin_up(which):
        for h in range(HALVES):
            up(which, 1, h).start()

    def begin_down(which):
        for h in range(HALVES):
            down(which, 1, h).start()

    def relay_up(which, k, side):
        @pl.when((col >= k) & (col < last) & side)
        def _():
            for h in range(HALVES):
                landed(which, k, h)
                up(which, k + 1, h).start()

    def relay_down(which, k, side):
        @pl.when((col + k < tp) & (col > 0) & side)
        def _():
            for h in range(HALVES):
                landed(which, tp - k, h)
                down(which, k + 1, h).start()

    def relay_first():
        for h in range(HALVES):
            @pl.when((col > 0) & (col < last))
            def _():
                landed(0, 1, h)
                up(0, 2, h).start()
                landed(0, tp - 1, h)
                down(0, 2, h).start()

    def relay(which, k):
        relay_up(which, k, col < mid)
        relay_down(which, k, col >= mid)
        relay_up(which, k, col >= mid)
        relay_down(which, k, col < mid)

    def settle(which, k):
        for h in range(HALVES):
            pl.when((col >= k) & (col == last))(lambda: landed(which, k, h))
            pl.when((col + k < tp) & (col == 0))(lambda: landed(which, tp - k, h))

    def arrivals(k, body):
        pl.when(col >= k)(lambda: body(k))
        pl.when(col + k < tp)(lambda: body(tp - k))

    def follow(k):
        pl.when((col == k) & (col < last))(lambda: begin_up(1))
        pl.when((jnp.minimum(last - col, 1) == k) & (col > 0))(lambda: begin_down(1))

    pl.when(col < last)(lambda: begin_up(0))
    pl.when(col > 0)(lambda: begin_down(0))
    follow(0)

    def x_copy(d):
        return remote(
            states_ref, x_in.at[2 * (d - 1)], p_snd.at[0, d - 1], p_rcv.at[0, d - 1],
            {"seq": device(-d, core)},
        )

    def c_copy(d):
        return remote(
            cot_ref, c_in.at[2 * (d - 1)], p_snd.at[1, d - 1], p_rcv.at[1, d - 1],
            {"seq": device(d, core)},
        )

    def far_copy(src):
        return remote(
            src, d_in.at[0], p_snd.at[2, 0], p_rcv.at[2, 0], {"seq": device(far, core)}
        )

    def x_pass(d):
        return remote(
            x_in.at[2 * (d - 1)], x_in.at[2 * (d - 1) + 1], f_snd.at[0, d - 1],
            f_rcv.at[0, d - 1], {"seq": partner},
        )

    def c_pass(d):
        return remote(
            c_in.at[2 * (d - 1)], c_in.at[2 * (d - 1) + 1], f_snd.at[1, d - 1],
            f_rcv.at[1, d - 1], {"seq": partner},
        )

    def far_pass():
        return remote(
            d_in.at[0], d_in.at[1], f_snd.at[2, 0], f_rcv.at[2, 0], {"seq": partner}
        )

    def start_near(d):
        x_copy(d).start()
        c_copy(d).start()

    each(1, far, start_near)
    pl.when(low_chip)(lambda: far_copy(states_ref).start())
    pl.when(chip >= far)(lambda: far_copy(cot_ref).start())
    order = [0] + [s for k in range(1, tp) for s in dict.fromkeys((k, tp - k)) if k <= tp - k]
    for part in (slice(0, 3), slice(3, 4)):
        for k in order:
            for c in weight_copies[k][part]:
                c.start()

    def pass_near(d):
        x_copy(d).wait_recv()
        x_pass(d).start()
        c_copy(d).wait_recv()
        c_pass(d).start()

    def pass_far():
        far_copy(states_ref).wait_recv()
        far_pass().start()

    def own_block(which, slot):
        return inputs[which] if slot == 0 else held[which].at[slot - 1]

    def beside(which, slot):
        return remote(
            own_block(which, slot), b_in.at[slot], b_snd.at[slot], b_rcv.at[slot],
            {"seq": partner},
        )

    def square(which, slots):
        acc = None
        for slot in slots:
            x = own_block(which, slot)[...]
            piece = dot(x, x, NT)
            acc = piece if acc is None else acc + piece
        near[which] = acc

    def hand_over(which, slot):
        pl.when(core == 1 - which)(lambda: beside(which, slot).start())

    def multiply_beside(which):
        @pl.when(core == which)
        def _():
            acc = None
            for slot in range(tp):
                beside(which, slot).wait_recv()
                piece = dot(own_block(which, slot)[...], b_in[slot], NT)
                acc = piece if acc is None else acc + piece
            near[2] = acc

    def project_states(slot):
        for c in weight_copies[slot][:3]:
            c.wait()
        hand_over(0, slot)
        x = states_ref[...] if slot == 0 else xs[slot - 1]
        for acc, w in ((q_acc, wqb), (k_acc, wkb), (v_acc, wvb)):
            piece = dot(x, w[slot])
            acc[...] = piece if slot == 0 else acc[...] + piece

    def project_cot(slot):
        weight_copies[slot][3].wait()
        hand_over(1, slot)
        y = cot_ref[...] if slot == 0 else cs[slot - 1]
        piece = dot(y, wob[slot], NT)
        g_acc[...] = piece if slot == 0 else g_acc[...] + piece

    def inner(g, act):
        part = pl.ds(2 * g, 2)

        def copy(dst, rcv, to):
            return remote(ad.at[part], dst.at[part], i_snd.at[g], rcv.at[g], {"tp": to})

        pl.when(col < mid - 1)(lambda: act(copy(rin, r_rcv, (col + 1) % tp)))
        pl.when(col > mid)(lambda: act(copy(rin, r_rcv, (col + tp - 1) % tp)))
        pl.when(col == mid - 1)(lambda: act(copy(xin, s_rcv, (col + 1) % tp)))
        pl.when(col == mid)(lambda: act(copy(xin, s_rcv, (col + tp - 1) % tp)))

    def outer(g, act):
        part = pl.ds(2 * g, 2)

        def copy(to):
            return remote(full.at[part], full.at[part], o_snd.at[g], o_rcv.at[g], {"tp": to})

        pl.when((col < mid) & (col > 0))(lambda: act(copy((col + tp - 1) % tp)))
        pl.when((col >= mid) & (col < last))(lambda: act(copy((col + 1) % tp)))

    def waits_on(buf, rcv, g):
        part = pl.ds(2 * g, 2)
        remote(
            buf.at[part], buf.at[part], o_snd.at[g], rcv.at[g], {"tp": (col + 1) % tp}
        ).wait_recv()

    edge = (col == 0) | (col == last)
    central = (col == mid - 1) | (col == mid)

    def publish(g):
        pl.when(edge)(lambda: inner(g, lambda c: c.start()))

    def chain(g):
        part = pl.ds(2 * g, 2)

        @pl.when(jnp.logical_not(edge))
        def _():
            waits_on(rin, r_rcv, g)
            ad[part] = (ad[part].astype(F32) + rin[part].astype(F32)).astype(BF16)
            inner(g, lambda c: c.start())

    def total(g):
        part = pl.ds(2 * g, 2)

        @pl.when(central)
        def _():
            waits_on(xin, s_rcv, g)
            full[part] = (ad[part].astype(F32) + xin[part].astype(F32)).astype(BF16)

    def last_relays():
        for h in range(HALVES):
            @pl.when((col >= mid) & (col < last))
            def _():
                remote(
                    held[1].at[col - 1, rows_of(h), :], held[1].at[col, rows_of(h), :],
                    z_snd.at[1, 0, col, h], z_rcv.at[1, col, h], {"tp": (col + 1) % tp},
                ).wait_send()

            @pl.when((col < mid) & (col > 0))
            def _():
                remote(
                    held[1].at[col, rows_of(h), :], held[1].at[col - 1, rows_of(h), :],
                    z_snd.at[1, 1, last - col, h], z_rcv.at[1, col - 1, h],
                    {"tp": (col + tp - 1) % tp},
                ).wait_send()

    def send_totals():
        inside = jnp.logical_not(edge)
        pl.when(inside & (core == 1))(lambda: pl.semaphore_wait(clear_sem, 1))
        pl.when(central)(lambda: each(0, ring - 1, lambda g: outer(g, lambda c: c.start())))

        @pl.when(inside & (core == 0))
        def _():
            last_relays()
            pl.semaphore_signal(clear_sem, inc=1, device_id={"seq": partner})

    def totals_here(g):
        @pl.when(jnp.logical_not(central))
        def _():
            waits_on(full, o_rcv, g)
            pl.when(jnp.logical_not(edge))(lambda: outer(g, lambda c: c.start()))

    def two(own, buf, at):
        both = buf[pl.ds(at, 2)].reshape(2 * length, buf.shape[2])
        return dot(own[...], both, NT)

    def put(g, tiles):
        ad[2 * g] = tiles[:, :length].astype(BF16)
        ad[2 * g + 1] = tiles[:, length:].astype(BF16)
        publish(g)

    def multiply_near(d):
        x_pass(d).wait_recv()
        put(2 * d - 2, two(states_ref, x_in, 2 * (d - 1)))
        c_pass(d).wait_recv()
        put(2 * d - 1, two(cot_ref, c_in, 2 * (d - 1)))

    def multiply_far():
        far_pass().wait_recv()

        @pl.when(low_chip)
        def _():
            put(ring - 2, two(cot_ref, d_in, 0))

        @pl.when(chip >= far)
        def _():
            put(ring - 2, two(states_ref, d_in, 0))

    lane = lax.broadcasted_iota(jnp.int32, (length, LANES), 1)
    low = lane < HEAD_DIM
    first = lane % HEAD_DIM < HEAD_DIM // 2
    for c in input_copies[2:]:
        c.wait()
    cos, sin = cos_ref[...], sin_ref[...]
    causal = lax.broadcasted_iota(jnp.int32, (length, length), 0) >= lax.broadcasted_iota(
        jnp.int32, (length, length), 1
    )

    def swap(v):
        return pltpu.roll(v, HEAD_DIM, 1)

    def rope(v):
        turned = jnp.where(
            first, pltpu.roll(v, LANES - HEAD_DIM // 2, 1), pltpu.roll(v, HEAD_DIM // 2, 1)
        )
        return v * cos + turned * sin

    def halves(v):
        other = swap(v)
        zero = jnp.zeros_like(v)
        return (
            (jnp.where(low, v, zero).astype(BF16), jnp.where(low, zero, other).astype(BF16)),
            (jnp.where(low, other, zero).astype(BF16), jnp.where(low, zero, v).astype(BF16)),
        )

    blocks = [
        (b, g, (b * 2 + g) * (GROUP // 2) + pair)
        for b in range(kv_cols // LANES)
        for g in range(2)
        for pair in range(GROUP // 2)
    ]

    def attend():
        for b, g, at in blocks:
            kcut, cut = slice(b * LANES, (b + 1) * LANES), slice(at * LANES, (at + 1) * LANES)
            keys = halves(rope(k_acc[:, kcut]))
            values = halves(v_acc[:, kcut])
            q = rope(q_acc[:, cut]).astype(BF16)
            att = None
            for side in range(2):
                s = dot(q, keys[g][side], NT) * HEAD_DIM ** (-0.5)
                s = jnp.where(causal, s, -jnp.inf)
                e = jnp.exp(s - jnp.max(s, axis=1, keepdims=True))
                p = (e / jnp.sum(e, axis=1, keepdims=True)).astype(BF16)
                probs[2 * at + side] = p
                a = dot(p, values[g][side])
                att = a if att is None else att + a
            att_own[:, cut] = att.astype(BF16)

    def grad_values():
        sums = {}
        for b, g, at in blocks:
            ga = g_acc[:, at * LANES : (at + 1) * LANES].astype(BF16)
            for side in range(2):
                u = dot(probs[2 * at + side], ga, TN)
                key = (b, g, side)
                sums[key] = sums[key] + u if key in sums else u
        for b in range(kv_cols // LANES):
            grad = jnp.where(
                low,
                sums[b, 0, 0] + swap(sums[b, 0, 1]),
                swap(sums[b, 1, 0]) + sums[b, 1, 1],
            )
            gv_own[:, b * LANES : (b + 1) * LANES] = grad.astype(BF16)

    def a_copy(d):
        return remote(
            att_own, a_in.at[2 * (d - 1)], a_snd.at[d - 1], a_rcv.at[d - 1],
            {"seq": device(d, core)},
        )

    def a_far():
        return remote(
            att_own, ad_in.at[0], a_snd.at[far - 1], a_rcv.at[far - 1],
            {"seq": device(far, core)},
        )

    def a_beside():
        return remote(att_own, ab_in, b_snd.at[tp], b_rcv.at[tp], {"seq": partner})

    def a_pass(d):
        return remote(
            a_in.at[2 * (d - 1)], a_in.at[2 * (d - 1) + 1], af_snd.at[d - 1],
            af_rcv.at[d - 1], {"seq": partner},
        )

    def a_far_pass():
        return remote(
            ad_in.at[0], ad_in.at[1], af_snd.at[far - 1], af_rcv.at[far - 1], {"seq": partner}
        )

    def send_attended():
        each(1, far, lambda d: a_copy(d).start())
        pl.when(chip >= far)(lambda: a_far().start())
        pl.when(core == 0)(lambda: a_beside().start())

    def pass_attended():
        def one(d):
            a_copy(d).wait_recv()
            a_pass(d).start()

        each(1, far, one)

        @pl.when(low_chip)
        def _():
            a_far().wait_recv()
            a_far_pass().start()

    def g_copy(d, other):
        return remote(
            gv_own, g_in.at[2 * (d - 1) + other], g_snd.at[other, d - 1],
            g_rcv.at[other, d - 1], {"seq": device(-d, (core + other) % 2)},
        )

    def g_far(other):
        return remote(
            gv_own, gd_in.at[other], g_snd.at[other, far - 1], g_rcv.at[other, far - 1],
            {"seq": device(far, (core + other) % 2)},
        )

    def g_beside():
        return remote(gv_own, gb_in, b_snd.at[tp + 1], b_rcv.at[tp + 1], {"seq": partner})

    def send_grads():
        @pl.when(low_chip)
        def _():
            for other in range(2):
                g_far(other).start()

        def one(d):
            for other in range(2):
                g_copy(d, other).start()

        each(1, far, one)
        pl.when(core == 1)(lambda: g_beside().start())

    lane_at = lax.broadcasted_iota(jnp.int32, (1, lanes), 1)

    def weigh(source, d, b):
        at = pl.ds(source, 1)
        sums[at, :] = sums[at, :] + jnp.sum(d * b, axis=0, keepdims=True)

    def overlap_attended(d):
        a_pass(d).wait_recv()
        over[2 * d - 1] = two(att_own, a_in, 2 * (d - 1))

    def overlap_grads(d):
        for other in range(2):
            g_copy(d, other).wait_recv()
        over[2 * d - 2] = two(gv_own, g_in, 2 * (d - 1))

    def overlap_far_attended():
        @pl.when(low_chip)
        def _():
            a_far_pass().wait_recv()
            over[ring - 2] = two(att_own, ad_in, 0)

    def overlap_far_grads():
        @pl.when(chip >= far)
        def _():
            for other in range(2):
                g_far(other).wait_recv()
            over[ring - 2] = two(gv_own, gd_in, 0)

    def score(g, hop):
        for other in range(2):
            weigh(
                device(hop, (core + other) % 2), full[2 * g + other].astype(F32),
                over[g, :, other * length : (other + 1) * length],
            )

    def score_near(d):
        totals_here(2 * d - 2)
        score(2 * d - 2, d)
        totals_here(2 * d - 1)
        score(2 * d - 1, -d)

    lower, upper, anywhere = col < mid, col >= mid, col >= 0
    project_states(0)
    relay_first()
    follow(1)
    each(1, far, pass_near)
    settle(0, 1)
    arrivals(1, project_states)
    if tp > 2:
        relay_up(0, 2, anywhere)
        follow(2)
    each(1, far, multiply_near)
    relay_up(1, 1, lower)
    relay_down(1, 1, upper)
    if tp > 2:
        relay_down(0, 2, anywhere)
    for k in range(3, tp):
        relay(0, k)
        follow(k)
    project_cot(0)
    relay_up(1, 1, upper)
    pass_far()
    for k in range(2, tp - 1):
        settle(0, k)
        arrivals(k, project_states)
    multiply_far()
    each(0, ring - 2, chain)
    relay_down(1, 1, lower)
    for k in range(2, tp):
        relay(1, k)
    chain(ring - 2)
    for k in range(max(2, tp - 1), tp):
        settle(0, k)
        arrivals(k, project_states)
    attend()
    send_attended()
    square(0, range(tp))
    for k in range(1, tp):
        settle(1, k)
        arrivals(k, project_cot)
    grad_values()
    send_grads()
    each(0, ring - 1, total)
    send_totals()
    square(1, range(tp))
    multiply_beside(0)
    pass_attended()
    sums[...] = jnp.zeros_like(sums)
    weigh(me, near[1], dot(att_own[...], att_own[...], NT))
    weigh(me, near[0], dot(gv_own[...], gv_own[...], NT))

    @pl.when(core == 0)
    def _():
        g_beside().wait_recv()
        weigh(partner, near[2], dot(gv_own[...], gb_in[...], NT))

    each(1, far, overlap_attended)
    overlap_far_attended()
    multiply_beside(1)

    @pl.when(core == 1)
    def _():
        a_beside().wait_recv()
        weigh(partner, near[2], dot(att_own[...], ab_in[...], NT))

    each(1, far, overlap_grads)
    overlap_far_grads()
    each(1, far, score_near)
    totals_here(ring - 2)
    score(ring - 2, far)

    row_at = lax.broadcasted_iota(jnp.int32, (n, lanes), 0)
    spot_at = lax.broadcasted_iota(jnp.int32, (n, lanes), 1)
    pairs = jnp.sum(sums[...], axis=1, keepdims=True)[:n]
    t2[col * n + me] = jnp.sum(
        jnp.where(row_at == spot_at, pairs, 0.0), axis=0, keepdims=True
    )

    def send_scalars(plane, o):
        mine = t2.at[col * n + me]
        to = {"seq": (me + o) % n, "tp": plane}
        remote(mine, mine, r2_snd.at[0], r2_rcv.at[0], to).start()

    for t in range(tp):
        plane = jnp.where(col >= mid, t, last - t)
        each(1, n, lambda o: send_scalars(plane, o))
        pl.when(plane != col)(lambda: send_scalars(plane, 0))

    for k in range(1, tp):
        for which in range(2):
            for h in range(HALVES):
                done_up = which * (k == col + 1) * (col >= mid) * (core == 0)
                done_down = which * (k == tp - col) * (col < mid) * (core == 0)
                pl.when(sends_up(k) & (done_up == 0))(lambda: up(which, k, h).wait_send())
                pl.when(sends_down(k) & (done_down == 0))(lambda: down(which, k, h).wait_send())

    def drain_near(d):
        for c in (x_copy(d), c_copy(d), x_pass(d), c_pass(d), a_copy(d), a_pass(d)):
            c.wait_send()
        for other in range(2):
            g_copy(d, other).wait_send()

    each(1, far, drain_near)
    far_copy(states_ref).wait_send()
    far_pass().wait_send()
    for slot in range(tp):
        beside(0, slot).wait_send()
    pl.when(chip >= far)(lambda: a_far().wait_send())
    pl.when(core == 0)(lambda: a_beside().wait_send())
    pl.when(core == 1)(lambda: g_beside().wait_send())

    @pl.when(low_chip)
    def _():
        a_far_pass().wait_send()
        for other in range(2):
            g_far(other).wait_send()

    def drain_sums(g):
        inner(g, lambda c: c.wait_send())
        outer(g, lambda c: c.wait_send())

    each(0, ring - 1, drain_sums)
    others = t2.at[pl.ds(0, n * tp - 1)]
    everyone = remote(others, others, r2_snd.at[0], r2_rcv.at[0], {"seq": partner})
    everyone.wait_recv()
    table = t2[pl.ds(0, n)].reshape(n, lanes)
    for q in range(1, tp):
        table = table + t2[pl.ds(q * n, n)].reshape(n, lanes)
    rank, spot = row_at, spot_at
    eye = rank == spot
    column = jnp.sum(jnp.where(spot == me, table, 0.0), axis=1, keepdims=True)
    theirs = eye & (rank != me)
    mirrored = jnp.sum(jnp.where(theirs, column, 0.0), axis=0, keepdims=True)
    own = jnp.sum(jnp.where(rank == me, table, 0.0), axis=0, keepdims=True)
    diag = jnp.sum(jnp.where(eye, table, 0.0), axis=0, keepdims=True)
    own_diag = jnp.sum(jnp.where(lane_at == me, diag, 0.0), axis=1, keepdims=True)
    gram = (own + mirrored) / jnp.sqrt(own_diag * diag)
    out_ref[...] = gram[:, :n]
    everyone.wait_send()


def on_device(n, tp, states, cotangent, wq, wk, wv, wo):
    seq_dev, length, width = states.shape
    assert seq_dev == 1 and n % 4 == 0 and length == LANES and tp > 1
    kv = wk.shape[1]
    ring = n // 2
    far = ring // 2
    near = max(far - 1, 1)
    tiles = 2 * (ring - 1)
    lanes = -(-n // LANES) * LANES
    cos, sin = rope_tables(length)
    vmem = pl.BlockSpec(memory_space=pltpu.VMEM)
    hbm = pl.BlockSpec(memory_space=pl.ANY)
    sem = pltpu.SemaphoreType.DMA

    def half(*shape):
        return pltpu.VMEM(shape, BF16)

    def wide(*shape):
        return pltpu.VMEM(shape, F32)

    return pl.pallas_call(
        functools.partial(kernel, n, tp),
        out_shape=pltpu.VMEM((1, n), F32),
        in_specs=[hbm] * 8,
        out_specs=vmem,
        scratch_shapes=[
            half(length, width),
            half(length, width),
            wide(length, LANES),
            wide(length, LANES),
            half(tp - 1, length, width),
            half(tp - 1, length, width),
            half(tp, width, wq.shape[1]),
            half(tp, width, kv),
            half(tp, width, kv),
            half(tp, wo.shape[0], width),
            wide(length, wq.shape[1]),
            wide(length, kv),
            wide(length, kv),
            wide(length, wo.shape[0]),
            half(2 * near, length, width),
            half(2 * near, length, width),
            half(2, length, width),
            half(tp, length, width),
            half(length, width),
            half(2 * near, length, width),
            half(2, length, width),
            half(length, width),
            half(length, kv),
            half(2 * near, length, kv),
            half(2, length, kv),
            half(length, kv),
            half(width // HEAD_DIM, length, length),
            half(tiles, length, length),
            half(tiles, length, length),
            half(tiles, length, length),
            half(tiles, length, length),
            wide(3, length, length),
            wide(ring - 1, length, 2 * length),
            wide(-(-n // 8) * 8, LANES),
            wide(tp * n, 1, lanes),
            sem((4,)),
            pltpu.SemaphoreType.REGULAR,
            sem((4 * tp,)),
            sem((2, 2, tp - 1, HALVES)),
            sem((2, tp - 1, HALVES)),
            sem((3, far)),
            sem((3, far)),
            sem((3, far)),
            sem((3, far)),
            sem((tp + 2,)),
            sem((tp + 2,)),
            sem((far,)),
            sem((far,)),
            sem((far,)),
            sem((far,)),
            sem((2, far)),
            sem((2, far)),
            sem((ring - 1,)),
            sem((ring - 1,)),
            sem((ring - 1,)),
            sem((ring - 1,)),
            sem((ring - 1,)),
            sem((1,)),
            sem((1,)),
        ],
        compiler_params=pltpu.CompilerParams(
            collective_id=0, has_side_effects=True, vmem_limit_bytes=60 * 1024 * 1024
        ),
        name="ntk_gram",
    )(
        states.reshape(length, width), cotangent.reshape(length, width),
        jnp.asarray(cos), jnp.asarray(sin), wq, wk, wv, wo,
    )


def solution(mesh):
    in_specs = (
        P("seq", None, "tp"),
        P("seq", None, "tp"),
        P(None, "tp"),
        P(None, "tp"),
        P(None, "tp"),
        P("tp", None),
    )
    return jax.shard_map(
        functools.partial(on_device, mesh.shape["seq"], mesh.shape["tp"]),
        mesh=mesh, in_specs=in_specs, out_specs=P("seq", None), check_vma=False,
    )
```

```python
import functools

import jax
import jax.numpy as jnp
import numpy as np
from jax import lax
from jax.experimental import pallas as pl
from jax.experimental.pallas import tpu as pltpu
from jax.sharding import PartitionSpec as P

HEADS = 32
KV_HEADS = 8
HEAD_DIM = 64
THETA = 500000.0
LANES = 128
HALVES = 2
GROUP = HEADS // KV_HEADS
F32, BF16 = jnp.float32, jnp.bfloat16

NT = (((1,), (1,)), ((), ()))
TN = (((0,), (0,)), ((), ()))


def rope_tables(length):
    half = HEAD_DIM // 2
    freqs = np.float32(THETA) ** (-(np.arange(half, dtype=np.float32) * np.float32(2.0 / HEAD_DIM)))
    angles = np.arange(length, dtype=np.float32)[:, None] * freqs[None, :].astype(np.float32)
    cos, sin = np.cos(angles), np.sin(angles)
    return (
        np.concatenate([cos, cos] * 2, axis=1).astype(np.float32),
        np.concatenate([-sin, sin] * 2, axis=1).astype(np.float32),
    )


def dot(a, b, dims=None):
    if dims is None:
        return jnp.dot(a, b, preferred_element_type=F32)
    return lax.dot_general(a, b, dims, preferred_element_type=F32)


def place_of(index, n):
    if n % 8:
        return index
    block, rest = index // 8, index % 8
    row, col, core = rest // 4, (rest // 2) % 2, rest % 2
    return block * 8 + 2 * (2 * row + (row + col) % 2) + core


def index_at(place, n):
    if n % 8:
        return place
    block, rest = place // 8, place % 8
    spot, core = rest // 2, rest % 2
    row = spot // 2
    return block * 8 + 2 * (2 * row + (row + spot) % 2) + core


def kernel(
    n, tp,
    states_hbm, cot_hbm, cos_hbm, sin_hbm, wq_hbm, wk_hbm, wv_hbm, wo_hbm,
    out_ref,
    own, tables, xs, cs, wqkv, wob, qkv_acc, g_acc,
    x_in, c_in, d_in, b_in, att_own, a_in, ad_in, ab_in, gv_own, g_in, gd_in, gb_in,
    probs, ad, rin, xin, full, near, over, sums, t2,
    in_sem, clear_sem, w_sem, snd, last_snd, z_rcv, p_rcv, pd_rcv, f_rcv, fd_rcv, b_rcv,
    a_rcv, af_rcv, g_rcv, r_rcv, s_rcv, o_rcv, r2_snd, r2_rcv,
):
    states_ref, cot_ref = own.at[0], own.at[1]
    length, width = states_ref.shape
    q_cols = wq_hbm.shape[1]
    kv_cols = wk_hbm.shape[1]
    ring = n // 2
    far = ring // 2
    mid = tp // 2
    hrows = length // HALVES
    lanes = t2.shape[2]
    me = lax.axis_index("seq")
    col = lax.axis_index("tp")
    place = place_of(me, n)
    chip, core = place // 2, place % 2
    low_chip = chip < far
    last = tp - 1

    def device(hop, c):
        return index_at(2 * ((chip + hop + ring) % ring) + c, n)

    partner = device(0, 1 - core)

    def each(lo, hi, body):
        if hi - lo <= 8:
            for i in range(lo, hi):
                body(i)
        else:
            lax.fori_loop(lo, hi, lambda i, c: (body(i), c)[1], 0)

    def remote(src, dst, snd, rcv, to):
        return pltpu.make_async_remote_copy(
            src_ref=src, dst_ref=dst, send_sem=snd, recv_sem=rcv, device_id=to
        )

    local = pltpu.make_async_copy
    input_copies = [
        local(states_hbm, own.at[0], in_sem.at[0]),
        local(cot_hbm, own.at[1], in_sem.at[0]),
        local(cos_hbm, tables.at[0], in_sem.at[1]),
        local(sin_hbm, tables.at[1], in_sem.at[1]),
    ]
    kv_at = q_cols + kv_cols
    weight_copies = [
        local(wq_hbm, wqkv.at[:, pl.ds(0, q_cols)], w_sem.at[0]),
        local(wk_hbm, wqkv.at[:, pl.ds(q_cols, kv_cols)], w_sem.at[0]),
        local(wv_hbm, wqkv.at[:, pl.ds(kv_at, kv_cols)], w_sem.at[0]),
        local(wo_hbm, wob, w_sem.at[1]),
    ]

    barrier = pltpu.get_barrier_semaphore()
    pl.when(col > 0)(
        lambda: pl.semaphore_signal(barrier, inc=1, device_id={"tp": col - 1})
    )
    pl.when(col < last)(
        lambda: pl.semaphore_signal(barrier, inc=1, device_id={"tp": col + 1})
    )
    each(1, n, lambda o: pl.semaphore_signal(barrier, inc=1, device_id={"seq": (me + o) % n}))
    for c in input_copies:
        c.start()
    local(own, own, in_sem.at[0]).wait()
    ends = (col == 0).astype(jnp.int32) + (col == last).astype(jnp.int32)
    pl.semaphore_wait(barrier, n + 1 - ends)

    inputs = (states_ref, cot_ref)
    held = (xs, cs)

    def rows_of(h):
        return pl.ds(h * hrows, hrows)

    def up(which, k, h, sem=None):
        src = inputs[which] if k == 1 else held[which].at[k - 2]
        return remote(
            src.at[rows_of(h), :], held[which].at[k - 1, rows_of(h), :],
            snd.at[0] if sem is None else sem, z_rcv.at[which, k - 1, h], {"tp": (col + 1) % tp},
        )

    def down(which, k, h, sem=None):
        src = inputs[which] if k == 1 else held[which].at[tp - k]
        return remote(
            src.at[rows_of(h), :], held[which].at[tp - k - 1, rows_of(h), :],
            snd.at[0] if sem is None else sem, z_rcv.at[which, tp - k - 1, h],
            {"tp": (col + tp - 1) % tp},
        )

    def sends_up(k):
        return (col >= k - 1) & (col < last)

    def sends_down(k):
        return (col + k - 1 < tp) & (col > 0)

    def landed(which, slot, h):
        remote(
            inputs[which].at[rows_of(h), :], held[which].at[slot - 1, rows_of(h), :],
            snd.at[0], z_rcv.at[which, slot - 1, h], {"tp": (col + 1) % tp},
        ).wait_recv()

    def begin_up(which):
        for h in range(HALVES):
            up(which, 1, h).start()

    def begin_down(which):
        for h in range(HALVES):
            down(which, 1, h).start()

    def ends_up(which, k):
        return (which == 1) & (k == col) & (col >= mid)

    def ends_down(which, k):
        return (which == 1) & (k == last - col) & (col < mid)

    def relay_up(which, k, side):
        @pl.when((col >= k) & (col < last) & side)
        def _():
            for h in range(HALVES):
                landed(which, k, h)
                ends = ends_up(which, k)
                pl.when(ends)(lambda: up(which, k + 1, h, last_snd.at[h]).start())
                pl.when(jnp.logical_not(ends))(lambda: up(which, k + 1, h).start())

    def relay_down(which, k, side):
        @pl.when((col + k < tp) & (col > 0) & side)
        def _():
            for h in range(HALVES):
                landed(which, tp - k, h)
                ends = ends_down(which, k)
                pl.when(ends)(lambda: down(which, k + 1, h, last_snd.at[h]).start())
                pl.when(jnp.logical_not(ends))(lambda: down(which, k + 1, h).start())

    def relay_first():
        for h in range(HALVES):
            @pl.when((col > 0) & (col < last))
            def _():
                landed(0, 1, h)
                up(0, 2, h).start()
                landed(0, tp - 1, h)
                down(0, 2, h).start()

    def relay(which, k):
        relay_up(which, k, col < mid)
        relay_down(which, k, col >= mid)
        relay_up(which, k, col >= mid)
        relay_down(which, k, col < mid)

    def settle(which, k):
        for h in range(HALVES):
            pl.when((col >= k) & (col == last))(lambda: landed(which, k, h))
            pl.when((col + k < tp) & (col == 0))(lambda: landed(which, tp - k, h))

    def arrivals(k, body):
        pl.when(col >= k)(lambda: body(k))
        pl.when(col + k < tp)(lambda: body(tp - k))

    def follow(k):
        pl.when((col == k) & (col < last))(lambda: begin_up(1))
        pl.when((jnp.minimum(last - col, 1) == k) & (col > 0))(lambda: begin_down(1))

    pl.when(col < last)(lambda: begin_up(0))
    pl.when(col > 0)(lambda: begin_down(0))
    follow(0)

    def x_copy(d):
        return remote(
            states_ref, x_in.at[2 * (d - 1)], snd.at[0], p_rcv.at[0, d - 1],
            {"seq": device(-d, core)},
        )

    def c_copy(d):
        return remote(
            cot_ref, c_in.at[2 * (d - 1)], snd.at[0], p_rcv.at[1, d - 1],
            {"seq": device(d, core)},
        )

    def far_copy(src):
        return remote(
            src, d_in.at[0], snd.at[0], pd_rcv.at[0], {"seq": device(far, core)}
        )

    def x_pass(d):
        return remote(
            x_in.at[2 * (d - 1)], x_in.at[2 * (d - 1) + 1], snd.at[0],
            f_rcv.at[0, d - 1], {"seq": partner},
        )

    def c_pass(d):
        return remote(
            c_in.at[2 * (d - 1)], c_in.at[2 * (d - 1) + 1], snd.at[0],
            f_rcv.at[1, d - 1], {"seq": partner},
        )

    def far_pass():
        return remote(
            d_in.at[0], d_in.at[1], snd.at[0], fd_rcv.at[0], {"seq": partner}
        )

    def start_near(d):
        x_copy(d).start()
        c_copy(d).start()

    each(1, far, start_near)
    pl.when(low_chip)(lambda: far_copy(states_ref).start())
    pl.when(chip >= far)(lambda: far_copy(cot_ref).start())
    for c in weight_copies:
        c.start()

    def pass_near(d):
        x_copy(d).wait_recv()
        x_pass(d).start()
        c_copy(d).wait_recv()
        c_pass(d).start()

    def pass_far():
        far_copy(states_ref).wait_recv()
        far_pass().start()

    def own_block(which, slot):
        return inputs[which] if slot == 0 else held[which].at[slot - 1]

    def beside(which, slot):
        return remote(
            own_block(which, slot), b_in.at[slot], snd.at[0], b_rcv.at[0],
            {"seq": partner},
        )

    def square(which, slots):
        acc = None
        for slot in slots:
            x = own_block(which, slot)[...]
            piece = dot(x, x, NT)
            acc = piece if acc is None else acc + piece
        near[which] = acc

    def hand_over(which, slot):
        pl.when(core == 1 - which)(lambda: beside(which, slot).start())

    def multiply_beside(which):
        @pl.when(core == which)
        def _():
            acc = None
            remote(b_in, b_in, snd.at[0], b_rcv.at[0], {"seq": partner}).wait_recv()
            for slot in range(tp):
                piece = dot(own_block(which, slot)[...], b_in[slot], NT)
                acc = piece if acc is None else acc + piece
            near[2] = acc

    def features(slot):
        return pl.ds(pl.multiple_of(((col - slot + tp) % tp) * width, width), width)

    def project_states(slot):
        if slot == 0:
            local(wqkv, wqkv, w_sem.at[0]).wait()
        hand_over(0, slot)
        piece = dot(own_block(0, slot)[...], wqkv[features(slot), :])
        qkv_acc[...] = piece if slot == 0 else qkv_acc[...] + piece

    def project_cot(slot):
        if slot == 0:
            local(wob, wob, w_sem.at[1]).wait()
        hand_over(1, slot)
        piece = dot(own_block(1, slot)[...], wob[:, features(slot)], NT)
        g_acc[...] = piece if slot == 0 else g_acc[...] + piece

    def inner(g, act):
        part = pl.ds(2 * g, 2)

        def copy(dst, rcv, to):
            return remote(ad.at[part], dst.at[part], snd.at[0], rcv.at[g], {"tp": to})

        pl.when(col < mid - 1)(lambda: act(copy(rin, r_rcv, (col + 1) % tp)))
        pl.when(col > mid)(lambda: act(copy(rin, r_rcv, (col + tp - 1) % tp)))
        pl.when(col == mid - 1)(lambda: act(copy(xin, s_rcv, (col + 1) % tp)))
        pl.when(col == mid)(lambda: act(copy(xin, s_rcv, (col + tp - 1) % tp)))

    def outer(g, act):
        part = pl.ds(2 * g, 2)

        def copy(to):
            return remote(full.at[part], full.at[part], snd.at[0], o_rcv.at[g], {"tp": to})

        pl.when((col < mid) & (col > 0))(lambda: act(copy((col + tp - 1) % tp)))
        pl.when((col >= mid) & (col < last))(lambda: act(copy((col + 1) % tp)))

    def waits_on(buf, rcv, g):
        part = pl.ds(2 * g, 2)
        remote(
            buf.at[part], buf.at[part], snd.at[0], rcv.at[g], {"tp": (col + 1) % tp}
        ).wait_recv()

    edge = (col == 0) | (col == last)
    central = (col == mid - 1) | (col == mid)

    def publish(g):
        pl.when(edge)(lambda: inner(g, lambda c: c.start()))

    def chain(g):
        part = pl.ds(2 * g, 2)

        @pl.when(jnp.logical_not(edge))
        def _():
            waits_on(rin, r_rcv, g)
            ad[part] = (ad[part].astype(F32) + rin[part].astype(F32)).astype(BF16)
            inner(g, lambda c: c.start())

    def total(g):
        part = pl.ds(2 * g, 2)

        @pl.when(central)
        def _():
            waits_on(xin, s_rcv, g)
            full[part] = (ad[part].astype(F32) + xin[part].astype(F32)).astype(BF16)

    def last_relays():
        for h in range(HALVES):
            @pl.when((col >= mid) & (col < last))
            def _():
                remote(
                    held[1].at[col - 1, rows_of(h), :], held[1].at[col, rows_of(h), :],
                    last_snd.at[h], z_rcv.at[1, col, h], {"tp": (col + 1) % tp},
                ).wait_send()

            @pl.when((col < mid) & (col > 0))
            def _():
                remote(
                    held[1].at[col, rows_of(h), :], held[1].at[col - 1, rows_of(h), :],
                    last_snd.at[h], z_rcv.at[1, col - 1, h],
                    {"tp": (col + tp - 1) % tp},
                ).wait_send()

    def send_totals():
        inside = jnp.logical_not(edge)
        pl.when(inside & (core == 1))(lambda: pl.semaphore_wait(clear_sem, 1))
        pl.when(central)(lambda: each(0, ring - 1, lambda g: outer(g, lambda c: c.start())))

        @pl.when(inside & (core == 0))
        def _():
            last_relays()
            pl.semaphore_signal(clear_sem, inc=1, device_id={"seq": partner})

    def totals_here(g):
        @pl.when(jnp.logical_not(central))
        def _():
            waits_on(full, o_rcv, g)
            pl.when(jnp.logical_not(edge))(lambda: outer(g, lambda c: c.start()))

    def two(own, buf, at):
        both = buf[pl.ds(at, 2)].reshape(2 * length, buf.shape[2])
        return dot(own[...], both, NT)

    def put(g, tiles):
        ad[2 * g] = tiles[:, :length].astype(BF16)
        ad[2 * g + 1] = tiles[:, length:].astype(BF16)
        publish(g)

    def multiply_near(d):
        x_pass(d).wait_recv()
        put(2 * d - 2, two(states_ref, x_in, 2 * (d - 1)))
        c_pass(d).wait_recv()
        put(2 * d - 1, two(cot_ref, c_in, 2 * (d - 1)))

    def multiply_far():
        far_pass().wait_recv()

        @pl.when(low_chip)
        def _():
            put(ring - 2, two(cot_ref, d_in, 0))

        @pl.when(chip >= far)
        def _():
            put(ring - 2, two(states_ref, d_in, 0))

    lane = lax.broadcasted_iota(jnp.int32, (length, LANES), 1)
    low = lane < HEAD_DIM
    first = lane % HEAD_DIM < HEAD_DIM // 2
    local(tables, tables, in_sem.at[1]).wait()
    cos, sin = tables[0], tables[1]
    causal = lax.broadcasted_iota(jnp.int32, (length, length), 0) >= lax.broadcasted_iota(
        jnp.int32, (length, length), 1
    )

    def swap(v):
        return pltpu.roll(v, HEAD_DIM, 1)

    def rope(v):
        turned = jnp.where(
            first, pltpu.roll(v, LANES - HEAD_DIM // 2, 1), pltpu.roll(v, HEAD_DIM // 2, 1)
        )
        return v * cos + turned * sin

    def halves(v):
        other = swap(v)
        zero = jnp.zeros_like(v)
        return (
            (jnp.where(low, v, zero).astype(BF16), jnp.where(low, zero, other).astype(BF16)),
            (jnp.where(low, other, zero).astype(BF16), jnp.where(low, zero, v).astype(BF16)),
        )

    blocks = [
        (b, g, (b * 2 + g) * (GROUP // 2) + pair)
        for b in range(kv_cols // LANES)
        for g in range(2)
        for pair in range(GROUP // 2)
    ]

    def attend():
        for b in range(kv_cols // LANES):
            kcut = slice(q_cols + b * LANES, q_cols + (b + 1) * LANES)
            vcut = slice(kv_at + b * LANES, kv_at + (b + 1) * LANES)
            keys = [jnp.concatenate(h, axis=0) for h in halves(rope(qkv_acc[:, kcut]))]
            values = [jnp.concatenate(h, axis=0) for h in halves(qkv_acc[:, vcut])]
            for of, g, at in blocks:
                if of != b:
                    continue
                cut = slice(at * LANES, (at + 1) * LANES)
                q = rope(qkv_acc[:, cut]).astype(BF16)
                both = dot(q, keys[g], NT) * HEAD_DIM ** (-0.5)
                weights = []
                for side in range(2):
                    s = jnp.where(causal, both[:, side * length : (side + 1) * length], -jnp.inf)
                    e = jnp.exp(s - jnp.max(s, axis=1, keepdims=True))
                    p = (e / jnp.sum(e, axis=1, keepdims=True)).astype(BF16)
                    probs[2 * at + side] = p
                    weights.append(p)
                a = dot(jnp.concatenate(weights, axis=1), values[g])
                att_own[:, cut] = a.astype(BF16)

    def grad_values():
        sums = {}
        for b, g, at in blocks:
            ga = g_acc[:, at * LANES : (at + 1) * LANES].astype(BF16)
            for side in range(2):
                u = dot(probs[2 * at + side], ga, TN)
                key = (b, g, side)
                sums[key] = sums[key] + u if key in sums else u
        for b in range(kv_cols // LANES):
            grad = jnp.where(
                low,
                sums[b, 0, 0] + swap(sums[b, 0, 1]),
                swap(sums[b, 1, 0]) + sums[b, 1, 1],
            )
            gv_own[:, b * LANES : (b + 1) * LANES] = grad.astype(BF16)

    def a_copy(d):
        return remote(
            att_own, a_in.at[2 * (d - 1)], snd.at[0], a_rcv.at[d - 1],
            {"seq": device(d, core)},
        )

    def a_far():
        return remote(
            att_own, ad_in.at[0], snd.at[0], a_rcv.at[far - 1],
            {"seq": device(far, core)},
        )

    def a_beside():
        return remote(att_own, ab_in, snd.at[0], b_rcv.at[1], {"seq": partner})

    def a_pass(d):
        return remote(
            a_in.at[2 * (d - 1)], a_in.at[2 * (d - 1) + 1], snd.at[0],
            af_rcv.at[d - 1], {"seq": partner},
        )

    def a_far_pass():
        return remote(
            ad_in.at[0], ad_in.at[1], snd.at[0], af_rcv.at[far - 1], {"seq": partner}
        )

    def send_attended():
        each(1, far, lambda d: a_copy(d).start())
        pl.when(chip >= far)(lambda: a_far().start())
        pl.when(core == 0)(lambda: a_beside().start())

    def pass_attended():
        def one(d):
            a_copy(d).wait_recv()
            a_pass(d).start()

        each(1, far, one)

        @pl.when(low_chip)
        def _():
            a_far().wait_recv()
            a_far_pass().start()

    def g_copy(d, other):
        return remote(
            gv_own, g_in.at[2 * (d - 1) + other], snd.at[0],
            g_rcv.at[d - 1], {"seq": device(-d, (core + other) % 2)},
        )

    def g_far(other):
        return remote(
            gv_own, gd_in.at[other], snd.at[0], g_rcv.at[far - 1],
            {"seq": device(far, (core + other) % 2)},
        )

    def g_beside():
        return remote(gv_own, gb_in, snd.at[0], b_rcv.at[2], {"seq": partner})

    def send_grads():
        @pl.when(low_chip)
        def _():
            for other in range(2):
                g_far(other).start()

        def one(d):
            for other in range(2):
                g_copy(d, other).start()

        each(1, far, one)
        pl.when(core == 1)(lambda: g_beside().start())

    lane_at = lax.broadcasted_iota(jnp.int32, (1, lanes), 1)

    def weigh(source, d, b):
        at = pl.ds(source, 1)
        sums[at, :] = sums[at, :] + jnp.sum(d * b, axis=0, keepdims=True)

    def overlap_attended(d):
        a_pass(d).wait_recv()
        over[2 * d - 1] = two(att_own, a_in, 2 * (d - 1))

    def overlap_grads(d):
        both = g_in.at[pl.ds(2 * (d - 1), 2)]
        remote(both, both, snd.at[0], g_rcv.at[d - 1], {"seq": partner}).wait_recv()
        over[2 * d - 2] = two(gv_own, g_in, 2 * (d - 1))

    def overlap_far_attended():
        @pl.when(low_chip)
        def _():
            a_far_pass().wait_recv()
            over[ring - 2] = two(att_own, ad_in, 0)

    def overlap_far_grads():
        @pl.when(chip >= far)
        def _():
            remote(gd_in, gd_in, snd.at[0], g_rcv.at[far - 1], {"seq": partner}).wait_recv()
            over[ring - 2] = two(gv_own, gd_in, 0)

    def score(g, hop):
        for other in range(2):
            weigh(
                device(hop, (core + other) % 2), full[2 * g + other].astype(F32),
                over[g, :, other * length : (other + 1) * length],
            )

    def score_near(d):
        totals_here(2 * d - 2)
        score(2 * d - 2, d)
        totals_here(2 * d - 1)
        score(2 * d - 1, -d)

    lower, upper, anywhere = col < mid, col >= mid, col >= 0
    project_states(0)
    relay_first()
    follow(1)
    each(1, far, pass_near)
    settle(0, 1)
    arrivals(1, project_states)
    if tp > 2:
        relay_up(0, 2, anywhere)
        follow(2)
    each(1, far, multiply_near)
    relay_up(1, 1, lower)
    relay_down(1, 1, upper)
    if tp > 2:
        relay_down(0, 2, anywhere)
    for k in range(3, tp):
        relay(0, k)
        follow(k)
    project_cot(0)
    relay_up(1, 1, upper)
    pass_far()
    for k in range(2, tp - 1):
        settle(0, k)
        arrivals(k, project_states)

    each(0, ring - 2, chain)
    multiply_far()
    relay_down(1, 1, lower)
    chain(ring - 2)
    for k in range(2, tp):
        relay(1, k)
    for k in range(max(2, tp - 1), tp):
        settle(0, k)
        arrivals(k, project_states)

    attend()
    send_attended()

    square(0, range(tp))
    for k in range(1, tp):
        settle(1, k)
        arrivals(k, project_cot)
    grad_values()
    send_grads()
    each(0, ring - 1, total)
    send_totals()
    square(1, range(tp))
    multiply_beside(0)
    pass_attended()
    sums[...] = jnp.zeros_like(sums)
    weigh(me, near[1], dot(att_own[...], att_own[...], NT))
    weigh(me, near[0], dot(gv_own[...], gv_own[...], NT))

    @pl.when(core == 0)
    def _():
        g_beside().wait_recv()
        weigh(partner, near[2], dot(gv_own[...], gb_in[...], NT))

    each(1, far, overlap_attended)
    overlap_far_attended()
    multiply_beside(1)

    @pl.when(core == 1)
    def _():
        a_beside().wait_recv()
        weigh(partner, near[2], dot(att_own[...], ab_in[...], NT))

    each(1, far, overlap_grads)
    overlap_far_grads()
    each(1, far, score_near)
    totals_here(ring - 2)
    score(ring - 2, far)

    row_at = lax.broadcasted_iota(jnp.int32, (n, lanes), 0)
    spot_at = lax.broadcasted_iota(jnp.int32, (n, lanes), 1)
    pairs = jnp.sum(sums[...], axis=1, keepdims=True)[:n]
    t2[col * n + me] = jnp.sum(
        jnp.where(row_at == spot_at, pairs, 0.0), axis=0, keepdims=True
    )

    def send_scalars(plane, o):
        mine = t2.at[col * n + me]
        to = {"seq": (me + o) % n, "tp": plane}
        remote(mine, mine, r2_snd.at[0], r2_rcv.at[0], to).start()

    for t in range(tp):
        plane = jnp.where(col >= mid, t, last - t)
        each(1, n, lambda o: send_scalars(plane, o))
        pl.when(plane != col)(lambda: send_scalars(plane, 0))

    for k in range(1, tp):
        for which in range(2):
            for h in range(HALVES):
                if k == 1:
                    pl.when(sends_up(k))(lambda: up(which, k, h).wait_send())
                    pl.when(sends_down(k))(lambda: down(which, k, h).wait_send())
                else:
                    lasts_up, lasts_down = ends_up(which, k - 1), ends_down(which, k - 1)
                    pl.when(sends_up(k) & jnp.logical_not(lasts_up))(
                        lambda: up(which, k, h).wait_send()
                    )
                    pl.when(sends_down(k) & jnp.logical_not(lasts_down))(
                        lambda: down(which, k, h).wait_send()
                    )
    pl.when((core == 1) & jnp.logical_not(edge))(last_relays)

    def drain_near(d):
        for c in (x_copy(d), c_copy(d), x_pass(d), c_pass(d), a_copy(d), a_pass(d)):
            c.wait_send()
        for other in range(2):
            g_copy(d, other).wait_send()

    each(1, far, drain_near)
    far_copy(states_ref).wait_send()
    far_pass().wait_send()
    for slot in range(tp):
        beside(0, slot).wait_send()
    pl.when(chip >= far)(lambda: a_far().wait_send())
    pl.when(core == 0)(lambda: a_beside().wait_send())
    pl.when(core == 1)(lambda: g_beside().wait_send())

    @pl.when(low_chip)
    def _():
        a_far_pass().wait_send()
        for other in range(2):
            g_far(other).wait_send()

    def drain_sums(g):
        inner(g, lambda c: c.wait_send())
        outer(g, lambda c: c.wait_send())

    each(0, ring - 1, drain_sums)
    others = t2.at[pl.ds(0, n * tp - 1)]
    everyone = remote(others, others, r2_snd.at[0], r2_rcv.at[0], {"seq": partner})
    everyone.wait_recv()
    table = t2[pl.ds(0, n)].reshape(n, lanes)
    for q in range(1, tp):
        table = table + t2[pl.ds(q * n, n)].reshape(n, lanes)
    rank, spot = row_at, spot_at
    eye = rank == spot
    column = jnp.sum(jnp.where(spot == me, table, 0.0), axis=1, keepdims=True)
    theirs = eye & (rank != me)
    mirrored = jnp.sum(jnp.where(theirs, column, 0.0), axis=0, keepdims=True)
    own = jnp.sum(jnp.where(rank == me, table, 0.0), axis=0, keepdims=True)
    diag = jnp.sum(jnp.where(eye, table, 0.0), axis=0, keepdims=True)
    own_diag = jnp.sum(jnp.where(lane_at == me, diag, 0.0), axis=1, keepdims=True)
    gram = (own + mirrored) / jnp.sqrt(own_diag * diag)
    out_ref[...] = gram[:, :n]
    everyone.wait_send()


def on_device(n, tp, states, cotangent, wq, wk, wv, wo):
    seq_dev, length, width = states.shape
    assert seq_dev == 1 and n % 4 == 0 and length == LANES and tp > 1
    kv = wk.shape[1]
    ring = n // 2
    far = ring // 2
    near = max(far - 1, 1)
    tiles = 2 * (ring - 1)
    lanes = -(-n // LANES) * LANES
    cos, sin = rope_tables(length)
    vmem = pl.BlockSpec(memory_space=pltpu.VMEM)
    hbm = pl.BlockSpec(memory_space=pl.ANY)
    sem = pltpu.SemaphoreType.DMA

    def half(*shape):
        return pltpu.VMEM(shape, BF16)

    def wide(*shape):
        return pltpu.VMEM(shape, F32)

    return pl.pallas_call(
        functools.partial(kernel, n, tp),
        out_shape=pltpu.VMEM((1, n), F32),
        in_specs=[hbm] * 8,
        out_specs=vmem,
        scratch_shapes=[
            half(2, length, width),
            wide(2, length, LANES),
            half(tp - 1, length, width),
            half(tp - 1, length, width),
            half(tp * width, wq.shape[1] + 2 * kv),
            half(wo.shape[0], tp * width),
            wide(length, wq.shape[1] + 2 * kv),
            wide(length, wo.shape[0]),
            half(2 * near, length, width),
            half(2 * near, length, width),
            half(2, length, width),
            half(tp, length, width),
            half(length, width),
            half(2 * near, length, width),
            half(2, length, width),
            half(length, width),
            half(length, kv),
            half(2 * near, length, kv),
            half(2, length, kv),
            half(length, kv),
            half(width // HEAD_DIM, length, length),
            half(tiles, length, length),
            half(tiles, length, length),
            half(tiles, length, length),
            half(tiles, length, length),
            wide(3, length, length),
            wide(ring - 1, length, 2 * length),
            wide(-(-n // 8) * 8, LANES),
            wide(tp * n, 1, lanes),
            sem((2,)),
            pltpu.SemaphoreType.REGULAR,
            sem((2,)),
            sem((1,)),
            sem((HALVES,)),
            sem((2, tp - 1, HALVES)),
            sem((2, near)),
            sem((1,)),
            sem((2, near)),
            sem((1,)),
            sem((3,)),
            sem((far,)),
            sem((far,)),
            sem((far,)),
            sem((ring - 1,)),
            sem((ring - 1,)),
            sem((ring - 1,)),
            sem((1,)),
            sem((1,)),
        ],
        compiler_params=pltpu.CompilerParams(
            collective_id=0, has_side_effects=True, vmem_limit_bytes=60 * 1024 * 1024
        ),
        name="ntk_gram",
    )(
        states.reshape(length, width), cotangent.reshape(length, width),
        jnp.asarray(cos), jnp.asarray(sin), wq, wk, wv, wo,
    )


def solution(mesh):
    in_specs = (
        P("seq", None, "tp"),
        P("seq", None, "tp"),
        P(None, "tp"),
        P(None, "tp"),
        P(None, "tp"),
        P("tp", None),
    )
    return jax.shard_map(
        functools.partial(on_device, mesh.shape["seq"], mesh.shape["tp"]),
        mesh=mesh, in_specs=in_specs, out_specs=P("seq", None), check_vma=False,
    )
```

```python
import functools

import jax
import jax.numpy as jnp
import numpy as np
from jax import lax
from jax.experimental import pallas as pl
from jax.experimental.pallas import tpu as pltpu
from jax.sharding import PartitionSpec as P

HEADS = 32
KV_HEADS = 8
HEAD_DIM = 64
THETA = 500000.0
LANES = 128
HALVES = 2
GROUP = HEADS // KV_HEADS
F32, BF16 = jnp.float32, jnp.bfloat16

NT = (((1,), (1,)), ((), ()))
TN = (((0,), (0,)), ((), ()))


def rope_tables(length):
    half = HEAD_DIM // 2
    freqs = np.float32(THETA) ** (-(np.arange(half, dtype=np.float32) * np.float32(2.0 / HEAD_DIM)))
    angles = np.arange(length, dtype=np.float32)[:, None] * freqs[None, :].astype(np.float32)
    cos, sin = np.cos(angles), np.sin(angles)
    return (
        np.concatenate([cos, cos] * 2, axis=1).astype(np.float32),
        np.concatenate([-sin, sin] * 2, axis=1).astype(np.float32),
    )


def dot(a, b, dims=None):
    if dims is None:
        return jnp.dot(a, b, preferred_element_type=F32)
    return lax.dot_general(a, b, dims, preferred_element_type=F32)


def place_of(index, n):
    if n % 8:
        return index
    block, rest = index // 8, index % 8
    row, col, core = rest // 4, (rest // 2) % 2, rest % 2
    return block * 8 + 2 * (2 * row + (row + col) % 2) + core


def index_at(place, n):
    if n % 8:
        return place
    block, rest = place // 8, place % 8
    spot, core = rest // 2, rest % 2
    row = spot // 2
    return block * 8 + 2 * (2 * row + (row + spot) % 2) + core


def kernel(
    n, tp,
    states_hbm, cot_hbm, cos_hbm, sin_hbm, wq_hbm, wk_hbm, wv_hbm, wo_hbm,
    out_ref,
    own, tables, xs, cs, wqkv, wob, qkv_acc, g_acc,
    x_in, c_in, d_in, b_in, att, a_in, ad_in, gv, g_in, gd_in,
    probs, ad, rin, xin, full, near, over, sums, t2,
    in_sem, clear_sem, w_sem, snd, last_snd, z_rcv, p_rcv, pd_rcv, pair_rcv, b_rcv,
    a_rcv, g_rcv, r_rcv, s_rcv, o_rcv, r2_snd, r2_rcv,
):
    states_ref, cot_ref = own.at[0, 0], own.at[1, 0]
    att_own, gv_own = att.at[0], gv.at[0]
    length, width = states_ref.shape
    q_cols = wq_hbm.shape[1]
    kv_cols = wk_hbm.shape[1]
    ring = n // 2
    far = ring // 2
    mid = tp // 2
    hrows = length // HALVES
    lanes = t2.shape[2] // 2
    me = lax.axis_index("seq")
    col = lax.axis_index("tp")
    place = place_of(me, n)
    chip, core = place // 2, place % 2
    low_chip = chip < far
    last = tp - 1

    def device(hop, c):
        return index_at(2 * ((chip + hop + ring) % ring) + c, n)

    partner = device(0, 1 - core)

    def each(lo, hi, body):
        if hi - lo <= 8:
            for i in range(lo, hi):
                body(i)
        else:
            lax.fori_loop(lo, hi, lambda i, c: (body(i), c)[1], 0)

    def remote(src, dst, snd, rcv, to):
        return pltpu.make_async_remote_copy(
            src_ref=src, dst_ref=dst, send_sem=snd, recv_sem=rcv, device_id=to
        )

    local = pltpu.make_async_copy
    input_copies = [
        local(states_hbm, states_ref, in_sem.at[0]),
        local(cot_hbm, cot_ref, in_sem.at[0]),
        local(cos_hbm, tables.at[0], in_sem.at[1]),
        local(sin_hbm, tables.at[1], in_sem.at[1]),
    ]
    kv_at = q_cols + kv_cols
    weight_copies = [
        local(wq_hbm, wqkv.at[:, pl.ds(0, q_cols)], w_sem.at[0]),
        local(wk_hbm, wqkv.at[:, pl.ds(q_cols, kv_cols)], w_sem.at[0]),
        local(wv_hbm, wqkv.at[:, pl.ds(kv_at, kv_cols)], w_sem.at[0]),
        local(wo_hbm, wob, w_sem.at[1]),
    ]

    barrier = pltpu.get_barrier_semaphore()
    pl.when(col > 0)(
        lambda: pl.semaphore_signal(barrier, inc=1, device_id={"tp": col - 1})
    )
    pl.when(col < last)(
        lambda: pl.semaphore_signal(barrier, inc=1, device_id={"tp": col + 1})
    )
    each(1, n, lambda o: pl.semaphore_signal(barrier, inc=1, device_id={"seq": (me + o) % n}))
    for c in input_copies:
        c.start()
    local(own.at[0], own.at[0], in_sem.at[0]).wait()
    ends = (col == 0).astype(jnp.int32) + (col == last).astype(jnp.int32)
    pl.semaphore_wait(barrier, n + 1 - ends)

    inputs = (states_ref, cot_ref)
    held = (xs, cs)

    def rows_of(h):
        return pl.ds(h * hrows, hrows)

    def up(which, k, h, sem=None):
        src = inputs[which] if k == 1 else held[which].at[k - 2]
        return remote(
            src.at[rows_of(h), :], held[which].at[k - 1, rows_of(h), :],
            snd.at[0] if sem is None else sem, z_rcv.at[which, k - 1, h], {"tp": (col + 1) % tp},
        )

    def down(which, k, h, sem=None):
        src = inputs[which] if k == 1 else held[which].at[tp - k]
        return remote(
            src.at[rows_of(h), :], held[which].at[tp - k - 1, rows_of(h), :],
            snd.at[0] if sem is None else sem, z_rcv.at[which, tp - k - 1, h],
            {"tp": (col + tp - 1) % tp},
        )

    def sends_up(k):
        return (col >= k - 1) & (col < last)

    def sends_down(k):
        return (col + k - 1 < tp) & (col > 0)

    def landed(which, slot, h):
        remote(
            inputs[which].at[rows_of(h), :], held[which].at[slot - 1, rows_of(h), :],
            snd.at[0], z_rcv.at[which, slot - 1, h], {"tp": (col + 1) % tp},
        ).wait_recv()

    def begin_up(which):
        for h in range(HALVES):
            up(which, 1, h).start()

    def begin_down(which):
        for h in range(HALVES):
            down(which, 1, h).start()

    def ends_up(which, k):
        return (which == 1) & (k == col) & (col >= mid)

    def ends_down(which, k):
        return (which == 1) & (k == last - col) & (col < mid)

    def relay_up(which, k, side):
        @pl.when((col >= k) & (col < last) & side)
        def _():
            for h in range(HALVES):
                landed(which, k, h)
                ends = ends_up(which, k)
                pl.when(ends)(lambda: up(which, k + 1, h, last_snd.at[h]).start())
                pl.when(jnp.logical_not(ends))(lambda: up(which, k + 1, h).start())

    def relay_down(which, k, side):
        @pl.when((col + k < tp) & (col > 0) & side)
        def _():
            for h in range(HALVES):
                landed(which, tp - k, h)
                ends = ends_down(which, k)
                pl.when(ends)(lambda: down(which, k + 1, h, last_snd.at[h]).start())
                pl.when(jnp.logical_not(ends))(lambda: down(which, k + 1, h).start())

    def relay_first():
        for h in range(HALVES):
            @pl.when((col > 0) & (col < last))
            def _():
                landed(0, 1, h)
                up(0, 2, h).start()
                landed(0, tp - 1, h)
                down(0, 2, h).start()

    def relay(which, k):
        relay_up(which, k, col < mid)
        relay_down(which, k, col >= mid)
        relay_up(which, k, col >= mid)
        relay_down(which, k, col < mid)

    def settle(which, k):
        for h in range(HALVES):
            pl.when((col >= k) & (col == last))(lambda: landed(which, k, h))
            pl.when((col + k < tp) & (col == 0))(lambda: landed(which, tp - k, h))

    def arrivals(k, body):
        pl.when(col >= k)(lambda: body(k))
        pl.when(col + k < tp)(lambda: body(tp - k))

    def follow(k):
        pl.when((col == k) & (col < last))(lambda: begin_up(1))
        pl.when((jnp.minimum(last - col, 1) == k) & (col > 0))(lambda: begin_down(1))

    pl.when(col < last)(lambda: begin_up(0))
    pl.when(col > 0)(lambda: begin_down(0))
    follow(0)

    def x_copy(d):
        return remote(
            states_ref, x_in.at[d - 1], snd.at[0], p_rcv.at[0, d - 1],
            {"seq": device(-d, core)},
        )

    def c_copy(d):
        return remote(
            cot_ref, c_in.at[d - 1], snd.at[0], p_rcv.at[1, d - 1],
            {"seq": device(d, core)},
        )

    def far_copy(src):
        return remote(
            src, d_in, snd.at[0], pd_rcv.at[0], {"seq": device(far, core)}
        )

    def pair_copy(which):
        return remote(
            own.at[which, 0], own.at[which, 1], snd.at[0], pair_rcv.at[0], {"seq": partner}
        )

    def start_near(d):
        x_copy(d).start()
        c_copy(d).start()

    for which in range(2):
        pair_copy(which).start()
    each(1, far, start_near)
    pl.when(low_chip)(lambda: far_copy(states_ref).start())
    pl.when(chip >= far)(lambda: far_copy(cot_ref).start())
    for c in weight_copies:
        c.start()

    def own_block(which, slot):
        return inputs[which] if slot == 0 else held[which].at[slot - 1]

    def beside(which, slot):
        return remote(
            own_block(which, slot), b_in.at[slot], snd.at[0], b_rcv.at[0],
            {"seq": partner},
        )

    def square(which, slots):
        acc = None
        for slot in slots:
            x = own_block(which, slot)[...]
            piece = dot(x, x, NT)
            acc = piece if acc is None else acc + piece
        near[which] = acc

    def hand_over(which, slot):
        pl.when(core == 1 - which)(lambda: beside(which, slot).start())

    def multiply_beside(which):
        @pl.when(core == which)
        def _():
            acc = None
            remote(b_in, b_in, snd.at[0], b_rcv.at[0], {"seq": partner}).wait_recv()
            for slot in range(tp):
                piece = dot(own_block(which, slot)[...], b_in[slot], NT)
                acc = piece if acc is None else acc + piece
            near[2] = acc

    def features(slot):
        return pl.ds(pl.multiple_of(((col - slot + tp) % tp) * width, width), width)

    def project_states(slot):
        if slot == 0:
            local(wqkv, wqkv, w_sem.at[0]).wait()
        hand_over(0, slot)
        piece = dot(own_block(0, slot)[...], wqkv[features(slot), :])
        qkv_acc[...] = piece if slot == 0 else qkv_acc[...] + piece

    def project_cot(slot):
        if slot == 0:
            local(wob, wob, w_sem.at[1]).wait()
        hand_over(1, slot)
        piece = dot(own_block(1, slot)[...], wob[:, features(slot)], NT)
        g_acc[...] = piece if slot == 0 else g_acc[...] + piece

    def inner(g, act):
        part = pl.ds(2 * g, 2)

        def copy(dst, rcv, to):
            return remote(ad.at[part], dst.at[part], snd.at[0], rcv.at[g], {"tp": to})

        pl.when(col < mid - 1)(lambda: act(copy(rin, r_rcv, (col + 1) % tp)))
        pl.when(col > mid)(lambda: act(copy(rin, r_rcv, (col + tp - 1) % tp)))
        pl.when(col == mid - 1)(lambda: act(copy(xin, s_rcv, (col + 1) % tp)))
        pl.when(col == mid)(lambda: act(copy(xin, s_rcv, (col + tp - 1) % tp)))

    def outer(g, act):
        part = pl.ds(2 * g, 2)

        def copy(to):
            return remote(full.at[part], full.at[part], snd.at[0], o_rcv.at[g], {"tp": to})

        pl.when((col < mid) & (col > 0))(lambda: act(copy((col + tp - 1) % tp)))
        pl.when((col >= mid) & (col < last))(lambda: act(copy((col + 1) % tp)))

    def waits_on(buf, rcv, g):
        part = pl.ds(2 * g, 2)
        remote(
            buf.at[part], buf.at[part], snd.at[0], rcv.at[g], {"tp": (col + 1) % tp}
        ).wait_recv()

    edge = (col == 0) | (col == last)
    central = (col == mid - 1) | (col == mid)

    def publish(g):
        pl.when(edge)(lambda: inner(g, lambda c: c.start()))

    def chain(g):
        part = pl.ds(2 * g, 2)

        @pl.when(jnp.logical_not(edge))
        def _():
            waits_on(rin, r_rcv, g)
            ad[part] = (ad[part].astype(F32) + rin[part].astype(F32)).astype(BF16)
            inner(g, lambda c: c.start())

    def total(g):
        part = pl.ds(2 * g, 2)

        @pl.when(central)
        def _():
            waits_on(xin, s_rcv, g)
            full[part] = (ad[part].astype(F32) + xin[part].astype(F32)).astype(BF16)

    def last_relays():
        for h in range(HALVES):
            @pl.when((col >= mid) & (col < last))
            def _():
                remote(
                    held[1].at[col - 1, rows_of(h), :], held[1].at[col, rows_of(h), :],
                    last_snd.at[h], z_rcv.at[1, col, h], {"tp": (col + 1) % tp},
                ).wait_send()

            @pl.when((col < mid) & (col > 0))
            def _():
                remote(
                    held[1].at[col, rows_of(h), :], held[1].at[col - 1, rows_of(h), :],
                    last_snd.at[h], z_rcv.at[1, col - 1, h],
                    {"tp": (col + tp - 1) % tp},
                ).wait_send()

    def total_out(g):
        total(g)
        pl.when(central)(lambda: outer(g, lambda c: c.start()))

    def clear_links():
        @pl.when(jnp.logical_not(edge) & (core == 0))
        def _():
            last_relays()
            pl.semaphore_signal(clear_sem, inc=1, device_id={"seq": partner})

        pl.when(jnp.logical_not(edge) & (core == 1))(lambda: pl.semaphore_wait(clear_sem, 1))

    def totals_here(g):
        @pl.when(jnp.logical_not(central))
        def _():
            waits_on(full, o_rcv, g)
            pl.when(jnp.logical_not(edge))(lambda: outer(g, lambda c: c.start()))

    def two(pair, other):
        return dot(other[...], pair[...].reshape(2 * length, pair.shape[2]), NT)

    def put(g, tiles):
        ad[2 * g] = tiles[:, :length].astype(BF16)
        ad[2 * g + 1] = tiles[:, length:].astype(BF16)
        publish(g)

    def multiply_near(d):
        x_copy(d).wait_recv()
        put(2 * d - 2, two(own.at[0], x_in.at[d - 1]))
        c_copy(d).wait_recv()
        put(2 * d - 1, two(own.at[1], c_in.at[d - 1]))

    def multiply_far():
        far_copy(states_ref).wait_recv()
        pl.when(low_chip)(lambda: put(ring - 2, two(own.at[1], d_in)))
        pl.when(chip >= far)(lambda: put(ring - 2, two(own.at[0], d_in)))

    lane = lax.broadcasted_iota(jnp.int32, (length, LANES), 1)
    low = lane < HEAD_DIM
    first = lane % HEAD_DIM < HEAD_DIM // 2
    local(tables, tables, in_sem.at[1]).wait()
    cos, sin = tables[0], tables[1]
    causal = lax.broadcasted_iota(jnp.int32, (length, length), 0) >= lax.broadcasted_iota(
        jnp.int32, (length, length), 1
    )

    def swap(v):
        return pltpu.roll(v, HEAD_DIM, 1)

    def rope(v):
        turned = jnp.where(
            first, pltpu.roll(v, LANES - HEAD_DIM // 2, 1), pltpu.roll(v, HEAD_DIM // 2, 1)
        )
        return v * cos + turned * sin

    def halves(v):
        other = swap(v)
        zero = jnp.zeros_like(v)
        return (
            (jnp.where(low, v, zero).astype(BF16), jnp.where(low, zero, other).astype(BF16)),
            (jnp.where(low, other, zero).astype(BF16), jnp.where(low, zero, v).astype(BF16)),
        )

    blocks = [
        (b, g, (b * 2 + g) * (GROUP // 2) + pair)
        for b in range(kv_cols // LANES)
        for g in range(2)
        for pair in range(GROUP // 2)
    ]

    def attend():
        for b in range(kv_cols // LANES):
            kcut = slice(q_cols + b * LANES, q_cols + (b + 1) * LANES)
            vcut = slice(kv_at + b * LANES, kv_at + (b + 1) * LANES)
            keys = [jnp.concatenate(h, axis=0) for h in halves(rope(qkv_acc[:, kcut]))]
            values = [jnp.concatenate(h, axis=0) for h in halves(qkv_acc[:, vcut])]
            for of, g, at in blocks:
                if of != b:
                    continue
                cut = slice(at * LANES, (at + 1) * LANES)
                q = rope(qkv_acc[:, cut]).astype(BF16)
                both = dot(q, keys[g], NT) * HEAD_DIM ** (-0.5)
                weights = []
                for side in range(2):
                    s = jnp.where(causal, both[:, side * length : (side + 1) * length], -jnp.inf)
                    e = jnp.exp(s - jnp.max(s, axis=1, keepdims=True))
                    p = (e / jnp.sum(e, axis=1, keepdims=True)).astype(BF16)
                    probs[2 * at + side] = p
                    weights.append(p)
                a = dot(jnp.concatenate(weights, axis=1), values[g])
                att_own[:, cut] = a.astype(BF16)

    def grad_values():
        sums = {}
        for b, g, at in blocks:
            ga = g_acc[:, at * LANES : (at + 1) * LANES].astype(BF16)
            for side in range(2):
                u = dot(probs[2 * at + side], ga, TN)
                key = (b, g, side)
                sums[key] = sums[key] + u if key in sums else u
        for b in range(kv_cols // LANES):
            grad = jnp.where(
                low,
                sums[b, 0, 0] + swap(sums[b, 0, 1]),
                swap(sums[b, 1, 0]) + sums[b, 1, 1],
            )
            gv_own[:, b * LANES : (b + 1) * LANES] = grad.astype(BF16)

    def a_copy(d):
        return remote(
            att_own, a_in.at[d - 1], snd.at[0], a_rcv.at[d - 1], {"seq": device(d, core)}
        )

    def a_far():
        return remote(
            att_own, ad_in, snd.at[0], a_rcv.at[far - 1], {"seq": device(far, core)}
        )

    def a_beside():
        return remote(att_own, att.at[1], snd.at[0], b_rcv.at[1], {"seq": partner})

    def send_attended():
        each(1, far, lambda d: a_copy(d).start())
        pl.when(chip >= far)(lambda: a_far().start())
        a_beside().start()

    def g_copy(d):
        return remote(
            gv_own, g_in.at[d - 1], snd.at[0], g_rcv.at[d - 1], {"seq": device(-d, core)}
        )

    def g_far():
        return remote(
            gv_own, gd_in, snd.at[0], g_rcv.at[far - 1], {"seq": device(far, core)}
        )

    def g_beside():
        return remote(gv_own, gv.at[1], snd.at[0], b_rcv.at[2], {"seq": partner})

    def send_grads():
        pl.when(low_chip)(lambda: g_far().start())
        each(1, far, lambda d: g_copy(d).start())
        g_beside().start()

    lane_at = lax.broadcasted_iota(jnp.int32, (1, lanes), 1)

    def weigh(row, source, d, b):
        at = pl.ds(source, 1)
        sums[row, at, :] = sums[row, at, :] + jnp.sum(d * b, axis=0, keepdims=True)

    def overlap_attended(d):
        a_copy(d).wait_recv()
        over[2 * d - 1] = two(att, a_in.at[d - 1])

    def overlap_grads(d):
        g_copy(d).wait_recv()
        over[2 * d - 2] = two(gv, g_in.at[d - 1])

    def overlap_far_attended():
        @pl.when(low_chip)
        def _():
            a_far().wait_recv()
            over[ring - 2] = two(att, ad_in)

    def overlap_far_grads():
        @pl.when(chip >= far)
        def _():
            g_far().wait_recv()
            over[ring - 2] = two(gv, gd_in)

    def score(g, hop):
        for row in range(2):
            weigh(
                row, device(hop, core), full[2 * g + row].astype(F32),
                over[g, :, row * length : (row + 1) * length],
            )

    def score_near(d):
        totals_here(2 * d - 2)
        score(2 * d - 2, d)
        totals_here(2 * d - 1)
        score(2 * d - 1, -d)

    lower, upper, anywhere = col < mid, col >= mid, col >= 0
    project_states(0)
    relay_first()
    follow(1)
    remote(own.at[0], own.at[0], snd.at[0], pair_rcv.at[0], {"seq": partner}).wait_recv()
    settle(0, 1)
    arrivals(1, project_states)
    if tp > 2:
        relay_up(0, 2, anywhere)
        follow(2)
    each(1, far, multiply_near)
    relay_up(1, 1, lower)
    relay_down(1, 1, upper)
    if tp > 2:
        relay_down(0, 2, anywhere)
    for k in range(3, tp):
        relay(0, k)
        follow(k)
    project_cot(0)
    relay_up(1, 1, upper)
    for k in range(2, tp - 1):
        settle(0, k)
        arrivals(k, project_states)

    each(0, ring - 2, chain)
    multiply_far()
    relay_down(1, 1, lower)

    @pl.when(jnp.logical_not(edge))
    def _():
        attend()
        send_attended()

    chain(ring - 2)
    for k in range(2, tp):
        relay(1, k)
    for k in range(max(2, tp - 1), tp):
        settle(0, k)
        arrivals(k, project_states)

    @pl.when(edge)
    def _():
        attend()
        send_attended()

    square(0, range(tp))
    for k in range(1, tp):
        settle(1, k)
        arrivals(k, project_cot)
    grad_values()
    send_grads()
    pl.when(core == 0)(lambda: each(0, ring - 1, total_out))
    pl.when(core == 1)(lambda: each(0, ring - 1, total))
    clear_links()
    pl.when((core == 1) & central)(
        lambda: each(0, ring - 1, lambda g: outer(g, lambda c: c.start()))
    )
    square(1, range(tp))
    multiply_beside(0)
    a_beside().wait_recv()
    sums[...] = jnp.zeros_like(sums)
    weigh(0, me, near[1], dot(att_own[...], att_own[...], NT))
    weigh(0, me, near[0], dot(gv_own[...], gv_own[...], NT))

    each(1, far, overlap_attended)
    overlap_far_attended()
    multiply_beside(1)

    @pl.when(core == 1)
    def _():
        weigh(0, partner, near[2], dot(att_own[...], att[1], NT))

    g_beside().wait_recv()

    @pl.when(core == 0)
    def _():
        weigh(0, partner, near[2], dot(gv_own[...], gv[1], NT))

    each(1, far, overlap_grads)
    overlap_far_grads()
    each(1, far, score_near)
    totals_here(ring - 2)
    score(ring - 2, far)

    row_at = lax.broadcasted_iota(jnp.int32, (n, lanes), 0)
    spot_at = lax.broadcasted_iota(jnp.int32, (n, lanes), 1)
    for row in range(2):
        pairs = jnp.sum(sums[row], axis=1, keepdims=True)[:n]
        t2[col * n + me, :, row * lanes : (row + 1) * lanes] = jnp.sum(
            jnp.where(row_at == spot_at, pairs, 0.0), axis=0, keepdims=True
        )

    def send_scalars(plane, o):
        mine = t2.at[col * n + me]
        to = {"seq": (me + o) % n, "tp": plane}
        remote(mine, mine, r2_snd.at[0], r2_rcv.at[0], to).start()

    for t in range(tp):
        plane = jnp.where(col >= mid, t, last - t)
        each(1, n, lambda o: send_scalars(plane, o))
        pl.when(plane != col)(lambda: send_scalars(plane, 0))

    for k in range(1, tp):
        for which in range(2):
            for h in range(HALVES):
                if k == 1:
                    pl.when(sends_up(k))(lambda: up(which, k, h).wait_send())
                    pl.when(sends_down(k))(lambda: down(which, k, h).wait_send())
                else:
                    lasts_up, lasts_down = ends_up(which, k - 1), ends_down(which, k - 1)
                    pl.when(sends_up(k) & jnp.logical_not(lasts_up))(
                        lambda: up(which, k, h).wait_send()
                    )
                    pl.when(sends_down(k) & jnp.logical_not(lasts_down))(
                        lambda: down(which, k, h).wait_send()
                    )
    pl.when((core == 1) & jnp.logical_not(edge))(last_relays)

    def drain_near(d):
        for c in (x_copy(d), c_copy(d), a_copy(d), g_copy(d)):
            c.wait_send()

    each(1, far, drain_near)
    far_copy(states_ref).wait_send()
    for c in (pair_copy(0), pair_copy(1), a_beside(), g_beside()):
        c.wait_send()
    for slot in range(tp):
        beside(0, slot).wait_send()
    pl.when(chip >= far)(lambda: a_far().wait_send())
    pl.when(low_chip)(lambda: g_far().wait_send())

    def drain_sums(g):
        inner(g, lambda c: c.wait_send())
        outer(g, lambda c: c.wait_send())

    each(0, ring - 1, drain_sums)
    others = t2.at[pl.ds(0, n * tp - 1)]
    everyone = remote(others, others, r2_snd.at[0], r2_rcv.at[0], {"seq": partner})
    everyone.wait_recv()
    both = t2[pl.ds(0, n)].reshape(n, 2 * lanes)
    for q in range(1, tp):
        both = both + t2[pl.ds(q * n, n)].reshape(n, 2 * lanes)
    aside = both[:, lanes:]
    aside = jnp.where(row_at % 2 == 0, pltpu.roll(aside, n - 1, 0), pltpu.roll(aside, 1, 0))
    table = both[:, :lanes] + aside
    rank, spot = row_at, spot_at
    eye = rank == spot
    column = jnp.sum(jnp.where(spot == me, table, 0.0), axis=1, keepdims=True)
    theirs = eye & (rank != me)
    mirrored = jnp.sum(jnp.where(theirs, column, 0.0), axis=0, keepdims=True)
    own = jnp.sum(jnp.where(rank == me, table, 0.0), axis=0, keepdims=True)
    diag = jnp.sum(jnp.where(eye, table, 0.0), axis=0, keepdims=True)
    own_diag = jnp.sum(jnp.where(lane_at == me, diag, 0.0), axis=1, keepdims=True)
    gram = (own + mirrored) / jnp.sqrt(own_diag * diag)
    out_ref[...] = gram[:, :n]
    everyone.wait_send()


def on_device(n, tp, states, cotangent, wq, wk, wv, wo):
    seq_dev, length, width = states.shape
    assert seq_dev == 1 and n % 4 == 0 and length == LANES and tp > 1
    kv = wk.shape[1]
    ring = n // 2
    far = ring // 2
    near = max(far - 1, 1)
    tiles = 2 * (ring - 1)
    lanes = -(-n // LANES) * LANES
    cos, sin = rope_tables(length)
    vmem = pl.BlockSpec(memory_space=pltpu.VMEM)
    hbm = pl.BlockSpec(memory_space=pl.ANY)
    sem = pltpu.SemaphoreType.DMA

    def half(*shape):
        return pltpu.VMEM(shape, BF16)

    def wide(*shape):
        return pltpu.VMEM(shape, F32)

    return pl.pallas_call(
        functools.partial(kernel, n, tp),
        out_shape=pltpu.VMEM((1, n), F32),
        in_specs=[hbm] * 8,
        out_specs=vmem,
        scratch_shapes=[
            half(2, 2, length, width),
            wide(2, length, LANES),
            half(tp - 1, length, width),
            half(tp - 1, length, width),
            half(tp * width, wq.shape[1] + 2 * kv),
            half(wo.shape[0], tp * width),
            wide(length, wq.shape[1] + 2 * kv),
            wide(length, wo.shape[0]),
            half(near, length, width),
            half(near, length, width),
            half(length, width),
            half(tp, length, width),
            half(2, length, width),
            half(near, length, width),
            half(length, width),
            half(2, length, kv),
            half(near, length, kv),
            half(length, kv),
            half(width // HEAD_DIM, length, length),
            half(tiles, length, length),
            half(tiles, length, length),
            half(tiles, length, length),
            half(tiles, length, length),
            wide(3, length, length),
            wide(ring - 1, length, 2 * length),
            wide(2, -(-n // 8) * 8, LANES),
            wide(tp * n, 1, 2 * lanes),
            sem((2,)),
            pltpu.SemaphoreType.REGULAR,
            sem((2,)),
            sem((1,)),
            sem((HALVES,)),
            sem((2, tp - 1, HALVES)),
            sem((2, near)),
            sem((1,)),
            sem((1,)),
            sem((3,)),
            sem((far,)),
            sem((far,)),
            sem((ring - 1,)),
            sem((ring - 1,)),
            sem((ring - 1,)),
            sem((1,)),
            sem((1,)),
        ],
        compiler_params=pltpu.CompilerParams(
            collective_id=0, has_side_effects=True, vmem_limit_bytes=60 * 1024 * 1024
        ),
        name="ntk_gram",
    )(
        states.reshape(length, width), cotangent.reshape(length, width),
        jnp.asarray(cos), jnp.asarray(sin), wq, wk, wv, wo,
    )


def solution(mesh):
    in_specs = (
        P("seq", None, "tp"),
        P("seq", None, "tp"),
        P(None, "tp"),
        P(None, "tp"),
        P(None, "tp"),
        P("tp", None),
    )
    return jax.shard_map(
        functools.partial(on_device, mesh.shape["seq"], mesh.shape["tp"]),
        mesh=mesh, in_specs=in_specs, out_specs=P("seq", None), check_vma=False,
    )
```

```python
import functools

import jax
import jax.numpy as jnp
import numpy as np
from jax import lax
from jax.experimental import pallas as pl
from jax.experimental.pallas import tpu as pltpu
from jax.sharding import PartitionSpec as P

HEADS = 32
KV_HEADS = 8
HEAD_DIM = 64
THETA = 500000.0
LANES = 128
HALVES = 2
GROUP = HEADS // KV_HEADS
F32, BF16 = jnp.float32, jnp.bfloat16

NT = (((1,), (1,)), ((), ()))
TN = (((0,), (0,)), ((), ()))


def rope_tables(length):
    half = HEAD_DIM // 2
    freqs = np.float32(THETA) ** (-(np.arange(half, dtype=np.float32) * np.float32(2.0 / HEAD_DIM)))
    angles = np.arange(length, dtype=np.float32)[:, None] * freqs[None, :].astype(np.float32)
    cos, sin = np.cos(angles), np.sin(angles)
    return (
        np.concatenate([cos, cos] * 2, axis=1).astype(np.float32),
        np.concatenate([-sin, sin] * 2, axis=1).astype(np.float32),
    )


def dot(a, b, dims=None):
    if dims is None:
        return jnp.dot(a, b, preferred_element_type=F32)
    return lax.dot_general(a, b, dims, preferred_element_type=F32)


def place_of(index, n):
    if n % 8:
        return index
    block, rest = index // 8, index % 8
    row, col, core = rest // 4, (rest // 2) % 2, rest % 2
    return block * 8 + 2 * (2 * row + (row + col) % 2) + core


def index_at(place, n):
    if n % 8:
        return place
    block, rest = place // 8, place % 8
    spot, core = rest // 2, rest % 2
    row = spot // 2
    return block * 8 + 2 * (2 * row + (row + spot) % 2) + core


def kernel(
    n, tp,
    states_hbm, cot_hbm, cos_hbm, sin_hbm, wq_hbm, wk_hbm, wv_hbm, wo_hbm,
    out_ref,
    own, tables, xs, cs, wqkv, wob, qkv_acc, g_acc,
    x_in, c_in, d_in, b_in, att, a_in, ad_in, gv, g_in, gd_in,
    probs, ad, rin, xin, full, near, over, sums, t2,
    in_sem, clear_sem, w_sem, snd, last_snd, z_rcv, p_rcv, pd_rcv, pair_rcv, b_rcv,
    a_rcv, g_rcv, r_rcv, s_rcv, o_rcv, r2_snd, r2_rcv,
):
    states_ref, cot_ref = own.at[0, 0], own.at[1, 0]
    att_own, gv_own = att.at[0], gv.at[0]
    length, width = states_ref.shape
    q_cols = wq_hbm.shape[1]
    kv_cols = wk_hbm.shape[1]
    ring = n // 2
    far = ring // 2
    mid = tp // 2
    hrows = length // HALVES
    lanes = t2.shape[2] // 2
    me = lax.axis_index("seq")
    col = lax.axis_index("tp")
    place = place_of(me, n)
    chip, core = place // 2, place % 2
    low_chip = chip < far
    last = tp - 1

    def device(hop, c):
        return index_at(2 * ((chip + hop + ring) % ring) + c, n)

    partner = device(0, 1 - core)

    def each(lo, hi, body):
        if hi - lo <= 8:
            for i in range(lo, hi):
                body(i)
        else:
            lax.fori_loop(lo, hi, lambda i, c: (body(i), c)[1], 0)

    def remote(src, dst, snd, rcv, to):
        return pltpu.make_async_remote_copy(
            src_ref=src, dst_ref=dst, send_sem=snd, recv_sem=rcv, device_id=to
        )

    local = pltpu.make_async_copy
    input_copies = [
        local(states_hbm, states_ref, in_sem.at[0]),
        local(cot_hbm, cot_ref, in_sem.at[0]),
        local(cos_hbm, tables.at[0], in_sem.at[1]),
        local(sin_hbm, tables.at[1], in_sem.at[1]),
    ]
    kv_at = q_cols + kv_cols
    weight_copies = [
        local(wq_hbm, wqkv.at[:, pl.ds(0, q_cols)], w_sem.at[0]),
        local(wk_hbm, wqkv.at[:, pl.ds(q_cols, kv_cols)], w_sem.at[0]),
        local(wv_hbm, wqkv.at[:, pl.ds(kv_at, kv_cols)], w_sem.at[0]),
        local(wo_hbm, wob, w_sem.at[1]),
    ]

    barrier = pltpu.get_barrier_semaphore()
    pl.when(col > 0)(
        lambda: pl.semaphore_signal(barrier, inc=1, device_id={"tp": col - 1})
    )
    pl.when(col < last)(
        lambda: pl.semaphore_signal(barrier, inc=1, device_id={"tp": col + 1})
    )
    each(1, n, lambda o: pl.semaphore_signal(barrier, inc=1, device_id={"seq": (me + o) % n}))
    for c in input_copies:
        c.start()
    local(own.at[0], own.at[0], in_sem.at[0]).wait()
    ends = (col == 0).astype(jnp.int32) + (col == last).astype(jnp.int32)
    pl.semaphore_wait(barrier, n + 1 - ends)

    inputs = (states_ref, cot_ref)
    held = (xs, cs)

    def rows_of(h):
        return pl.ds(h * hrows, hrows)

    def up(which, k, h, sem=None):
        src = inputs[which] if k == 1 else held[which].at[k - 2]
        return remote(
            src.at[rows_of(h), :], held[which].at[k - 1, rows_of(h), :],
            snd.at[0] if sem is None else sem, z_rcv.at[which, k - 1, h], {"tp": (col + 1) % tp},
        )

    def down(which, k, h, sem=None):
        src = inputs[which] if k == 1 else held[which].at[tp - k]
        return remote(
            src.at[rows_of(h), :], held[which].at[tp - k - 1, rows_of(h), :],
            snd.at[0] if sem is None else sem, z_rcv.at[which, tp - k - 1, h],
            {"tp": (col + tp - 1) % tp},
        )

    def sends_up(k):
        return (col >= k - 1) & (col < last)

    def sends_down(k):
        return (col + k - 1 < tp) & (col > 0)

    def landed(which, slot, h):
        remote(
            inputs[which].at[rows_of(h), :], held[which].at[slot - 1, rows_of(h), :],
            snd.at[0], z_rcv.at[which, slot - 1, h], {"tp": (col + 1) % tp},
        ).wait_recv()

    def begin_up(which):
        for h in range(HALVES):
            up(which, 1, h).start()

    def begin_down(which):
        for h in range(HALVES):
            down(which, 1, h).start()

    def ends_up(which, k):
        return (which == 1) & (k == col) & (col >= mid)

    def ends_down(which, k):
        return (which == 1) & (k == last - col) & (col < mid)

    def relay_up(which, k, side):
        @pl.when((col >= k) & (col < last) & side)
        def _():
            for h in range(HALVES):
                landed(which, k, h)
                ends = ends_up(which, k)
                pl.when(ends)(lambda: up(which, k + 1, h, last_snd.at[h]).start())
                pl.when(jnp.logical_not(ends))(lambda: up(which, k + 1, h).start())

    def relay_down(which, k, side):
        @pl.when((col + k < tp) & (col > 0) & side)
        def _():
            for h in range(HALVES):
                landed(which, tp - k, h)
                ends = ends_down(which, k)
                pl.when(ends)(lambda: down(which, k + 1, h, last_snd.at[h]).start())
                pl.when(jnp.logical_not(ends))(lambda: down(which, k + 1, h).start())

    def relay_first():
        for h in range(HALVES):
            @pl.when((col > 0) & (col < last))
            def _():
                landed(0, 1, h)
                up(0, 2, h).start()
                landed(0, tp - 1, h)
                down(0, 2, h).start()

    def relay(which, k):
        relay_up(which, k, col < mid)
        relay_down(which, k, col >= mid)
        relay_up(which, k, col >= mid)
        relay_down(which, k, col < mid)

    def settle(which, k):
        for h in range(HALVES):
            pl.when((col >= k) & (col == last))(lambda: landed(which, k, h))
            pl.when((col + k < tp) & (col == 0))(lambda: landed(which, tp - k, h))

    def arrivals(k, body):
        pl.when(col >= k)(lambda: body(k))
        pl.when(col + k < tp)(lambda: body(tp - k))

    def follow(k):
        pl.when((col == k) & (col < last))(lambda: begin_up(1))
        pl.when((jnp.minimum(last - col, 1) == k) & (col > 0))(lambda: begin_down(1))

    pl.when(col < last)(lambda: begin_up(0))
    pl.when(col > 0)(lambda: begin_down(0))
    follow(0)

    def x_copy(d):
        return remote(
            states_ref, x_in.at[d - 1], snd.at[0], p_rcv.at[0, d - 1],
            {"seq": device(-d, core)},
        )

    def c_copy(d):
        return remote(
            cot_ref, c_in.at[d - 1], snd.at[0], p_rcv.at[1, d - 1],
            {"seq": device(d, core)},
        )

    def far_copy(src):
        return remote(
            src, d_in, snd.at[0], pd_rcv.at[0], {"seq": device(far, core)}
        )

    def pair_copy(which):
        return remote(
            own.at[which, 0], own.at[which, 1], snd.at[0], pair_rcv.at[0], {"seq": partner}
        )

    def start_near(d):
        x_copy(d).start()
        c_copy(d).start()

    for which in range(2):
        pair_copy(which).start()
    each(1, far, start_near)
    pl.when(low_chip)(lambda: far_copy(states_ref).start())
    pl.when(chip >= far)(lambda: far_copy(cot_ref).start())
    for c in weight_copies:
        c.start()

    def own_block(which, slot):
        return inputs[which] if slot == 0 else held[which].at[slot - 1]

    def beside(which, slot):
        return remote(
            own_block(which, slot), b_in.at[slot], snd.at[0], b_rcv.at[0],
            {"seq": partner},
        )

    def square(which, slots):
        acc = None
        for slot in slots:
            x = own_block(which, slot)[...]
            piece = dot(x, x, NT)
            acc = piece if acc is None else acc + piece
        near[which] = acc

    def hand_over(which, slot):
        pl.when(core == 1 - which)(lambda: beside(which, slot).start())

    def multiply_beside(which):
        @pl.when(core == which)
        def _():
            acc = None
            remote(b_in, b_in, snd.at[0], b_rcv.at[0], {"seq": partner}).wait_recv()
            for slot in range(tp):
                piece = dot(own_block(which, slot)[...], b_in[slot], NT)
                acc = piece if acc is None else acc + piece
            near[2] = acc

    def features(slot):
        return pl.ds(pl.multiple_of(((col - slot + tp) % tp) * width, width), width)

    def project_states(slot):
        if slot == 0:
            local(wqkv, wqkv, w_sem.at[0]).wait()
        hand_over(0, slot)
        piece = dot(own_block(0, slot)[...], wqkv[features(slot), :])
        qkv_acc[...] = piece if slot == 0 else qkv_acc[...] + piece

    def project_cot(slot):
        if slot == 0:
            local(wob, wob, w_sem.at[1]).wait()
        hand_over(1, slot)
        piece = dot(own_block(1, slot)[...], wob[:, features(slot)], NT)
        g_acc[...] = piece if slot == 0 else g_acc[...] + piece

    def inner(g, act):
        part = pl.ds(2 * g, 2)

        def copy(dst, rcv, to):
            return remote(ad.at[part], dst.at[part], snd.at[0], rcv.at[g], {"tp": to})

        pl.when(col < mid - 1)(lambda: act(copy(rin, r_rcv, (col + 1) % tp)))
        pl.when(col > mid)(lambda: act(copy(rin, r_rcv, (col + tp - 1) % tp)))
        pl.when(col == mid - 1)(lambda: act(copy(xin, s_rcv, (col + 1) % tp)))
        pl.when(col == mid)(lambda: act(copy(xin, s_rcv, (col + tp - 1) % tp)))

    def outer(g, act):
        part = pl.ds(2 * g, 2)

        def copy(to):
            return remote(full.at[part], full.at[part], snd.at[0], o_rcv.at[g], {"tp": to})

        pl.when((col < mid) & (col > 0))(lambda: act(copy((col + tp - 1) % tp)))
        pl.when((col >= mid) & (col < last))(lambda: act(copy((col + 1) % tp)))

    def waits_on(buf, rcv, g):
        part = pl.ds(2 * g, 2)
        remote(
            buf.at[part], buf.at[part], snd.at[0], rcv.at[g], {"tp": (col + 1) % tp}
        ).wait_recv()

    edge = (col == 0) | (col == last)
    central = (col == mid - 1) | (col == mid)

    def publish(g):
        pl.when(edge)(lambda: inner(g, lambda c: c.start()))

    def chain(g):
        part = pl.ds(2 * g, 2)

        @pl.when(jnp.logical_not(edge))
        def _():
            waits_on(rin, r_rcv, g)
            ad[part] = (ad[part].astype(F32) + rin[part].astype(F32)).astype(BF16)
            inner(g, lambda c: c.start())

    def total(g):
        part = pl.ds(2 * g, 2)

        @pl.when(central)
        def _():
            waits_on(xin, s_rcv, g)
            full[part] = (ad[part].astype(F32) + xin[part].astype(F32)).astype(BF16)

    def last_relays():
        for h in range(HALVES):
            @pl.when((col >= mid) & (col < last))
            def _():
                remote(
                    held[1].at[col - 1, rows_of(h), :], held[1].at[col, rows_of(h), :],
                    last_snd.at[h], z_rcv.at[1, col, h], {"tp": (col + 1) % tp},
                ).wait_send()

            @pl.when((col < mid) & (col > 0))
            def _():
                remote(
                    held[1].at[col, rows_of(h), :], held[1].at[col - 1, rows_of(h), :],
                    last_snd.at[h], z_rcv.at[1, col - 1, h],
                    {"tp": (col + tp - 1) % tp},
                ).wait_send()

    def total_out(g):
        total(g)
        pl.when(central)(lambda: outer(g, lambda c: c.start()))

    def clear_links():
        @pl.when(jnp.logical_not(edge) & (core == 0))
        def _():
            pl.semaphore_signal(clear_sem, inc=1, device_id={"seq": partner})

        pl.when(jnp.logical_not(edge) & (core == 1))(lambda: pl.semaphore_wait(clear_sem, 1))

    def totals_here(g):
        @pl.when(jnp.logical_not(central))
        def _():
            waits_on(full, o_rcv, g)
            pl.when(jnp.logical_not(edge))(lambda: outer(g, lambda c: c.start()))

    def two(pair, other):
        return dot(other[...], pair[...].reshape(2 * length, pair.shape[2]), NT)

    def put(g, tiles):
        ad[2 * g] = tiles[:, :length].astype(BF16)
        ad[2 * g + 1] = tiles[:, length:].astype(BF16)
        publish(g)

    def multiply_near(d):
        x_copy(d).wait_recv()
        put(2 * d - 2, two(own.at[0], x_in.at[d - 1]))
        c_copy(d).wait_recv()
        put(2 * d - 1, two(own.at[1], c_in.at[d - 1]))

    def multiply_far():
        far_copy(states_ref).wait_recv()
        pl.when(low_chip)(lambda: put(ring - 2, two(own.at[1], d_in)))
        pl.when(chip >= far)(lambda: put(ring - 2, two(own.at[0], d_in)))

    lane = lax.broadcasted_iota(jnp.int32, (length, LANES), 1)
    low = lane < HEAD_DIM
    first = lane % HEAD_DIM < HEAD_DIM // 2
    local(tables, tables, in_sem.at[1]).wait()
    cos, sin = tables[0], tables[1]
    causal = lax.broadcasted_iota(jnp.int32, (length, length), 0) >= lax.broadcasted_iota(
        jnp.int32, (length, length), 1
    )

    def swap(v):
        return pltpu.roll(v, HEAD_DIM, 1)

    def rope(v):
        turned = jnp.where(
            first, pltpu.roll(v, LANES - HEAD_DIM // 2, 1), pltpu.roll(v, HEAD_DIM // 2, 1)
        )
        return v * cos + turned * sin

    def halves(v):
        other = swap(v)
        zero = jnp.zeros_like(v)
        return (
            (jnp.where(low, v, zero).astype(BF16), jnp.where(low, zero, other).astype(BF16)),
            (jnp.where(low, other, zero).astype(BF16), jnp.where(low, zero, v).astype(BF16)),
        )

    blocks = [
        (b, g, (b * 2 + g) * (GROUP // 2) + pair)
        for b in range(kv_cols // LANES)
        for g in range(2)
        for pair in range(GROUP // 2)
    ]

    def attend():
        for b in range(kv_cols // LANES):
            kcut = slice(q_cols + b * LANES, q_cols + (b + 1) * LANES)
            vcut = slice(kv_at + b * LANES, kv_at + (b + 1) * LANES)
            keys = [jnp.concatenate(h, axis=0) for h in halves(rope(qkv_acc[:, kcut]))]
            values = [jnp.concatenate(h, axis=0) for h in halves(qkv_acc[:, vcut])]
            for of, g, at in blocks:
                if of != b:
                    continue
                cut = slice(at * LANES, (at + 1) * LANES)
                q = rope(qkv_acc[:, cut]).astype(BF16)
                both = dot(q, keys[g], NT) * HEAD_DIM ** (-0.5)
                weights = []
                for side in range(2):
                    s = jnp.where(causal, both[:, side * length : (side + 1) * length], -jnp.inf)
                    e = jnp.exp(s - jnp.max(s, axis=1, keepdims=True))
                    p = (e / jnp.sum(e, axis=1, keepdims=True)).astype(BF16)
                    probs[2 * at + side] = p
                    weights.append(p)
                a = dot(jnp.concatenate(weights, axis=1), values[g])
                att_own[:, cut] = a.astype(BF16)

    def grad_values():
        sums = {}
        for b, g, at in blocks:
            ga = g_acc[:, at * LANES : (at + 1) * LANES].astype(BF16)
            for side in range(2):
                u = dot(probs[2 * at + side], ga, TN)
                key = (b, g, side)
                sums[key] = sums[key] + u if key in sums else u
        for b in range(kv_cols // LANES):
            grad = jnp.where(
                low,
                sums[b, 0, 0] + swap(sums[b, 0, 1]),
                swap(sums[b, 1, 0]) + sums[b, 1, 1],
            )
            gv_own[:, b * LANES : (b + 1) * LANES] = grad.astype(BF16)

    def a_copy(d):
        return remote(
            att_own, a_in.at[d - 1], snd.at[0], a_rcv.at[d - 1], {"seq": device(d, core)}
        )

    def a_far():
        return remote(
            att_own, ad_in, snd.at[0], a_rcv.at[far - 1], {"seq": device(far, core)}
        )

    def a_beside():
        return remote(att_own, att.at[1], snd.at[0], b_rcv.at[1], {"seq": partner})

    def send_attended():
        each(1, far, lambda d: a_copy(d).start())
        pl.when(chip >= far)(lambda: a_far().start())
        a_beside().start()

    def g_copy(d):
        return remote(
            gv_own, g_in.at[d - 1], snd.at[0], g_rcv.at[d - 1], {"seq": device(-d, core)}
        )

    def g_far():
        return remote(
            gv_own, gd_in, snd.at[0], g_rcv.at[far - 1], {"seq": device(far, core)}
        )

    def g_beside():
        return remote(gv_own, gv.at[1], snd.at[0], b_rcv.at[2], {"seq": partner})

    def send_grads():
        pl.when(low_chip)(lambda: g_far().start())
        each(1, far, lambda d: g_copy(d).start())
        g_beside().start()

    lane_at = lax.broadcasted_iota(jnp.int32, (1, lanes), 1)

    def weigh(row, source, d, b):
        at = pl.ds(source, 1)
        sums[row, at, :] = sums[row, at, :] + jnp.sum(d * b, axis=0, keepdims=True)

    def overlap_attended(d):
        a_copy(d).wait_recv()
        over[2 * d - 1] = two(att, a_in.at[d - 1])

    def overlap_grads(d):
        g_copy(d).wait_recv()
        over[2 * d - 2] = two(gv, g_in.at[d - 1])

    def overlap_far_attended():
        @pl.when(low_chip)
        def _():
            a_far().wait_recv()
            over[ring - 2] = two(att, ad_in)

    def overlap_far_grads():
        @pl.when(chip >= far)
        def _():
            g_far().wait_recv()
            over[ring - 2] = two(gv, gd_in)

    def score(g, hop):
        for row in range(2):
            weigh(
                row, device(hop, core), full[2 * g + row].astype(F32),
                over[g, :, row * length : (row + 1) * length],
            )

    def score_near(d):
        totals_here(2 * d - 2)
        score(2 * d - 2, d)
        totals_here(2 * d - 1)
        score(2 * d - 1, -d)

    lower, upper, anywhere = col < mid, col >= mid, col >= 0
    project_states(0)
    relay_first()
    follow(1)
    remote(own.at[0], own.at[0], snd.at[0], pair_rcv.at[0], {"seq": partner}).wait_recv()
    settle(0, 1)
    arrivals(1, project_states)
    if tp > 2:
        relay_up(0, 2, anywhere)
        follow(2)
    each(1, far, multiply_near)
    relay_up(1, 1, lower)
    relay_down(1, 1, upper)
    if tp > 2:
        relay_down(0, 2, anywhere)
    for k in range(3, tp):
        relay(0, k)
        follow(k)
    project_cot(0)
    relay_up(1, 1, upper)
    for k in range(2, tp - 1):
        settle(0, k)
        arrivals(k, project_states)

    each(0, ring - 2, chain)
    multiply_far()
    relay_down(1, 1, lower)

    @pl.when(jnp.logical_not(edge))
    def _():
        attend()
        send_attended()

    chain(ring - 2)
    for k in range(2, tp):
        relay(1, k)
    for k in range(max(2, tp - 1), tp):
        settle(0, k)
        arrivals(k, project_states)

    @pl.when(edge)
    def _():
        attend()
        send_attended()

    square(0, range(tp))
    for k in range(1, tp):
        settle(1, k)
        arrivals(k, project_cot)
    grad_values()
    send_grads()
    pl.when(core == 0)(lambda: each(0, ring - 1, total_out))
    pl.when(core == 1)(lambda: each(0, ring - 1, total))
    clear_links()
    pl.when((core == 1) & central)(
        lambda: each(0, ring - 1, lambda g: outer(g, lambda c: c.start()))
    )
    square(1, range(tp))
    multiply_beside(0)
    a_beside().wait_recv()
    sums[...] = jnp.zeros_like(sums)
    weigh(0, me, near[1], dot(att_own[...], att_own[...], NT))
    weigh(0, me, near[0], dot(gv_own[...], gv_own[...], NT))

    each(1, far, overlap_attended)
    overlap_far_attended()
    multiply_beside(1)

    @pl.when(core == 1)
    def _():
        weigh(0, partner, near[2], dot(att_own[...], att[1], NT))

    g_beside().wait_recv()

    @pl.when(core == 0)
    def _():
        weigh(0, partner, near[2], dot(gv_own[...], gv[1], NT))

    each(1, far, overlap_grads)
    overlap_far_grads()
    each(1, far, score_near)
    totals_here(ring - 2)
    score(ring - 2, far)

    row_at = lax.broadcasted_iota(jnp.int32, (n, lanes), 0)
    spot_at = lax.broadcasted_iota(jnp.int32, (n, lanes), 1)
    for row in range(2):
        pairs = jnp.sum(sums[row], axis=1, keepdims=True)[:n]
        t2[col * n + me, :, row * lanes : (row + 1) * lanes] = jnp.sum(
            jnp.where(row_at == spot_at, pairs, 0.0), axis=0, keepdims=True
        )

    def send_scalars(plane, o):
        mine = t2.at[col * n + me]
        to = {"seq": (me + o) % n, "tp": plane}
        remote(mine, mine, r2_snd.at[0], r2_rcv.at[0], to).start()

    for t in range(tp):
        plane = jnp.where(col >= mid, t, last - t)
        each(1, n, lambda o: send_scalars(plane, o))
        pl.when(plane != col)(lambda: send_scalars(plane, 0))

    for k in range(1, tp):
        for which in range(2):
            for h in range(HALVES):
                if k == 1:
                    pl.when(sends_up(k))(lambda: up(which, k, h).wait_send())
                    pl.when(sends_down(k))(lambda: down(which, k, h).wait_send())
                else:
                    lasts_up, lasts_down = ends_up(which, k - 1), ends_down(which, k - 1)
                    pl.when(sends_up(k) & jnp.logical_not(lasts_up))(
                        lambda: up(which, k, h).wait_send()
                    )
                    pl.when(sends_down(k) & jnp.logical_not(lasts_down))(
                        lambda: down(which, k, h).wait_send()
                    )
    pl.when(jnp.logical_not(edge))(last_relays)

    def drain_near(d):
        for c in (x_copy(d), c_copy(d), a_copy(d), g_copy(d)):
            c.wait_send()

    each(1, far, drain_near)
    far_copy(states_ref).wait_send()
    for c in (pair_copy(0), pair_copy(1), a_beside(), g_beside()):
        c.wait_send()
    for slot in range(tp):
        beside(0, slot).wait_send()
    pl.when(chip >= far)(lambda: a_far().wait_send())
    pl.when(low_chip)(lambda: g_far().wait_send())

    def drain_sums(g):
        inner(g, lambda c: c.wait_send())
        outer(g, lambda c: c.wait_send())

    each(0, ring - 1, drain_sums)
    others = t2.at[pl.ds(0, n * tp - 1)]
    everyone = remote(others, others, r2_snd.at[0], r2_rcv.at[0], {"seq": partner})
    everyone.wait_recv()
    both = t2[pl.ds(0, n)].reshape(n, 2 * lanes)
    for q in range(1, tp):
        both = both + t2[pl.ds(q * n, n)].reshape(n, 2 * lanes)
    aside = both[:, lanes:]
    aside = jnp.where(row_at % 2 == 0, pltpu.roll(aside, n - 1, 0), pltpu.roll(aside, 1, 0))
    table = both[:, :lanes] + aside
    rank, spot = row_at, spot_at
    eye = rank == spot
    column = jnp.sum(jnp.where(spot == me, table, 0.0), axis=1, keepdims=True)
    theirs = eye & (rank != me)
    mirrored = jnp.sum(jnp.where(theirs, column, 0.0), axis=0, keepdims=True)
    own = jnp.sum(jnp.where(rank == me, table, 0.0), axis=0, keepdims=True)
    diag = jnp.sum(jnp.where(eye, table, 0.0), axis=0, keepdims=True)
    own_diag = jnp.sum(jnp.where(lane_at == me, diag, 0.0), axis=1, keepdims=True)
    gram = (own + mirrored) / jnp.sqrt(own_diag * diag)
    out_ref[...] = gram[:, :n]
    everyone.wait_send()


def on_device(n, tp, states, cotangent, wq, wk, wv, wo):
    seq_dev, length, width = states.shape
    assert seq_dev == 1 and n % 4 == 0 and length == LANES and tp > 1
    kv = wk.shape[1]
    ring = n // 2
    far = ring // 2
    near = max(far - 1, 1)
    tiles = 2 * (ring - 1)
    lanes = -(-n // LANES) * LANES
    cos, sin = rope_tables(length)
    vmem = pl.BlockSpec(memory_space=pltpu.VMEM)
    hbm = pl.BlockSpec(memory_space=pl.ANY)
    sem = pltpu.SemaphoreType.DMA

    def half(*shape):
        return pltpu.VMEM(shape, BF16)

    def wide(*shape):
        return pltpu.VMEM(shape, F32)

    return pl.pallas_call(
        functools.partial(kernel, n, tp),
        out_shape=pltpu.VMEM((1, n), F32),
        in_specs=[hbm] * 8,
        out_specs=vmem,
        scratch_shapes=[
            half(2, 2, length, width),
            wide(2, length, LANES),
            half(tp - 1, length, width),
            half(tp - 1, length, width),
            half(tp * width, wq.shape[1] + 2 * kv),
            half(wo.shape[0], tp * width),
            wide(length, wq.shape[1] + 2 * kv),
            wide(length, wo.shape[0]),
            half(near, length, width),
            half(near, length, width),
            half(length, width),
            half(tp, length, width),
            half(2, length, width),
            half(near, length, width),
            half(length, width),
            half(2, length, kv),
            half(near, length, kv),
            half(length, kv),
            half(width // HEAD_DIM, length, length),
            half(tiles, length, length),
            half(tiles, length, length),
            half(tiles, length, length),
            half(tiles, length, length),
            wide(3, length, length),
            wide(ring - 1, length, 2 * length),
            wide(2, -(-n // 8) * 8, LANES),
            wide(tp * n, 1, 2 * lanes),
            sem((2,)),
            pltpu.SemaphoreType.REGULAR,
            sem((2,)),
            sem((1,)),
            sem((HALVES,)),
            sem((2, tp - 1, HALVES)),
            sem((2, near)),
            sem((1,)),
            sem((1,)),
            sem((3,)),
            sem((far,)),
            sem((far,)),
            sem((ring - 1,)),
            sem((ring - 1,)),
            sem((ring - 1,)),
            sem((1,)),
            sem((1,)),
        ],
        compiler_params=pltpu.CompilerParams(
            collective_id=0, has_side_effects=True, vmem_limit_bytes=60 * 1024 * 1024
        ),
        name="ntk_gram",
    )(
        states.reshape(length, width), cotangent.reshape(length, width),
        jnp.asarray(cos), jnp.asarray(sin), wq, wk, wv, wo,
    )


def solution(mesh):
    in_specs = (
        P("seq", None, "tp"),
        P("seq", None, "tp"),
        P(None, "tp"),
        P(None, "tp"),
        P(None, "tp"),
        P("tp", None),
    )
    return jax.shard_map(
        functools.partial(on_device, mesh.shape["seq"], mesh.shape["tp"]),
        mesh=mesh, in_specs=in_specs, out_specs=P("seq", None), check_vma=False,
    )
```
